32 devices in a mesh: dp: 16 (over z, y, core), shard: 2 (over x).
Axes of the slice: x: 2, y: 2, z: 4, core: 2. Of those that a mesh axis runs over, the one named last changes fastest.
Arguments:
- inputs: bfloat16 [64, 576, 768], P(('dp', 'shard')), may hold values from -6 to 6
- cotangent: bfloat16 [64, 576, 768], P(('dp', 'shard')), may hold values from -6 to 6
- regions: int32 [576], replicated, may hold values from 0 to 8, as said below
- attend: float32 [768, 2304], P('dp', 'shard'), may hold values from -0.21875 to 0.21875
- attend_first: float32 [768, 2304], P('dp', 'shard'), may hold values from -0.0078125 to 0.0078125
- attend_second: float32 [768, 2304], P('dp', 'shard'), may hold values from 8.138021e-09 to 8.138021e-08
- project: float32 [768, 768], P('dp', 'shard'), may hold values from -0.4375 to 0.4375
- project_first: float32 [768, 768], P('dp', 'shard'), may hold values from -0.0078125 to 0.0078125
- project_second: float32 [768, 768], P('dp', 'shard'), may hold values from 8.138021e-09 to 8.138021e-08
- expand: float32 [768, 3072], P('dp', 'shard'), may hold values from -0.21875 to 0.21875
- expand_first: float32 [768, 3072], P('dp', 'shard'), may hold values from -0.0078125 to 0.0078125
- expand_second: float32 [768, 3072], P('dp', 'shard'), may hold values from 8.138021e-09 to 8.138021e-08
- contract: float32 [3072, 768], P('dp', 'shard'), may hold values from -0.109375 to 0.109375
- contract_first: float32 [3072, 768], P('dp', 'shard'), may hold values from -0.0078125 to 0.0078125
- contract_second: float32 [3072, 768], P('dp', 'shard'), may hold values from 8.138021e-09 to 8.138021e-08
- gains: float32 [2, 768], replicated, may hold values from 0.5 to 1.5
- gains_first: float32 [2, 768], replicated, may hold values from -0.0078125 to 0.0078125
- gains_second: float32 [2, 768], replicated, may hold values from 8.138021e-09 to 8.138021e-08
- shifts: float32 [2, 768], replicated, may hold values from -2 to 2
- shifts_first: float32 [2, 768], replicated, may hold values from -0.0078125 to 0.0078125
- shifts_second: float32 [2, 768], replicated, may hold values from 8.138021e-09 to 8.138021e-08
- biases: float32 [6912], replicated, may hold values from -2 to 2
- biases_first: float32 [6912], replicated, may hold values from -0.0078125 to 0.0078125
- biases_second: float32 [6912], replicated, may hold values from 8.138021e-09 to 8.138021e-08
- position: float32 [529, 24], replicated, may hold values from -4 to 4
- position_first: float32 [529, 24], replicated, may hold values from -0.0078125 to 0.0078125
- position_second: float32 [529, 24], replicated, may hold values from 8.138021e-09 to 8.138021e-08
Outputs:
- block_output: bfloat16 [64, 576, 768], P(('dp', 'shard'))
- input_gradient: float32 [64, 576, 768], P(('dp', 'shard'))
- attend_weight: float32 [768, 2304], P('dp', 'shard')
- attend_momentum: float32 [768, 2304], P('dp', 'shard')
- attend_variance: float32 [768, 2304], P('dp', 'shard')
- attend_copy: bfloat16 [768, 2304], P('dp', 'shard')
- project_weight: float32 [768, 768], P('dp', 'shard')
- project_momentum: float32 [768, 768], P('dp', 'shard')
- project_variance: float32 [768, 768], P('dp', 'shard')
- project_copy: bfloat16 [768, 768], P('dp', 'shard')
- expand_weight: float32 [768, 3072], P('dp', 'shard')
- expand_momentum: float32 [768, 3072], P('dp', 'shard')
- expand_variance: float32 [768, 3072], P('dp', 'shard')
- expand_copy: bfloat16 [768, 3072], P('dp', 'shard')
- contract_weight: float32 [3072, 768], P('dp', 'shard')
- contract_momentum: float32 [3072, 768], P('dp', 'shard')
- contract_variance: float32 [3072, 768], P('dp', 'shard')
- contract_copy: bfloat16 [3072, 768], P('dp', 'shard')
- gains_weight: float32 [2, 768], replicated
- gains_momentum: float32 [2, 768], replicated
- gains_variance: float32 [2, 768], replicated
- shifts_weight: float32 [2, 768], replicated
- shifts_momentum: float32 [2, 768], replicated
- shifts_variance: float32 [2, 768], replicated
- biases_weight: float32 [6912], replicated
- biases_momentum: float32 [6912], replicated
- biases_variance: float32 [6912], replicated
- position_weight: float32 [529, 24], replicated
- position_momentum: float32 [529, 24], replicated
- position_variance: float32 [529, 24], replicated
- norm_pairs: float32 [8, 2], replicated
The draws below stay inside these ranges and needn't reach their ends.
Inputs may be any that keep to these rules, and one draw needn't show every extreme that they name: `regions`: label of each token of the rolled 24 x 24 grid, row-major: 3 times the band of its row plus the band of its column, where a line's bands are split at 12 and at one drawn position after it, drawn for rows and columns apart.
All inputs are finite; a program needn't handle non-finite values.
Results may differ from the reference program's by a relative error of at most 0.0095.
The reference program's roundings to bfloat16 on the way count: a program that leaves them out, or rounds other values in their place, can miss the bound.
Values may be sent and summed in bfloat16 or wider, within the bound.
A program may use at most 256 MiB of HBM per device.

```python
import math
import jax
import jax.numpy as jnp
from jax import lax

D = 768
FF = 3072
HD = 32
WIN = 12
STEP = 10
HEADS = 24
GRID = 24
SHIFT = 6
IMG_TOK = 576
TABLE = 529
IMAGES = 64
TOKENS = 36864


def draw_regions(key, part):
    first_key, second_key = jax.random.split(jax.random.fold_in(key, 17))
    row_cut = jax.random.randint(first_key, (), 1, WIN)
    column_cut = jax.random.randint(second_key, (), 1, WIN)
    places = jnp.arange(GRID, dtype=jnp.int32)

    def bands(cut_at):
        return (places >= GRID - WIN).astype(jnp.int32) + (places >= GRID - cut_at).astype(jnp.int32)
    labels = bands(row_cut)[:, None] * 3 + bands(column_cut)[None, :]
    return labels.reshape(GRID * GRID).astype(jnp.int32)


def levels(key, dims, pieces, least, largest):
    def one(dim, blocks):
        heights = jax.random.uniform(jax.random.fold_in(jax.random.fold_in(key, 6), dim), (blocks,), jnp.float32, least / len(pieces), largest / len(pieces))
        return jnp.repeat(jnp.exp(heights), dims[dim] // blocks).reshape((-1,) + (1,) * (len(dims) - dim - 1))

    loudness = one(*pieces[0])
    for cut in pieces[1:]:
        loudness = loudness * one(*cut)
    return loudness


def scatter_about(own_key, dims, deviation, most, shards=(), held_as=jnp.bfloat16):
    entries = deviation * jax.random.normal(own_key, dims, jnp.float32)
    if shards:
        entries = entries * levels(own_key, dims, shards, -0.22, 0.18)
    return jnp.clip(entries, -most, most).astype(held_as)


def setup_inputs(seed: int = 0) -> dict:
    seeds = jax.random.split(jax.random.key(seed), 28)
    return {
        "inputs": scatter_about(seeds[0], (IMAGES, IMG_TOK, D), 1.0, 6.0, ((0, 32),)),
        "cotangent": scatter_about(seeds[1], (IMAGES, IMG_TOK, D), 1.0, 6.0, ((0, 32),)),
        "regions": draw_regions(jax.random.fold_in(seeds[27], 71), 0),
        "attend": scatter_about(seeds[3], (D, 3 * D), D ** -0.5, 0.21875, ((0, 16), (1, 2)), jnp.float32),
        "attend_first": scatter_about(seeds[4], (D, 3 * D), (0.1 * TOKENS ** -0.5), 0.0078125, ((0, 16), (1, 2)), jnp.float32),
        "attend_second": jnp.clip(jnp.exp(math.log(8.138020746173424e-08) - 2.3025851 * jax.random.uniform(seeds[5], (D, 3 * D), jnp.float32) ** levels(seeds[5], (D, 3 * D), ((0, 16), (1, 2)), -0.2, 0.2)), 8.138020923809108e-09, 8.138020746173424e-08),
        "project": scatter_about(seeds[6], (D, D), (D // 4) ** -0.5, 0.4375, ((0, 16), (1, 2)), jnp.float32),
        "project_first": scatter_about(seeds[7], (D, D), (0.1 * TOKENS ** -0.5), 0.0078125, ((0, 16), (1, 2)), jnp.float32),
        "project_second": jnp.clip(jnp.exp(math.log(8.138020746173424e-08) - 2.3025851 * jax.random.uniform(seeds[8], (D, D), jnp.float32) ** levels(seeds[8], (D, D), ((0, 16), (1, 2)), -0.2, 0.2)), 8.138020923809108e-09, 8.138020746173424e-08),
        "expand": scatter_about(seeds[9], (D, FF), D ** -0.5, 0.21875, ((0, 16), (1, 2)), jnp.float32),
        "expand_first": scatter_about(seeds[10], (D, FF), (0.1 * TOKENS ** -0.5), 0.0078125, ((0, 16), (1, 2)), jnp.float32),
        "expand_second": jnp.clip(jnp.exp(math.log(8.138020746173424e-08) - 2.3025851 * jax.random.uniform(seeds[11], (D, FF), jnp.float32) ** levels(seeds[11], (D, FF), ((0, 16), (1, 2)), -0.2, 0.2)), 8.138020923809108e-09, 8.138020746173424e-08),
        "contract": scatter_about(seeds[12], (FF, D), FF ** -0.5, 0.109375, ((0, 16), (1, 2)), jnp.float32),
        "contract_first": scatter_about(seeds[13], (FF, D), (0.1 * TOKENS ** -0.5), 0.0078125, ((0, 16), (1, 2)), jnp.float32),
        "contract_second": jnp.clip(jnp.exp(math.log(8.138020746173424e-08) - 2.3025851 * jax.random.uniform(seeds[14], (FF, D), jnp.float32) ** levels(seeds[14], (FF, D), ((0, 16), (1, 2)), -0.2, 0.2)), 8.138020923809108e-09, 8.138020746173424e-08),
        "gains": jnp.clip(1.0 + 0.1 * jax.random.normal(seeds[15], (2, D), jnp.float32), 0.5, 1.5),
        "gains_first": scatter_about(seeds[16], (2, D), (0.1 * TOKENS ** -0.5), 0.0078125, (), jnp.float32),
        "gains_second": jnp.clip(jnp.exp(jax.random.uniform(seeds[17], (2, D), jnp.float32, math.log(8.138020923809108e-09), math.log(8.138020746173424e-08))), 8.138020923809108e-09, 8.138020746173424e-08),
        "shifts": scatter_about(seeds[18], (2, D), 0.3, 2.0, (), jnp.float32),
        "shifts_first": scatter_about(seeds[19], (2, D), (0.1 * TOKENS ** -0.5), 0.0078125, (), jnp.float32),
        "shifts_second": jnp.clip(jnp.exp(jax.random.uniform(seeds[20], (2, D), jnp.float32, math.log(8.138020923809108e-09), math.log(8.138020746173424e-08))), 8.138020923809108e-09, 8.138020746173424e-08),
        "biases": scatter_about(seeds[21], (5 * D + FF,), 0.3, 2.0, (), jnp.float32),
        "biases_first": scatter_about(seeds[22], (5 * D + FF,), (0.1 * TOKENS ** -0.5), 0.0078125, (), jnp.float32),
        "biases_second": jnp.clip(jnp.exp(jax.random.uniform(seeds[23], (5 * D + FF,), jnp.float32, math.log(8.138020923809108e-09), math.log(8.138020746173424e-08))), 8.138020923809108e-09, 8.138020746173424e-08),
        "position": scatter_about(seeds[24], (TABLE, HEADS), 1.0, 4.0, (), jnp.float32),
        "position_first": scatter_about(seeds[25], (TABLE, HEADS), (0.1 * TOKENS ** -0.5), 0.0078125, (), jnp.float32),
        "position_second": jnp.clip(jnp.exp(jax.random.uniform(seeds[26], (TABLE, HEADS), jnp.float32, math.log(8.138020923809108e-09), math.log(8.138020746173424e-08))), 8.138020923809108e-09, 8.138020746173424e-08),
    }


beta_one = 0.9
beta_two = 0.999
adam_eps = 1e-06
decay_rate = 0.01
learn_rate = 0.25
norm_eps = 1e-05
masked_score = -100.0
highest = lax.Precision.HIGHEST

@jax.custom_vjp
def low(v):
    return lax.optimization_barrier(v.astype(jnp.bfloat16)).astype(jnp.float32)

@jax.custom_vjp
def low_back(v):
    return v

def low_keep(v):
    return (low(v), None)

def low_pass(kept, grad):
    return (grad,)

def back_keep(v):
    return (v, None)

def back_low(kept, grad):
    return (low(grad),)
low.defvjp(low_keep, low_pass)
low_back.defvjp(back_keep, back_low)

def layer_norm(values, gain_row, shift_row):
    centred = values - lax.optimization_barrier(jnp.mean(values, axis=-1, keepdims=True))
    spread = lax.optimization_barrier(jnp.mean(centred * centred, axis=-1, keepdims=True))
    return centred * lax.rsqrt(spread + norm_eps) * gain_row + shift_row

def gelu_exact(values):
    return jax.nn.gelu(values, approximate=False)

def to_windows(values):
    images = values.shape[0]
    channels = values.shape[-1]
    layout = values.reshape(images, GRID, GRID, channels)
    layout = jnp.roll(layout, (-SHIFT, -SHIFT), axis=(1, 2))
    layout = layout.reshape(images, GRID // WIN, WIN, GRID // WIN, WIN, channels)
    return layout.transpose(0, 1, 3, 2, 4, 5).reshape(images * (GRID // WIN) ** 2, WIN * WIN, channels)

def from_windows(values, images):
    channels = values.shape[-1]
    layout = values.reshape(images, GRID // WIN, GRID // WIN, WIN, WIN, channels)
    layout = layout.transpose(0, 1, 3, 2, 4, 5).reshape(images, GRID, GRID, channels)
    layout = jnp.roll(layout, (SHIFT, SHIFT), axis=(1, 2))
    return layout.reshape(images, GRID * GRID, channels)

def relative_index():
    places = jnp.arange(WIN * WIN, dtype=jnp.int32)
    row_of = places // WIN
    column = places % WIN
    return ((row_of[:, None] - row_of[None, :] + WIN - 1) * (2 * WIN - 1) + (column[:, None] - column[None, :] + WIN - 1)).astype(jnp.int32)

def window_allowed(regions):
    labels = regions.reshape(GRID // WIN, WIN, GRID // WIN, WIN).transpose(0, 2, 1, 3).reshape((GRID // WIN) ** 2, WIN * WIN)
    return labels[:, :, None] == labels[:, None, :]

def block_forward(values, params, allowed):
    attend, project, expand, contract, gains, shifts, biases, position = params
    images = values.shape[0]
    windows_count = images * (GRID // WIN) ** 2
    normed = low(layer_norm(values, gains[0], shifts[0]))
    windowed = to_windows(normed)
    triple = jnp.einsum('wtc,ce->wte', windowed, attend, precision=highest) + biases[:3 * D]
    triple = low(low_back(triple)).reshape(windows_count, WIN * WIN, 3, HEADS, HD)
    raw = low_back(jnp.einsum('wihd,wjhd->whij', triple[:, :, 0], triple[:, :, 1], precision=highest))
    table_bias = jnp.take(position, relative_index(), axis=0).transpose(2, 0, 1)
    scores = (raw * HD ** (-0.5) + table_bias[None]).reshape(images, (GRID // WIN) ** 2, HEADS, WIN * WIN, WIN * WIN)
    scores = jnp.where(allowed[None, :, None], scores, masked_score).reshape(windows_count, HEADS, WIN * WIN, WIN * WIN)
    weights = low(jax.nn.softmax(scores, axis=-1))
    mixed = jnp.einsum('whij,wjhd->wihd', weights, triple[:, :, 2], precision=highest).reshape(windows_count, WIN * WIN, D)
    merged = from_windows(low(low_back(mixed)), images)
    branch = low_back(jnp.einsum('itc,ce->ite', merged, project, precision=highest) + biases[3 * D:4 * D])
    middle = values + branch
    normed_two = low(layer_norm(middle, gains[1], shifts[1]))
    hidden = low_back(jnp.einsum('itc,cf->itf', normed_two, expand, precision=highest) + biases[4 * D:4 * D + FF])
    active = low(gelu_exact(hidden))
    return middle + low_back(jnp.einsum('itf,fc->itc', active, contract, precision=highest) + biases[4 * D + FF:])

def lamb_step(weight, first, second, gradient, decay):
    momentum = beta_one * first + (1.0 - beta_one) * gradient
    variance = beta_two * second + (1.0 - beta_two) * gradient * gradient
    ratio = momentum / (1.0 - beta_one ** STEP) / (jnp.sqrt(variance / (1.0 - beta_two ** STEP)) + adam_eps)
    update = ratio + decay * weight
    norms = jnp.stack([jnp.sqrt(jnp.sum(weight * weight)), jnp.sqrt(jnp.sum(update * update))])
    fresh = weight - learn_rate * norms[0] / (norms[1] + adam_eps) * update
    return (fresh, momentum, variance, norms)

def reference(inputs, cotangent, regions, attend, attend_first, attend_second, project, project_first, project_second, expand, expand_first, expand_second, contract, contract_first, contract_second, gains, gains_first, gains_second, shifts, shifts_first, shifts_second, biases, biases_first, biases_second, position, position_first, position_second):
    allowed = window_allowed(regions)
    masters = (attend, project, expand, contract, gains, shifts, biases, position)
    firsts = (attend_first, project_first, expand_first, contract_first, gains_first, shifts_first, biases_first, position_first)
    seconds = (attend_second, project_second, expand_second, contract_second, gains_second, shifts_second, biases_second, position_second)
    params = (low(attend), low(project), low(expand), low(contract), gains, shifts, biases, position)

    def forward(values, params_in):
        grouped = values.reshape(IMAGES // 4, 4, GRID * GRID, D)

        def one_group(piece):
            return block_forward(piece, params_in, allowed)
        outputs = lax.map(jax.checkpoint(one_group), grouped)
        return outputs.reshape(IMAGES, GRID * GRID, D)
    result, pullback = jax.vjp(forward, inputs.astype(jnp.float32), params)
    input_gradient, param_grads = pullback(cotangent.astype(jnp.float32))
    outputs = [result.astype(jnp.bfloat16), input_gradient]
    pairs = []
    for slot in range(8):
        decay = decay_rate if slot < 4 else 0.0
        fresh, momentum, variance, norms = lamb_step(masters[slot], firsts[slot], seconds[slot], param_grads[slot] / TOKENS, decay)
        outputs = outputs + [fresh, momentum, variance]
        if slot < 4:
            outputs = outputs + [fresh.astype(jnp.bfloat16)]
        pairs.append(norms)
    outputs = outputs + [jnp.stack(pairs)]
    return tuple(outputs)
```

```python
import jax
import jax.numpy as jnp
from jax import lax
from jax.experimental import pallas as pl
from jax.experimental.pallas import tpu as pltpu
from jax.sharding import PartitionSpec as P

HD = 32
WIN = 12
STEP = 10
HEADS = 24
GRID = 24
SHIFT = 6


beta_one = 0.9
beta_two = 0.999
adam_eps = 1e-06
decay_rate = 0.01
learn_rate = 0.25
norm_eps = 1e-05
masked_score = -100.0


def layer_norm(values, gain_row, shift_row):
    centred = values - jnp.mean(values, axis=-1, keepdims=True)
    spread = jnp.mean(centred * centred, axis=-1, keepdims=True)
    return centred * lax.rsqrt(spread + norm_eps) * gain_row + shift_row


def gelu_exact(values):
    return jax.nn.gelu(values, approximate=False)


def to_windows(values):
    images = values.shape[0]
    channels = values.shape[-1]
    layout = values.reshape(images, GRID, GRID, channels)
    layout = jnp.roll(layout, (-SHIFT, -SHIFT), axis=(1, 2))
    layout = layout.reshape(images, GRID // WIN, WIN, GRID // WIN, WIN, channels)
    return layout.transpose(0, 1, 3, 2, 4, 5).reshape(
        images * (GRID // WIN) ** 2, WIN * WIN, channels
    )


def from_windows(values, images):
    channels = values.shape[-1]
    layout = values.reshape(images, GRID // WIN, GRID // WIN, WIN, WIN, channels)
    layout = layout.transpose(0, 1, 3, 2, 4, 5).reshape(images, GRID, GRID, channels)
    layout = jnp.roll(layout, (SHIFT, SHIFT), axis=(1, 2))
    return layout.reshape(images, GRID * GRID, channels)


def window_labels(regions):
    return (
        regions.reshape(GRID // WIN, WIN, GRID // WIN, WIN)
        .transpose(0, 2, 1, 3)
        .reshape((GRID // WIN) ** 2, WIN * WIN)
    )


AREA = WIN * WIN
SPAN = 2 * WIN - 1
REACH = 384
TABLE_PAD = 640
HEAD_STEP = 4
CENTRE = (WIN - 1) * SPAN + WIN - 1


def dot00(left, right):
    return lax.dot_general(
        left, right, (((0,), (0,)), ((), ())), preferred_element_type=jnp.float32
    )


def dot11(left, right):
    return lax.dot_general(
        left, right, (((1,), (1,)), ((), ())), preferred_element_type=jnp.float32
    )


def dot10(left, right):
    return lax.dot_general(
        left, right, (((1,), (0,)), ((), ())), preferred_element_type=jnp.float32
    )


def spread_places(shape, table_dim, token_dim):
    token = lax.broadcasted_iota(jnp.int32, shape, token_dim)
    place = lax.broadcasted_iota(jnp.int32, shape, table_dim)
    token_row = token // WIN
    return place == token + (SPAN - WIN) * token_row


def bias_kernel(table_ref, bias_ref):
    spot = spread_places((REACH, AREA), 0, 1).astype(jnp.bfloat16)
    table = table_ref[...]
    for row in range(WIN):
        rolled = []
        for column in range(WIN):
            back = SPAN * (WIN - 1 - row) + WIN - 1 - column
            rolled.append(pltpu.roll(table, (TABLE_PAD - back) % TABLE_PAD, 1)[:, :REACH])
        block = jnp.concatenate(rolled, axis=0)
        high = block.astype(jnp.bfloat16)
        rest = block - high.astype(jnp.float32)
        middle = rest.astype(jnp.bfloat16)
        low = (rest - middle.astype(jnp.float32)).astype(jnp.bfloat16)
        picked = dot10(high, spot) + (dot10(middle, spot) + dot10(low, spot))
        for column in range(WIN):
            bias_ref[row * WIN + column] = picked[column * HEADS : (column + 1) * HEADS]


def table_kernel(scores_ref, table_ref):
    spot = spread_places((AREA, REACH), 1, 0).astype(jnp.bfloat16)
    total = jnp.zeros((HEADS, TABLE_PAD), jnp.float32)
    for row in range(WIN):
        block = scores_ref[row * WIN : (row + 1) * WIN].reshape(WIN * HEADS, AREA)
        high = block.astype(jnp.bfloat16)
        low = (block - high.astype(jnp.float32)).astype(jnp.bfloat16)
        spread = dot10(high, spot) + dot10(low, spot)
        inner = spread[:HEADS]
        for column in range(1, WIN):
            inner = pltpu.roll(inner, 1, 1) + spread[column * HEADS : (column + 1) * HEADS]
        inner = jnp.concatenate(
            [inner, jnp.zeros((HEADS, TABLE_PAD - REACH), jnp.float32)], axis=1
        )
        if row:
            total = pltpu.roll(total, SPAN, 1)
        total = total + inner
    table_ref[...] = total


def table_to_bias(position):
    rows = position.shape[0]
    table = jnp.pad(position.T, ((0, 0), (0, TABLE_PAD - rows)))
    spread = pl.pallas_call(
        bias_kernel,
        out_shape=jax.ShapeDtypeStruct((AREA, HEADS, AREA), jnp.float32),
        name="bias_kernel",
    )(table)
    return spread.transpose(1, 0, 2)


def scores_to_table(scores, rows):
    table = pl.pallas_call(
        table_kernel,
        out_shape=jax.ShapeDtypeStruct((HEADS, TABLE_PAD), jnp.float32),
        name="table_kernel",
    )(scores.transpose(1, 0, 2))
    return table[:, :rows].T


def scores_of(keyed, query, bias, allowed):
    return jnp.where(allowed, dot00(keyed, query) * HD ** (-0.5) + bias, masked_score)


def head_slices(ref, head):
    width = HEADS * HD
    return tuple(
        ref[0, pl.ds(pl.multiple_of(block * width + head * HD, HD), HD), :] for block in range(3)
    )


def forward_kernel(triple_ref, bias_ref, label_ref, column_ref, mixed_ref, log_ref):
    allowed = column_ref[0] == label_ref[0]

    def step(group, carry):
        for member in range(HEAD_STEP):
            head = group * HEAD_STEP + member
            query, keyed, valued = head_slices(triple_ref, head)
            scores = scores_of(keyed, query, bias_ref[head], allowed)
            top = jnp.max(scores, axis=0, keepdims=True)
            raised = jnp.exp(scores - top)
            total = jnp.sum(raised, axis=0, keepdims=True)
            probs = (raised * (1.0 / total)).astype(jnp.bfloat16)
            mixed_ref[0, pl.ds(pl.multiple_of(head * HD, HD), HD), :] = dot10(
                valued, probs
            ).astype(jnp.bfloat16)
            log_ref[0, head] = top + jnp.log(total)
        return carry

    lax.fori_loop(0, HEADS // HEAD_STEP, step, 0)


def backward_kernel(
    triple_ref, grad_ref, log_ref, bias_ref, label_ref, column_ref, out_ref, scores_ref
):
    allowed = column_ref[0] == label_ref[0]
    width = HEADS * HD

    @pl.when(pl.program_id(0) == 0)
    def _():
        scores_ref[...] = jnp.zeros_like(scores_ref)

    def step(group, carry):
        for member in range(HEAD_STEP):
            head = group * HEAD_STEP + member
            query, keyed, valued = head_slices(triple_ref, head)
            grad = grad_ref[0, pl.ds(pl.multiple_of(head * HD, HD), HD), :]
            scores = scores_of(keyed, query, bias_ref[head], allowed)
            probs = jnp.exp(scores - log_ref[0, head])
            grad_probs = dot00(valued, grad)
            weighted = probs * grad_probs
            mean = jnp.sum(weighted, axis=0, keepdims=True)
            grad_scores = jnp.where(allowed, weighted - probs * mean, 0.0)
            scores_ref[head] += grad_scores
            raw = (grad_scores * HD ** (-0.5)).astype(jnp.bfloat16)
            results = (
                dot10(keyed, raw),
                dot11(query, raw),
                dot11(grad, probs.astype(jnp.bfloat16)),
            )
            for block in range(3):
                rows = pl.ds(pl.multiple_of(block * width + head * HD, HD), HD)
                out_ref[0, rows, :] = results[block].astype(jnp.bfloat16)
        return carry

    lax.fori_loop(0, HEADS // HEAD_STEP, step, 0)


def window_block(rows):
    return pl.BlockSpec((1, rows, AREA), lambda window: (window, 0, 0))


def label_blocks(count):
    return [
        pl.BlockSpec((1, 1, AREA), lambda window: (window % count, 0, 0)),
        pl.BlockSpec((1, AREA, 1), lambda window: (window % count, 0, 0)),
    ]


def attend_forward(triple, bias, labels):
    windows = triple.shape[0]
    width = HEADS * HD
    whole = pl.BlockSpec((HEADS, AREA, AREA), lambda window: (0, 0, 0))
    log_block = pl.BlockSpec((1, HEADS, 1, AREA), lambda window: (window, 0, 0, 0))
    return pl.pallas_call(
        forward_kernel,
        grid=(windows,),
        in_specs=[window_block(3 * width), whole] + label_blocks(labels.shape[0]),
        out_specs=[window_block(width), log_block],
        out_shape=[
            jax.ShapeDtypeStruct((windows, width, AREA), jnp.bfloat16),
            jax.ShapeDtypeStruct((windows, HEADS, 1, AREA), jnp.float32),
        ],
        name="forward_kernel",
    )(triple, bias, labels[:, None, :], labels[:, :, None])


def attend_backward(triple, grad, log_total, bias, labels):
    windows = triple.shape[0]
    width = HEADS * HD
    whole = pl.BlockSpec((HEADS, AREA, AREA), lambda window: (0, 0, 0))
    log_block = pl.BlockSpec((1, HEADS, 1, AREA), lambda window: (window, 0, 0, 0))
    return pl.pallas_call(
        backward_kernel,
        grid=(windows,),
        in_specs=[window_block(3 * width), window_block(width), log_block, whole]
        + label_blocks(labels.shape[0]),
        out_specs=[window_block(3 * width), whole],
        out_shape=[
            jax.ShapeDtypeStruct((windows, 3 * width, AREA), jnp.bfloat16),
            jax.ShapeDtypeStruct((HEADS, AREA, AREA), jnp.float32),
        ],
        name="backward_kernel",
    )(triple, grad, log_total, bias, labels[:, None, :], labels[:, :, None])


def product_left(left, right):
    return lax.dot_general(
        left, right, (((0,), (0,)), ((), ())), preferred_element_type=jnp.float32
    )


def product_right(left, right):
    return lax.dot_general(
        left, right, (((1,), (1,)), ((), ())), preferred_element_type=jnp.float32
    )


def whole_step(values_low, cot_low, full, gains, shifts, biases, bias, labels, table_rows):
    attend, project, expand, contract = full
    width = attend.shape[0]
    hidden_width = expand.shape[1]
    windows = values_low.shape[0] // AREA
    values = values_low.astype(jnp.float32)
    normed, norm_back = jax.vjp(layer_norm, values, gains[0], shifts[0])
    normed_low = normed.astype(jnp.bfloat16)
    windowed = normed_low.reshape(windows, AREA, width)
    triple = jnp.einsum("wtc,ce->wet", windowed, attend, preferred_element_type=jnp.float32)
    triple = (triple + biases[: 3 * width][None, :, None]).astype(jnp.bfloat16)
    mixed, log_total = attend_forward(triple, bias, labels)
    branch = (
        jnp.einsum("wct,ce->wte", mixed, project, preferred_element_type=jnp.float32).reshape(
            -1, width
        )
        + biases[3 * width : 4 * width]
    )
    middle = values + branch
    normed_two, norm_two_back = jax.vjp(layer_norm, middle, gains[1], shifts[1])
    normed_two_low = normed_two.astype(jnp.bfloat16)
    hidden = (
        jnp.dot(normed_two_low, expand, preferred_element_type=jnp.float32)
        + biases[4 * width : 4 * width + hidden_width]
    )
    active, gelu_back = jax.vjp(gelu_exact, hidden)
    active_low = active.astype(jnp.bfloat16)
    result = middle + (
        jnp.dot(active_low, contract, preferred_element_type=jnp.float32)
        + biases[4 * width + hidden_width :]
    )
    cot_float = cot_low.astype(jnp.float32)
    grad_contract = product_left(active_low, cot_low)
    grad_bias_contract = jnp.sum(cot_float, axis=0)
    grad_active = product_right(cot_low, contract)
    grad_hidden_low = gelu_back(grad_active)[0].astype(jnp.bfloat16)
    grad_expand = product_left(normed_two_low, grad_hidden_low)
    grad_bias_expand = jnp.sum(grad_hidden_low, axis=0, dtype=jnp.float32)
    grad_normed_two = product_right(grad_hidden_low, expand)
    grad_middle_part, grad_gain_two, grad_shift_two = norm_two_back(grad_normed_two)
    grad_middle = cot_float + grad_middle_part
    grad_branch_low = grad_middle.astype(jnp.bfloat16)
    grad_branch_windows = grad_branch_low.reshape(windows, AREA, width)
    grad_project = jnp.einsum(
        "wct,wte->ce", mixed, grad_branch_windows, preferred_element_type=jnp.float32
    )
    grad_bias_project = jnp.sum(grad_branch_low, axis=0, dtype=jnp.float32)
    grad_mixed = jnp.einsum(
        "wte,ce->wct", grad_branch_windows, project, preferred_element_type=jnp.float32
    ).astype(jnp.bfloat16)
    grad_triple, grad_scores = attend_backward(triple, grad_mixed, log_total, bias, labels)
    grad_position = scores_to_table(grad_scores, table_rows)
    grad_attend = jnp.einsum(
        "wtc,wet->ce", windowed, grad_triple, preferred_element_type=jnp.float32
    )
    grad_bias_attend = jnp.sum(grad_triple, axis=(0, 2), dtype=jnp.float32)
    grad_normed = jnp.einsum(
        "wet,ce->wtc", grad_triple, attend, preferred_element_type=jnp.float32
    ).reshape(-1, width)
    grad_input_part, grad_gain_one, grad_shift_one = norm_back(grad_normed)
    grad_input = grad_middle + grad_input_part
    grads = (
        grad_attend,
        grad_project,
        grad_expand,
        grad_contract,
        jnp.stack([grad_gain_one, grad_gain_two]),
        jnp.stack([grad_shift_one, grad_shift_two]),
        jnp.concatenate(
            [grad_bias_attend, grad_bias_project, grad_bias_expand, grad_bias_contract]
        ),
        grad_position,
    )
    return (result.astype(jnp.bfloat16), grad_input, grads)


def moments(weight, first, second, gradient, decay):
    momentum = beta_one * first + (1.0 - beta_one) * gradient
    variance = beta_two * second + (1.0 - beta_two) * gradient * gradient
    ratio = (
        momentum / (1.0 - beta_one**STEP) / (jnp.sqrt(variance / (1.0 - beta_two**STEP)) + adam_eps)
    )
    return (momentum, variance, ratio + decay * weight)


def body(
    inputs,
    cotangent,
    regions,
    attend,
    attend_first,
    attend_second,
    project,
    project_first,
    project_second,
    expand,
    expand_first,
    expand_second,
    contract,
    contract_first,
    contract_second,
    gains,
    gains_first,
    gains_second,
    shifts,
    shifts_first,
    shifts_second,
    biases,
    biases_first,
    biases_second,
    position,
    position_first,
    position_second,
):
    masters = (attend, project, expand, contract, gains, shifts, biases, position)
    firsts = (
        attend_first,
        project_first,
        expand_first,
        contract_first,
        gains_first,
        shifts_first,
        biases_first,
        position_first,
    )
    seconds = (
        attend_second,
        project_second,
        expand_second,
        contract_second,
        gains_second,
        shifts_second,
        biases_second,
        position_second,
    )
    dp_count = lax.axis_size("dp")
    shard_count = lax.axis_size("shard")
    tokens_all = inputs.shape[0] * inputs.shape[1] * dp_count * shard_count
    halves = (
        lax.all_gather(attend.astype(jnp.bfloat16), "dp", axis=0, tiled=True),
        lax.all_gather(project.astype(jnp.bfloat16), "dp", axis=0, tiled=True),
        lax.all_gather(expand.astype(jnp.bfloat16), "dp", axis=0, tiled=True),
        lax.all_gather(contract.astype(jnp.bfloat16), "dp", axis=0, tiled=True),
    )
    labels = window_labels(regions)
    bias = table_to_bias(position)
    images = inputs.shape[0]
    width = inputs.shape[2]
    full = tuple(lax.all_gather(half, "shard", axis=1, tiled=True) for half in halves)
    result_low, grad_input, totals = whole_step(
        to_windows(inputs).reshape(-1, width),
        to_windows(cotangent).reshape(-1, width),
        full,
        gains,
        shifts,
        biases,
        bias,
        labels,
        position.shape[0],
    )
    result_low = from_windows(result_low, images)
    grad_input = from_windows(grad_input, images)
    totals = tuple((entry / tokens_all for entry in totals))
    small_grads = totals[4:]
    small_total = lax.psum(
        (small_grads[0], small_grads[1], small_grads[2], small_grads[3]), ("dp", "shard")
    )
    columns = (
        lax.psum_scatter(
            totals[0].astype(jnp.bfloat16), "shard", scatter_dimension=1, tiled=True
        ).astype(jnp.float32),
        lax.psum_scatter(
            totals[1].astype(jnp.bfloat16), "shard", scatter_dimension=1, tiled=True
        ).astype(jnp.float32),
        lax.psum_scatter(
            totals[2].astype(jnp.bfloat16), "shard", scatter_dimension=1, tiled=True
        ).astype(jnp.float32),
        lax.psum_scatter(
            totals[3].astype(jnp.bfloat16), "shard", scatter_dimension=1, tiled=True
        ).astype(jnp.float32),
    )
    owned = (
        lax.psum_scatter(columns[0], "dp", scatter_dimension=0, tiled=True),
        lax.psum_scatter(columns[1], "dp", scatter_dimension=0, tiled=True),
        lax.psum_scatter(columns[2], "dp", scatter_dimension=0, tiled=True),
        lax.psum_scatter(columns[3], "dp", scatter_dimension=0, tiled=True),
    )
    pieces = [
        moments(masters[slot], firsts[slot], seconds[slot], owned[slot], decay_rate)
        for slot in range(4)
    ]
    partial_value = jnp.stack(
        [
            jnp.stack(
                [jnp.sum(masters[slot] * masters[slot]), jnp.sum(pieces[slot][2] * pieces[slot][2])]
            )
            for slot in range(4)
        ]
    )
    squares = jnp.sum(lax.all_gather(partial_value, ("dp", "shard")), axis=0)
    matrix_norms = jnp.sqrt(squares)
    outputs = [result_low, grad_input]
    pairs = []
    for slot in range(4):
        momentum, variance, update = pieces[slot]
        fresh = (
            masters[slot]
            - learn_rate * matrix_norms[slot, 0] / (matrix_norms[slot, 1] + adam_eps) * update
        )
        outputs = outputs + [fresh, momentum, variance, fresh.astype(jnp.bfloat16)]
        pairs.append(matrix_norms[slot])
    for slot in range(4):
        weight = masters[4 + slot]
        momentum, variance, update = moments(
            weight, firsts[4 + slot], seconds[4 + slot], small_total[slot], 0.0
        )
        norms = jnp.stack([jnp.sqrt(jnp.sum(weight * weight)), jnp.sqrt(jnp.sum(update * update))])
        fresh = weight - learn_rate * norms[0] / (norms[1] + adam_eps) * update
        outputs = outputs + [fresh, momentum, variance]
        pairs.append(norms)
    outputs = outputs + [jnp.stack(pairs)]
    return tuple(outputs)


def solution(mesh):
    return jax.shard_map(
        body,
        mesh=mesh,
        in_specs=(
            P(("dp", "shard"), None, None),
            P(("dp", "shard"), None, None),
            P(),
            P("dp", "shard"),
            P("dp", "shard"),
            P("dp", "shard"),
            P("dp", "shard"),
            P("dp", "shard"),
            P("dp", "shard"),
            P("dp", "shard"),
            P("dp", "shard"),
            P("dp", "shard"),
            P("dp", "shard"),
            P("dp", "shard"),
            P("dp", "shard"),
            P(),
            P(),
            P(),
            P(),
            P(),
            P(),
            P(),
            P(),
            P(),
            P(),
            P(),
            P(),
        ),
        out_specs=(
            P(("dp", "shard"), None, None),
            P(("dp", "shard"), None, None),
            P("dp", "shard"),
            P("dp", "shard"),
            P("dp", "shard"),
            P("dp", "shard"),
            P("dp", "shard"),
            P("dp", "shard"),
            P("dp", "shard"),
            P("dp", "shard"),
            P("dp", "shard"),
            P("dp", "shard"),
            P("dp", "shard"),
            P("dp", "shard"),
            P("dp", "shard"),
            P("dp", "shard"),
            P("dp", "shard"),
            P("dp", "shard"),
            P(),
            P(),
            P(),
            P(),
            P(),
            P(),
            P(),
            P(),
            P(),
            P(),
            P(),
            P(),
            P(),
        ),
        check_vma=False,
    )
```

```python
import jax
import jax.numpy as jnp
from jax import lax
from jax.experimental import pallas as pl
from jax.experimental.pallas import tpu as pltpu
from jax.sharding import PartitionSpec as P

HD = 32
WIN = 12
STEP = 10
HEADS = 24
GRID = 24
SHIFT = 6


beta_one = 0.9
beta_two = 0.999
adam_eps = 1e-06
decay_rate = 0.01
learn_rate = 0.25
norm_eps = 1e-05
masked_score = -100.0


def layer_norm(values, gain_row, shift_row):
    centred = values - jnp.mean(values, axis=-1, keepdims=True)
    spread = jnp.mean(centred * centred, axis=-1, keepdims=True)
    return centred * lax.rsqrt(spread + norm_eps) * gain_row + shift_row


def gelu_exact(values):
    return jax.nn.gelu(values, approximate=False)


def to_windows(values):
    images = values.shape[0]
    channels = values.shape[-1]
    layout = values.reshape(images, GRID, GRID, channels)
    layout = jnp.roll(layout, (-SHIFT, -SHIFT), axis=(1, 2))
    layout = layout.reshape(images, GRID // WIN, WIN, GRID // WIN, WIN, channels)
    return layout.transpose(0, 1, 3, 2, 4, 5).reshape(
        images * (GRID // WIN) ** 2, WIN * WIN, channels
    )


def from_windows(values, images):
    channels = values.shape[-1]
    layout = values.reshape(images, GRID // WIN, GRID // WIN, WIN, WIN, channels)
    layout = layout.transpose(0, 1, 3, 2, 4, 5).reshape(images, GRID, GRID, channels)
    layout = jnp.roll(layout, (SHIFT, SHIFT), axis=(1, 2))
    return layout.reshape(images, GRID * GRID, channels)


def window_labels(regions):
    return (
        regions.reshape(GRID // WIN, WIN, GRID // WIN, WIN)
        .transpose(0, 2, 1, 3)
        .reshape((GRID // WIN) ** 2, WIN * WIN)
    )


AREA = WIN * WIN
SPAN = 2 * WIN - 1
REACH = 384
TABLE_PAD = 640
HEAD_STEP = 4
CENTRE = (WIN - 1) * SPAN + WIN - 1


def dot00(left, right):
    return lax.dot_general(
        left, right, (((0,), (0,)), ((), ())), preferred_element_type=jnp.float32
    )


def dot11(left, right):
    return lax.dot_general(
        left, right, (((1,), (1,)), ((), ())), preferred_element_type=jnp.float32
    )


def dot10(left, right):
    return lax.dot_general(
        left, right, (((1,), (0,)), ((), ())), preferred_element_type=jnp.float32
    )


def spread_places(shape, table_dim, token_dim):
    token = lax.broadcasted_iota(jnp.int32, shape, token_dim)
    place = lax.broadcasted_iota(jnp.int32, shape, table_dim)
    token_row = token // WIN
    return place == token + (SPAN - WIN) * token_row


def bias_kernel(table_ref, bias_ref):
    spot = spread_places((REACH, AREA), 0, 1).astype(jnp.bfloat16)
    table = table_ref[...]
    for row in range(WIN):
        rolled = []
        for column in range(WIN):
            back = SPAN * (WIN - 1 - row) + WIN - 1 - column
            rolled.append(pltpu.roll(table, (TABLE_PAD - back) % TABLE_PAD, 1)[:, :REACH])
        block = jnp.concatenate(rolled, axis=0)
        high = block.astype(jnp.bfloat16)
        rest = block - high.astype(jnp.float32)
        middle = rest.astype(jnp.bfloat16)
        low = (rest - middle.astype(jnp.float32)).astype(jnp.bfloat16)
        picked = dot10(high, spot) + (dot10(middle, spot) + dot10(low, spot))
        for column in range(WIN):
            bias_ref[row * WIN + column] = picked[column * HEADS : (column + 1) * HEADS]


def table_kernel(scores_ref, table_ref):
    spot = spread_places((AREA, REACH), 1, 0).astype(jnp.bfloat16)
    total = jnp.zeros((HEADS, TABLE_PAD), jnp.float32)
    for row in range(WIN):
        block = scores_ref[row * WIN : (row + 1) * WIN].reshape(WIN * HEADS, AREA)
        high = block.astype(jnp.bfloat16)
        low = (block - high.astype(jnp.float32)).astype(jnp.bfloat16)
        spread = dot10(high, spot) + dot10(low, spot)
        inner = spread[:HEADS]
        for column in range(1, WIN):
            inner = pltpu.roll(inner, 1, 1) + spread[column * HEADS : (column + 1) * HEADS]
        inner = jnp.concatenate(
            [inner, jnp.zeros((HEADS, TABLE_PAD - REACH), jnp.float32)], axis=1
        )
        if row:
            total = pltpu.roll(total, SPAN, 1)
        total = total + inner
    table_ref[...] = total


def table_to_bias(position):
    rows = position.shape[0]
    table = jnp.pad(position.T, ((0, 0), (0, TABLE_PAD - rows)))
    spread = pl.pallas_call(
        bias_kernel,
        out_shape=jax.ShapeDtypeStruct((AREA, HEADS, AREA), jnp.float32),
        name="bias_kernel",
    )(table)
    return spread.transpose(1, 0, 2)


def scores_to_table(scores, rows):
    table = pl.pallas_call(
        table_kernel,
        out_shape=jax.ShapeDtypeStruct((HEADS, TABLE_PAD), jnp.float32),
        name="table_kernel",
    )(scores.transpose(1, 0, 2))
    return table[:, :rows].T


def scores_of(keyed, query, bias, allowed):
    return jnp.where(allowed, dot00(keyed, query) * HD ** (-0.5) + bias, masked_score)


def head_slices(ref, head):
    width = HEADS * HD
    return tuple(
        ref[0, pl.ds(pl.multiple_of(block * width + head * HD, HD), HD), :] for block in range(3)
    )


def forward_kernel(triple_ref, bias_ref, label_ref, column_ref, mixed_ref, log_ref):
    allowed = column_ref[0] == label_ref[0]

    def step(group, carry):
        for member in range(HEAD_STEP):
            head = group * HEAD_STEP + member
            query, keyed, valued = head_slices(triple_ref, head)
            scores = scores_of(keyed, query, bias_ref[head], allowed)
            top = jnp.max(scores, axis=0, keepdims=True)
            raised = jnp.exp(scores - top)
            total = jnp.sum(raised, axis=0, keepdims=True)
            probs = (raised * (1.0 / total)).astype(jnp.bfloat16)
            mixed_ref[0, pl.ds(pl.multiple_of(head * HD, HD), HD), :] = dot10(
                valued, probs
            ).astype(jnp.bfloat16)
            log_ref[0, head] = top + jnp.log(total)
        return carry

    lax.fori_loop(0, HEADS // HEAD_STEP, step, 0)


def backward_kernel(
    triple_ref, grad_ref, log_ref, bias_ref, label_ref, column_ref, out_ref, scores_ref
):
    allowed = column_ref[0] == label_ref[0]
    width = HEADS * HD

    @pl.when(pl.program_id(0) == 0)
    def _():
        scores_ref[...] = jnp.zeros_like(scores_ref)

    def step(group, carry):
        for member in range(HEAD_STEP):
            head = group * HEAD_STEP + member
            query, keyed, valued = head_slices(triple_ref, head)
            grad = grad_ref[0, pl.ds(pl.multiple_of(head * HD, HD), HD), :]
            scores = scores_of(keyed, query, bias_ref[head], allowed)
            probs = jnp.exp(scores - log_ref[0, head])
            grad_probs = dot00(valued, grad)
            weighted = probs * grad_probs
            mean = jnp.sum(weighted, axis=0, keepdims=True)
            grad_scores = jnp.where(allowed, weighted - probs * mean, 0.0)
            scores_ref[head] += grad_scores
            raw = (grad_scores * HD ** (-0.5)).astype(jnp.bfloat16)
            results = (
                dot10(keyed, raw),
                dot11(query, raw),
                dot11(grad, probs.astype(jnp.bfloat16)),
            )
            for block in range(3):
                rows = pl.ds(pl.multiple_of(block * width + head * HD, HD), HD)
                out_ref[0, rows, :] = results[block].astype(jnp.bfloat16)
        return carry

    lax.fori_loop(0, HEADS // HEAD_STEP, step, 0)


def window_block(rows):
    return pl.BlockSpec((1, rows, AREA), lambda window: (window, 0, 0))


def label_blocks(count):
    return [
        pl.BlockSpec((1, 1, AREA), lambda window: (window % count, 0, 0)),
        pl.BlockSpec((1, AREA, 1), lambda window: (window % count, 0, 0)),
    ]


def attend_forward(triple, bias, labels):
    windows = triple.shape[0]
    width = HEADS * HD
    whole = pl.BlockSpec((HEADS, AREA, AREA), lambda window: (0, 0, 0))
    log_block = pl.BlockSpec((1, HEADS, 1, AREA), lambda window: (window, 0, 0, 0))
    return pl.pallas_call(
        forward_kernel,
        grid=(windows,),
        in_specs=[window_block(3 * width), whole] + label_blocks(labels.shape[0]),
        out_specs=[window_block(width), log_block],
        out_shape=[
            jax.ShapeDtypeStruct((windows, width, AREA), jnp.bfloat16),
            jax.ShapeDtypeStruct((windows, HEADS, 1, AREA), jnp.float32),
        ],
        name="forward_kernel",
    )(triple, bias, labels[:, None, :], labels[:, :, None])


def attend_backward(triple, grad, log_total, bias, labels):
    windows = triple.shape[0]
    width = HEADS * HD
    whole = pl.BlockSpec((HEADS, AREA, AREA), lambda window: (0, 0, 0))
    log_block = pl.BlockSpec((1, HEADS, 1, AREA), lambda window: (window, 0, 0, 0))
    return pl.pallas_call(
        backward_kernel,
        grid=(windows,),
        in_specs=[window_block(3 * width), window_block(width), log_block, whole]
        + label_blocks(labels.shape[0]),
        out_specs=[window_block(3 * width), whole],
        out_shape=[
            jax.ShapeDtypeStruct((windows, 3 * width, AREA), jnp.bfloat16),
            jax.ShapeDtypeStruct((HEADS, AREA, AREA), jnp.float32),
        ],
        name="backward_kernel",
    )(triple, grad, log_total, bias, labels[:, None, :], labels[:, :, None])


def product_left(left, right):
    return lax.dot_general(
        left, right, (((0,), (0,)), ((), ())), preferred_element_type=jnp.float32
    )


def product_right(left, right):
    return lax.dot_general(
        left, right, (((1,), (1,)), ((), ())), preferred_element_type=jnp.float32
    )


def whole_step(values_low, cot_low, full, gains, shifts, biases, bias, labels, table_rows):
    attend, project, expand, contract = full
    width = attend.shape[0]
    hidden_width = expand.shape[1]
    windows = values_low.shape[0] // AREA
    values = values_low.astype(jnp.float32)
    normed, norm_back = jax.vjp(layer_norm, values, gains[0], shifts[0])
    normed_low = normed.astype(jnp.bfloat16)
    windowed = normed_low.reshape(windows, AREA, width)
    triple = jnp.einsum("wtc,ce->wet", windowed, attend, preferred_element_type=jnp.float32)
    triple = (triple + biases[: 3 * width][None, :, None]).astype(jnp.bfloat16)
    mixed, log_total = attend_forward(triple, bias, labels)
    branch = (
        jnp.einsum("wct,ce->wte", mixed, project, preferred_element_type=jnp.float32).reshape(
            -1, width
        )
        + biases[3 * width : 4 * width]
    )
    middle = values + branch
    normed_two, norm_two_back = jax.vjp(layer_norm, middle, gains[1], shifts[1])
    normed_two_low = normed_two.astype(jnp.bfloat16)
    hidden = (
        jnp.dot(normed_two_low, expand, preferred_element_type=jnp.float32)
        + biases[4 * width : 4 * width + hidden_width]
    )
    active, gelu_back = jax.vjp(gelu_exact, hidden)
    active_low = active.astype(jnp.bfloat16)
    result = middle + (
        jnp.dot(active_low, contract, preferred_element_type=jnp.float32)
        + biases[4 * width + hidden_width :]
    )
    cot_float = cot_low.astype(jnp.float32)
    grad_contract = product_left(active_low, cot_low)
    grad_bias_contract = jnp.sum(cot_float, axis=0)
    grad_active = product_right(cot_low, contract)
    grad_hidden_low = gelu_back(grad_active)[0].astype(jnp.bfloat16)
    grad_expand = product_left(normed_two_low, grad_hidden_low)
    grad_bias_expand = jnp.sum(grad_hidden_low, axis=0, dtype=jnp.float32)
    grad_normed_two = product_right(grad_hidden_low, expand)
    grad_middle_part, grad_gain_two, grad_shift_two = norm_two_back(grad_normed_two)
    grad_middle = cot_float + grad_middle_part
    grad_branch_low = grad_middle.astype(jnp.bfloat16)
    grad_branch_windows = grad_branch_low.reshape(windows, AREA, width)
    grad_project = jnp.einsum(
        "wct,wte->ce", mixed, grad_branch_windows, preferred_element_type=jnp.float32
    )
    grad_bias_project = jnp.sum(grad_branch_low, axis=0, dtype=jnp.float32)
    grad_mixed = jnp.einsum(
        "wte,ce->wct", grad_branch_windows, project, preferred_element_type=jnp.float32
    ).astype(jnp.bfloat16)
    grad_triple, grad_scores = attend_backward(triple, grad_mixed, log_total, bias, labels)
    grad_position = scores_to_table(grad_scores, table_rows)
    grad_attend = jnp.einsum(
        "wtc,wet->ce", windowed, grad_triple, preferred_element_type=jnp.float32
    )
    grad_bias_attend = jnp.sum(grad_triple, axis=(0, 2), dtype=jnp.float32)
    grad_normed = jnp.einsum(
        "wet,ce->wtc", grad_triple, attend, preferred_element_type=jnp.float32
    ).reshape(-1, width)
    grad_input_part, grad_gain_one, grad_shift_one = norm_back(grad_normed)
    grad_input = grad_middle + grad_input_part
    grads = (
        grad_attend,
        grad_project,
        grad_expand,
        grad_contract,
        jnp.stack([grad_gain_one, grad_gain_two]),
        jnp.stack([grad_shift_one, grad_shift_two]),
        jnp.concatenate(
            [grad_bias_attend, grad_bias_project, grad_bias_expand, grad_bias_contract]
        ),
        grad_position,
    )
    return (result.astype(jnp.bfloat16), grad_input, grads)


ZS = 4
SPLIT = 2
GROUPS = ((0, 1, 2), (3, 4))
PARTS = ((0, None), (1, None), (3, 0), (2, None), (3, 1))


def special_mesh(dp_count, shard_count):
    return dp_count == ZS * SPLIT * SPLIT and shard_count == SPLIT


def places():
    at = lax.axis_index("dp")
    return at // 4, lax.rem(at // 2, 2), lax.rem(at, 2), lax.axis_index("shard")


def far_z(z, step):
    return (z, z + 1 - 2 * lax.rem(z, 2), lax.rem(z + 2, 4), 3 - z)[step]


def device(z, y, c, x):
    return {"dp": (z * 2 + y) * 2 + c, "shard": x}


def partners(z, y, c, x):
    return [device(far_z(z, step), y, c, x) for step in (1, 2, 3)] + [
        device(z, y, c, 1 - x),
        device(z, 1 - y, c, x),
        device(z, y, 1 - c, x),
    ]


def greet(devices):
    barrier = pltpu.get_barrier_semaphore()
    for one in devices:
        pl.semaphore_signal(
            barrier, inc=1, device_id=one, device_id_type=pl.DeviceIdType.MESH
        )
    pl.semaphore_wait(barrier, len(devices))


def remote(source, target, sends, receives, slot, where):
    return pltpu.make_async_remote_copy(
        src_ref=source,
        dst_ref=target,
        send_sem=sends.at[slot],
        recv_sem=receives.at[slot],
        device_id=where,
        device_id_type=pl.DeviceIdType.MESH,
    )


def columns_of(ref, x):
    half = ref.shape[-1] // 2
    return pl.ds(pl.multiple_of(x * half, 128), half)


def gather_kernel(*refs):
    own, full = refs[:4], refs[4:8]
    local_sem, sends, receives = refs[8:]
    z, y, c, x = places()
    greet(partners(z, y, c, x))
    count = len(PARTS)

    def own_part(part):
        matrix, half = PARTS[part]
        return own[matrix] if half is None else own[matrix].at[half]

    def spot(part, zi, yi, cols):
        matrix, half = PARTS[part]
        ref = full[matrix]
        if half is None:
            return ref.at[zi, yi, c, :, cols]
        return ref.at[zi, yi, c, half, :, cols]

    everything = slice(None)
    started = []

    def launch(source, target, phase, step, part, where):
        copy = remote(source, target, sends, receives, (phase * 4 + step) * count + part, where)
        copy.start()
        started.append(copy)
        return copy

    flights = {}
    for step in (1, 2, 3):
        for part in range(count):
            cols = columns_of(full[PARTS[part][0]], x)
            flights[0, step, part] = launch(
                own_part(part),
                spot(part, z, y, cols),
                0,
                step,
                part,
                device(far_z(z, step), y, c, x),
            )
    locals_ = []
    for part in range(count):
        cols = columns_of(full[PARTS[part][0]], x)
        copy = pltpu.make_async_copy(own_part(part), spot(part, z, y, cols), local_sem.at[part])
        copy.start()
        locals_.append(copy)
    for copy in locals_:
        copy.wait()
    across_x = device(z, y, c, 1 - x)
    across_y = device(z, 1 - y, c, x)
    across_core = device(z, y, 1 - c, x)

    def second(step):
        zi = far_z(z, step)
        for part in range(count):
            if step:
                flights[0, step, part].wait_recv()
            here = spot(part, zi, y, columns_of(full[PARTS[part][0]], x))
            where = across_x if part in GROUPS[0] else across_y
            flights[1, step, part] = launch(here, here, 1, step, part, where)

    def third(step):
        zi = far_z(z, step)
        for part in range(count):
            flights[1, step, part].wait_recv()
            if part in GROUPS[0]:
                here, where = spot(part, zi, y, everything), across_y
            else:
                cols = columns_of(full[PARTS[part][0]], x)
                here, where = spot(part, zi, everything, cols), across_x
            flights[2, step, part] = launch(here, here, 2, step, part, where)

    def fourth(step):
        zi = far_z(z, step)
        for part in range(count):
            flights[2, step, part].wait_recv()
            here = spot(part, zi, everything, everything)
            flights[3, step, part] = launch(here, here, 3, step, part, across_core)

    for stage in range(4 + 2):
        if stage < 4:
            second(stage)
        if 0 <= stage - 1 < 4:
            third(stage - 1)
        if 0 <= stage - 2 < 4:
            fourth(stage - 2)
    for step in range(4):
        for part in range(count):
            flights[3, step, part].wait_recv()
    for copy in started:
        copy.wait_send()


def gather_all(shards):
    rows = [shard.shape[0] for shard in shards]
    cols = [shard.shape[1] * 2 for shard in shards]
    own = list(shards[:3]) + [shards[3].reshape(2, rows[3] // 2, cols[3] // 2)]
    shapes = [(ZS, 2, 2, rows[m], cols[m]) for m in range(3)] + [
        (ZS, 2, 2, 2, rows[3] // 2, cols[3])
    ]
    anywhere = pl.BlockSpec(memory_space=pl.ANY)
    slots = 16 * len(PARTS)
    moved = sum(2 * ZS * 4 * rows[m] * cols[m] for m in range(4))
    full = pl.pallas_call(
        gather_kernel,
        in_specs=[anywhere] * 4,
        out_specs=[anywhere] * 4,
        out_shape=[jax.ShapeDtypeStruct(shape, jnp.bfloat16) for shape in shapes],
        scratch_shapes=[
            pltpu.SemaphoreType.DMA((len(PARTS),)),
            pltpu.SemaphoreType.DMA((slots,)),
            pltpu.SemaphoreType.DMA((slots,)),
        ],
        compiler_params=pltpu.CompilerParams(collective_id=0, has_side_effects=True),
        cost_estimate=pl.CostEstimate(flops=0, bytes_accessed=moved * 4, transcendentals=0),
        name="gather_kernel",
    )(*own)
    return tuple(full[m].reshape(ZS * 4 * rows[m], cols[m]) for m in range(4))


def add_rows(first, second, target):
    rows = target.shape[0]

    def step(index, carry):
        at = pl.ds(pl.multiple_of(index * 16, 16), 16)
        total = first(at).astype(jnp.float32) + second(at).astype(jnp.float32)
        target[at, :] = total.astype(target.dtype)
        return carry

    lax.fori_loop(0, rows // 16, step, 0)


def scatter_kernel(*refs):
    count = len(PARTS)
    grads, outs = refs[:4], refs[4:8]
    own = refs[8 : 8 + count]
    core_in = refs[8 + count : 8 + 2 * count]
    two_in = refs[8 + 2 * count : 8 + 3 * count]
    three_in = refs[8 + 3 * count : 8 + 4 * count]
    last = refs[8 + 4 * count : 8 + 5 * count]
    last_in = refs[8 + 5 * count : 8 + 6 * count]
    local_sem, sends, receives = refs[8 + 6 * count :]
    z, y, c, x = places()
    greet(partners(z, y, c, x))
    across_x = device(z, y, c, 1 - x)
    across_y = device(z, 1 - y, c, x)
    across_core = device(z, y, 1 - c, x)
    order = (3, 2, 1, 0)
    flights = {}
    started = []

    def launch(source, target, phase, step, part, where):
        copy = remote(source, target, sends, receives, (phase * 4 + step) * count + part, where)
        copy.start()
        started.append(copy)
        flights[phase, step, part] = copy

    def block(part, zi, ci):
        matrix, half = PARTS[part]
        ref = grads[matrix]
        return ref.at[zi, :, ci] if half is None else ref.at[zi, :, ci, half]

    held = {}
    for step in order:
        zi = far_z(z, step)
        for part in range(count):
            launch(block(part, zi, 1 - c), core_in[part].at[step], 0, step, part, across_core)
            copy = pltpu.make_async_copy(
                block(part, zi, c), own[part].at[step], local_sem.at[step * count + part]
            )
            copy.start()
            held[step, part] = copy

    def second(step):
        for part in range(count):
            held[step, part].wait()
            flights[0, step, part].wait_recv()
            for yi in range(2):
                mine, other = own[part].at[step, yi], core_in[part].at[step, yi]
                add_rows(lambda at: mine[at, :], lambda at: other[at, :], mine)
            if part in GROUPS[0]:
                away = own[part].at[step, :, :, columns_of(own[part], 1 - x)]
                launch(away, two_in[part].at[step], 1, step, part, across_x)
            else:
                launch(own[part].at[step, 1 - y], two_in[part].at[step], 1, step, part, across_y)

    def third(step):
        for part in range(count):
            flights[1, step, part].wait_recv()
            if part in GROUPS[0]:
                cols = columns_of(own[part], x)
                for yi in range(2):
                    mine, other = own[part].at[step, yi], two_in[part].at[step, yi]
                    add_rows(lambda at: mine[at, cols], lambda at: other[at, :], other)
                launch(two_in[part].at[step, 1 - y], three_in[part].at[step], 2, step, part, across_y)
            else:
                mine, other = own[part].at[step, y], two_in[part].at[step]
                add_rows(lambda at: mine[at, :], lambda at: other[at, :], other)
                away = two_in[part].at[step, :, columns_of(own[part], 1 - x)]
                launch(away, three_in[part].at[step], 2, step, part, across_x)

    def fourth(step):
        for part in range(count):
            flights[2, step, part].wait_recv()
            other = three_in[part].at[step]
            if part in GROUPS[0]:
                mine = two_in[part].at[step, y]
                first = lambda at: mine[at, :]
            else:
                mine = two_in[part].at[step]
                cols = columns_of(own[part], x)
                first = lambda at: mine[at, cols]
            add_rows(first, lambda at: other[at, :], last[part].at[step])
            if step:
                launch(
                    last[part].at[step],
                    last_in[part].at[step - 1],
                    3,
                    step,
                    part,
                    device(far_z(z, step), y, c, x),
                )

    for stage in range(4 + 2):
        if stage < 4:
            second(order[stage])
        if 0 <= stage - 1 < 4:
            third(order[stage - 1])
        if 0 <= stage - 2 < 4:
            fourth(order[stage - 2])
    for part in range(count):
        for step in (3, 2, 1):
            flights[3, step, part].wait_recv()
        matrix, half = PARTS[part]
        target = outs[matrix] if half is None else outs[matrix].at[half]
        mine, others = last[part].at[0], last_in[part]

        def finish(index, carry):
            at = pl.ds(pl.multiple_of(index * 16, 16), 16)
            total = mine[at, :].astype(jnp.float32)
            for step in range(3):
                total = total + others[step, at, :].astype(jnp.float32)
            target[at, :] = total
            return carry

        lax.fori_loop(0, target.shape[0] // 16, finish, 0)
    for copy in started:
        copy.wait_send()


def scatter_all(grads):
    rows = [grad.shape[0] // 16 for grad in grads]
    cols = [grad.shape[1] for grad in grads]
    viewed = [grads[m].reshape(ZS, 2, 2, rows[m], cols[m]) for m in range(3)] + [
        grads[3].reshape(ZS, 2, 2, 2, rows[3] // 2, cols[3])
    ]
    height = [rows[m] if half is None else rows[m] // 2 for m, half in PARTS]
    breadth = [cols[m] for m, _ in PARTS]
    both = range(len(PARTS))
    low = jnp.bfloat16
    scratch = (
        [pltpu.VMEM((4, 2, height[p], breadth[p]), low) for p in both]
        + [pltpu.VMEM((4, 2, height[p], breadth[p]), low) for p in both]
        + [
            pltpu.VMEM((4, 2, height[p], breadth[p] // 2), low)
            if p in GROUPS[0]
            else pltpu.VMEM((4, height[p], breadth[p]), low)
            for p in both
        ]
        + [pltpu.VMEM((4, height[p], breadth[p] // 2), low) for p in both]
        + [pltpu.VMEM((4, height[p], breadth[p] // 2), low) for p in both]
        + [pltpu.VMEM((3, height[p], breadth[p] // 2), low) for p in both]
    )
    slots = 16 * len(PARTS)
    shapes = [(rows[m], cols[m] // 2) for m in range(3)] + [(2, rows[3] // 2, cols[3] // 2)]
    outs = pl.pallas_call(
        scatter_kernel,
        in_specs=[pl.BlockSpec(memory_space=pl.ANY)] * 4,
        out_specs=[pl.BlockSpec(memory_space=pltpu.VMEM)] * 4,
        out_shape=[jax.ShapeDtypeStruct(shape, jnp.float32) for shape in shapes],
        scratch_shapes=scratch
        + [
            pltpu.SemaphoreType.DMA((4 * len(PARTS),)),
            pltpu.SemaphoreType.DMA((slots,)),
            pltpu.SemaphoreType.DMA((slots,)),
        ],
        compiler_params=pltpu.CompilerParams(
            collective_id=1, has_side_effects=True, vmem_limit_bytes=50 * 2**20
        ),
        name="scatter_kernel",
    )(*viewed)
    return tuple(outs[:3]) + (outs[3].reshape(rows[3], cols[3] // 2),)


def sum_kernel(value_ref, out_ref, incoming, sends, receives):
    z, y, c, x = places()
    hops = [
        device(z, y, 1 - c, x),
        device(z, y, c, 1 - x),
        device(z, 1 - y, c, x),
        device(far_z(z, 1), y, c, x),
        device(far_z(z, 2), y, c, x),
    ]
    greet(hops)
    source = value_ref
    for hop in range(5):
        copy = remote(source, incoming.at[hop], sends, receives, hop, hops[hop])
        copy.start()
        copy.wait()
        out_ref[...] = source[...] + incoming[hop]
        source = out_ref


def sum_all(value, name):
    return pl.pallas_call(
        sum_kernel,
        in_specs=[pl.BlockSpec(memory_space=pltpu.VMEM)],
        out_specs=pl.BlockSpec(memory_space=pltpu.VMEM),
        out_shape=jax.ShapeDtypeStruct(value.shape, jnp.float32),
        scratch_shapes=[
            pltpu.VMEM((5,) + value.shape, jnp.float32),
            pltpu.SemaphoreType.DMA((5,)),
            pltpu.SemaphoreType.DMA((5,)),
        ],
        compiler_params=pltpu.CompilerParams(collective_id=name, has_side_effects=True),
        name="sum_kernel",
    )(value)


def sum_small(arrays):
    sizes = [array.size for array in arrays]
    total = sum(sizes)
    rows = -(-total // 1024) * 8
    flat = jnp.concatenate([array.reshape(-1) for array in arrays])
    summed = sum_all(jnp.pad(flat, (0, rows * 128 - total)).reshape(rows, 128), 2).reshape(-1)
    outs = []
    at = 0
    for array, size in zip(arrays, sizes):
        outs.append(summed[at : at + size].reshape(array.shape))
        at += size
    return tuple(outs)


def sum_squares(value):
    wide = jnp.pad(value.reshape(-1), (0, 1024 - value.size)).reshape(8, 128)
    return sum_all(wide, 3).reshape(-1)[: value.size].reshape(value.shape)


def moments(weight, first, second, gradient, decay):
    momentum = beta_one * first + (1.0 - beta_one) * gradient
    variance = beta_two * second + (1.0 - beta_two) * gradient * gradient
    ratio = (
        momentum / (1.0 - beta_one**STEP) / (jnp.sqrt(variance / (1.0 - beta_two**STEP)) + adam_eps)
    )
    return (momentum, variance, ratio + decay * weight)


def body(
    inputs,
    cotangent,
    regions,
    attend,
    attend_first,
    attend_second,
    project,
    project_first,
    project_second,
    expand,
    expand_first,
    expand_second,
    contract,
    contract_first,
    contract_second,
    gains,
    gains_first,
    gains_second,
    shifts,
    shifts_first,
    shifts_second,
    biases,
    biases_first,
    biases_second,
    position,
    position_first,
    position_second,
):
    masters = (attend, project, expand, contract, gains, shifts, biases, position)
    firsts = (
        attend_first,
        project_first,
        expand_first,
        contract_first,
        gains_first,
        shifts_first,
        biases_first,
        position_first,
    )
    seconds = (
        attend_second,
        project_second,
        expand_second,
        contract_second,
        gains_second,
        shifts_second,
        biases_second,
        position_second,
    )
    dp_count = lax.axis_size("dp")
    shard_count = lax.axis_size("shard")
    tokens_all = inputs.shape[0] * inputs.shape[1] * dp_count * shard_count
    special = special_mesh(dp_count, shard_count)
    shards = tuple(master.astype(jnp.bfloat16) for master in masters[:4])
    if special:
        full = gather_all(shards)
    else:
        halves = [lax.all_gather(shard, "dp", axis=0, tiled=True) for shard in shards]
        full = tuple(lax.all_gather(half, "shard", axis=1, tiled=True) for half in halves)
    labels = window_labels(regions)
    bias = table_to_bias(position)
    images = inputs.shape[0]
    width = inputs.shape[2]
    result_low, grad_input, totals = whole_step(
        to_windows(inputs).reshape(-1, width),
        to_windows(cotangent).reshape(-1, width),
        full,
        gains,
        shifts,
        biases,
        bias,
        labels,
        position.shape[0],
    )
    result_low = from_windows(result_low, images)
    grad_input = from_windows(grad_input, images)
    totals = tuple((entry / tokens_all for entry in totals))
    small_grads = totals[4:]
    if special:
        small_total = sum_small(small_grads)
        owned = scatter_all([total.astype(jnp.bfloat16) for total in totals[:4]])
    else:
        small_total = lax.psum(small_grads, ("dp", "shard"))
        columns = [
            lax.psum_scatter(
                total.astype(jnp.bfloat16), "shard", scatter_dimension=1, tiled=True
            ).astype(jnp.float32)
            for total in totals[:4]
        ]
        owned = tuple(
            lax.psum_scatter(column, "dp", scatter_dimension=0, tiled=True) for column in columns
        )
    pieces = [
        moments(masters[slot], firsts[slot], seconds[slot], owned[slot], decay_rate)
        for slot in range(4)
    ]
    partial_value = jnp.stack(
        [
            jnp.stack(
                [jnp.sum(masters[slot] * masters[slot]), jnp.sum(pieces[slot][2] * pieces[slot][2])]
            )
            for slot in range(4)
        ]
    )
    if special:
        squares = sum_squares(partial_value)
    else:
        squares = lax.psum(partial_value, ("dp", "shard"))
    matrix_norms = jnp.sqrt(squares)
    outputs = [result_low, grad_input]
    pairs = []
    for slot in range(4):
        momentum, variance, update = pieces[slot]
        fresh = (
            masters[slot]
            - learn_rate * matrix_norms[slot, 0] / (matrix_norms[slot, 1] + adam_eps) * update
        )
        outputs = outputs + [fresh, momentum, variance, fresh.astype(jnp.bfloat16)]
        pairs.append(matrix_norms[slot])
    for slot in range(4):
        weight = masters[4 + slot]
        momentum, variance, update = moments(
            weight, firsts[4 + slot], seconds[4 + slot], small_total[slot], 0.0
        )
        norms = jnp.stack([jnp.sqrt(jnp.sum(weight * weight)), jnp.sqrt(jnp.sum(update * update))])
        fresh = weight - learn_rate * norms[0] / (norms[1] + adam_eps) * update
        outputs = outputs + [fresh, momentum, variance]
        pairs.append(norms)
    outputs = outputs + [jnp.stack(pairs)]
    return tuple(outputs)


def solution(mesh):
    return jax.shard_map(
        body,
        mesh=mesh,
        in_specs=(
            P(("dp", "shard"), None, None),
            P(("dp", "shard"), None, None),
            P(),
            P("dp", "shard"),
            P("dp", "shard"),
            P("dp", "shard"),
            P("dp", "shard"),
            P("dp", "shard"),
            P("dp", "shard"),
            P("dp", "shard"),
            P("dp", "shard"),
            P("dp", "shard"),
            P("dp", "shard"),
            P("dp", "shard"),
            P("dp", "shard"),
            P(),
            P(),
            P(),
            P(),
            P(),
            P(),
            P(),
            P(),
            P(),
            P(),
            P(),
            P(),
        ),
        out_specs=(
            P(("dp", "shard"), None, None),
            P(("dp", "shard"), None, None),
            P("dp", "shard"),
            P("dp", "shard"),
            P("dp", "shard"),
            P("dp", "shard"),
            P("dp", "shard"),
            P("dp", "shard"),
            P("dp", "shard"),
            P("dp", "shard"),
            P("dp", "shard"),
            P("dp", "shard"),
            P("dp", "shard"),
            P("dp", "shard"),
            P("dp", "shard"),
            P("dp", "shard"),
            P("dp", "shard"),
            P("dp", "shard"),
            P(),
            P(),
            P(),
            P(),
            P(),
            P(),
            P(),
            P(),
            P(),
            P(),
            P(),
            P(),
            P(),
        ),
        check_vma=False,
    )
```

```python
import jax
import jax.numpy as jnp
from jax import lax
from jax.experimental import pallas as pl
from jax.experimental.pallas import tpu as pltpu
from jax.sharding import PartitionSpec as P

HD = 32
WIN = 12
STEP = 10
HEADS = 24
GRID = 24
SHIFT = 6


beta_one = 0.9
beta_two = 0.999
adam_eps = 1e-06
decay_rate = 0.01
learn_rate = 0.25
norm_eps = 1e-05
masked_score = -100.0


def layer_norm(values, gain_row, shift_row):
    centred = values - jnp.mean(values, axis=-1, keepdims=True)
    spread = jnp.mean(centred * centred, axis=-1, keepdims=True)
    return centred * lax.rsqrt(spread + norm_eps) * gain_row + shift_row


def gelu_exact(values):
    return jax.nn.gelu(values, approximate=False)


def window_labels(regions):
    return (
        regions.reshape(GRID // WIN, WIN, GRID // WIN, WIN)
        .transpose(0, 2, 1, 3)
        .reshape((GRID // WIN) ** 2, WIN * WIN)
    )


AREA = WIN * WIN
SPAN = 2 * WIN - 1
REACH = 384
TABLE_PAD = 640
HEAD_STEP = 4
CENTRE = (WIN - 1) * SPAN + WIN - 1


def dot00(left, right):
    return lax.dot_general(
        left, right, (((0,), (0,)), ((), ())), preferred_element_type=jnp.float32
    )


def dot11(left, right):
    return lax.dot_general(
        left, right, (((1,), (1,)), ((), ())), preferred_element_type=jnp.float32
    )


def dot10(left, right):
    return lax.dot_general(
        left, right, (((1,), (0,)), ((), ())), preferred_element_type=jnp.float32
    )


def spread_places(shape, table_dim, token_dim):
    token = lax.broadcasted_iota(jnp.int32, shape, token_dim)
    place = lax.broadcasted_iota(jnp.int32, shape, table_dim)
    token_row = token // WIN
    return place == token + (SPAN - WIN) * token_row


def bias_kernel(table_ref, bias_ref):
    spot = spread_places((REACH, AREA), 0, 1).astype(jnp.bfloat16)
    table = table_ref[...]
    for row in range(WIN):
        rolled = []
        for column in range(WIN):
            back = SPAN * (WIN - 1 - row) + WIN - 1 - column
            rolled.append(pltpu.roll(table, (TABLE_PAD - back) % TABLE_PAD, 1)[:, :REACH])
        block = jnp.concatenate(rolled, axis=0)
        high = block.astype(jnp.bfloat16)
        rest = block - high.astype(jnp.float32)
        middle = rest.astype(jnp.bfloat16)
        low = (rest - middle.astype(jnp.float32)).astype(jnp.bfloat16)
        picked = dot10(high, spot) + (dot10(middle, spot) + dot10(low, spot))
        for column in range(WIN):
            bias_ref[row * WIN + column] = picked[column * HEADS : (column + 1) * HEADS]


def table_kernel(scores_ref, table_ref):
    spot = spread_places((AREA, REACH), 1, 0).astype(jnp.bfloat16)
    total = jnp.zeros((HEADS, TABLE_PAD), jnp.float32)
    for row in range(WIN):
        block = scores_ref[row * WIN : (row + 1) * WIN].reshape(WIN * HEADS, AREA)
        high = block.astype(jnp.bfloat16)
        low = (block - high.astype(jnp.float32)).astype(jnp.bfloat16)
        spread = dot10(high, spot) + dot10(low, spot)
        inner = spread[:HEADS]
        for column in range(1, WIN):
            inner = pltpu.roll(inner, 1, 1) + spread[column * HEADS : (column + 1) * HEADS]
        inner = jnp.concatenate(
            [inner, jnp.zeros((HEADS, TABLE_PAD - REACH), jnp.float32)], axis=1
        )
        if row:
            total = pltpu.roll(total, SPAN, 1)
        total = total + inner
    table_ref[...] = total


def table_to_bias(position):
    rows = position.shape[0]
    table = jnp.pad(position.T, ((0, 0), (0, TABLE_PAD - rows)))
    spread = pl.pallas_call(
        bias_kernel,
        out_shape=jax.ShapeDtypeStruct((AREA, HEADS, AREA), jnp.float32),
        name="bias_kernel",
    )(table)
    return spread.transpose(1, 0, 2)


def scores_to_table(scores, rows):
    table = pl.pallas_call(
        table_kernel,
        out_shape=jax.ShapeDtypeStruct((HEADS, TABLE_PAD), jnp.float32),
        name="table_kernel",
    )(scores.transpose(1, 0, 2))
    return table[:, :rows].T


def scores_of(keyed, query, bias, allowed):
    return jnp.where(allowed, dot00(keyed, query) * HD ** (-0.5) + bias, masked_score)


def head_slices(ref, head):
    width = HEADS * HD
    return tuple(
        ref[0, pl.ds(pl.multiple_of(block * width + head * HD, HD), HD), :] for block in range(3)
    )


def forward_kernel(triple_ref, bias_ref, label_ref, column_ref, mixed_ref, log_ref):
    allowed = column_ref[0] == label_ref[0]

    def step(group, carry):
        for member in range(HEAD_STEP):
            head = group * HEAD_STEP + member
            query, keyed, valued = head_slices(triple_ref, head)
            scores = scores_of(keyed, query, bias_ref[head], allowed)
            top = jnp.max(scores, axis=0, keepdims=True)
            raised = jnp.exp(scores - top)
            total = jnp.sum(raised, axis=0, keepdims=True)
            probs = (raised * (1.0 / total)).astype(jnp.bfloat16)
            mixed_ref[0, pl.ds(pl.multiple_of(head * HD, HD), HD), :] = dot10(
                valued, probs
            ).astype(jnp.bfloat16)
            log_ref[0, head] = top + jnp.log(total)
        return carry

    lax.fori_loop(0, HEADS // HEAD_STEP, step, 0)


def backward_kernel(
    triple_ref, grad_ref, log_ref, bias_ref, label_ref, column_ref, out_ref, scores_ref
):
    allowed = column_ref[0] == label_ref[0]
    width = HEADS * HD

    @pl.when(pl.program_id(0) == 0)
    def _():
        scores_ref[...] = jnp.zeros_like(scores_ref)

    def step(group, carry):
        for member in range(HEAD_STEP):
            head = group * HEAD_STEP + member
            query, keyed, valued = head_slices(triple_ref, head)
            grad = grad_ref[0, pl.ds(pl.multiple_of(head * HD, HD), HD), :]
            scores = scores_of(keyed, query, bias_ref[head], allowed)
            probs = jnp.exp(scores - log_ref[0, head])
            grad_probs = dot00(valued, grad)
            weighted = probs * grad_probs
            mean = jnp.sum(weighted, axis=0, keepdims=True)
            grad_scores = jnp.where(allowed, weighted - probs * mean, 0.0)
            scores_ref[head] += grad_scores
            raw = (grad_scores * HD ** (-0.5)).astype(jnp.bfloat16)
            results = (
                dot10(keyed, raw),
                dot11(query, raw),
                dot11(grad, probs.astype(jnp.bfloat16)),
            )
            for block in range(3):
                rows = pl.ds(pl.multiple_of(block * width + head * HD, HD), HD)
                out_ref[0, rows, :] = results[block].astype(jnp.bfloat16)
        return carry

    lax.fori_loop(0, HEADS // HEAD_STEP, step, 0)


def entry_kernel(value_ref, cot_ref, gain_ref, shift_ref, value_out, cot_out, norm_out, turned):
    for source, target in ((cot_ref, cot_out), (value_ref, value_out)):
        for row in range(GRID):
            line = source[0, row * GRID : (row + 1) * GRID, :].astype(jnp.float32)
            line = pltpu.roll(line, GRID - SHIFT, 0)
            place = (row - SHIFT) % GRID
            down, within = place // WIN, place % WIN
            for across in range(GRID // WIN):
                at = (down * (GRID // WIN) + across) * AREA + within * WIN
                turned[at : at + WIN, :] = line[across * WIN : (across + 1) * WIN]
        if source is cot_ref:
            target[...] = turned[...].astype(jnp.bfloat16)

    def step(index, carry):
        at = pl.ds(pl.multiple_of(index * 48, 48), 48)
        values = turned[at, :]
        value_out[at, :] = values.astype(jnp.bfloat16)
        norm_out[at, :] = layer_norm(values, gain_ref[...], shift_ref[...]).astype(jnp.bfloat16)
        return carry

    lax.fori_loop(0, GRID * GRID // 48, step, 0)


def enter(values, cot, gain, shift):
    images, tokens, width = values.shape
    image = pl.BlockSpec((1, tokens, width), lambda index: (index, 0, 0))
    line = pl.BlockSpec((1, width), lambda index: (0, 0))
    rows = pl.BlockSpec((tokens, width), lambda index: (index, 0))
    return pl.pallas_call(
        entry_kernel,
        grid=(images,),
        in_specs=[image, image, line, line],
        out_specs=[rows] * 3,
        out_shape=[jax.ShapeDtypeStruct((images * tokens, width), jnp.bfloat16)] * 3,
        scratch_shapes=[pltpu.VMEM((tokens, width), jnp.float32)],
        name="entry_kernel",
    )(values, cot, gain[None], shift[None])


def exit_kernel(result_ref, grad_ref, result_out, grad_out, turned):
    for source, target in ((result_ref, result_out), (grad_ref, grad_out)):
        turned[...] = source[...].astype(jnp.float32)
        for row in range(GRID):
            place = (row - SHIFT) % GRID
            down, within = place // WIN, place % WIN
            starts = [(down * (GRID // WIN) + across) * AREA + within * WIN for across in range(2)]
            line = jnp.concatenate([turned[at : at + WIN, :] for at in starts], axis=0)
            line = pltpu.roll(line, SHIFT, 0)
            target[0, row * GRID : (row + 1) * GRID, :] = line.astype(target.dtype)


def leave(result, grad, images):
    width = result.shape[1]
    tokens = GRID * GRID
    image = pl.BlockSpec((1, tokens, width), lambda index: (index, 0, 0))
    rows = pl.BlockSpec((tokens, width), lambda index: (index, 0))
    return pl.pallas_call(
        exit_kernel,
        grid=(images,),
        in_specs=[rows] * 2,
        out_specs=[image] * 2,
        out_shape=[
            jax.ShapeDtypeStruct((images, tokens, width), jnp.bfloat16),
            jax.ShapeDtypeStruct((images, tokens, width), jnp.float32),
        ],
        scratch_shapes=[pltpu.VMEM((tokens, width), jnp.float32)],
        name="exit_kernel",
    )(result, grad)


def window_block(rows):
    return pl.BlockSpec((1, rows, AREA), lambda window: (window, 0, 0))


def label_blocks(count):
    return [
        pl.BlockSpec((1, 1, AREA), lambda window: (window % count, 0, 0)),
        pl.BlockSpec((1, AREA, 1), lambda window: (window % count, 0, 0)),
    ]


def attend_forward(triple, bias, labels, shards):
    windows = triple.shape[0]
    width = HEADS * HD
    whole = pl.BlockSpec((HEADS, AREA, AREA), lambda window: (0, 0, 0))
    log_block = pl.BlockSpec((1, HEADS, 1, AREA), lambda window: (window, 0, 0, 0))
    in_specs = [window_block(3 * width), whole] + label_blocks(labels.shape[0])
    out_specs = [window_block(width), log_block]
    out_shape = [
        jax.ShapeDtypeStruct((windows, width, AREA), jnp.bfloat16),
        jax.ShapeDtypeStruct((windows, HEADS, 1, AREA), jnp.float32),
    ]
    arrays = (triple, bias, labels[:, None, :], labels[:, :, None])
    if shards is None:
        return pl.pallas_call(
            forward_kernel,
            grid=(windows,),
            in_specs=in_specs,
            out_specs=out_specs,
            out_shape=out_shape,
            name="forward_kernel",
        )(*arrays)
    anywhere = pl.BlockSpec(memory_space=pl.ANY)
    full_shapes = [(ZS, 2, 2, shard.shape[0], 2 * shard.shape[1]) for shard in shards]
    mixed, log_total, *full = pl.pallas_call(
        forward_riding,
        grid=(windows,),
        in_specs=in_specs + [anywhere] * 3,
        out_specs=out_specs + [anywhere] * 3,
        out_shape=out_shape + [jax.ShapeDtypeStruct(shape, jnp.bfloat16) for shape in full_shapes],
        scratch_shapes=comm_sems(3),
        compiler_params=pltpu.CompilerParams(collective_id=4, has_side_effects=True),
        name="forward_kernel",
    )(*arrays, *shards)
    full = [each.reshape(ZS * 4 * shard.shape[0], -1) for each, shard in zip(full, shards)]
    return mixed, log_total, full


def attend_backward(triple, grad, log_total, bias, labels, grads):
    windows = triple.shape[0]
    width = HEADS * HD
    whole = pl.BlockSpec((HEADS, AREA, AREA), lambda window: (0, 0, 0))
    log_block = pl.BlockSpec((1, HEADS, 1, AREA), lambda window: (window, 0, 0, 0))
    in_specs = [window_block(3 * width), window_block(width), log_block, whole]
    in_specs = in_specs + label_blocks(labels.shape[0])
    out_specs = [window_block(3 * width), whole]
    out_shape = [
        jax.ShapeDtypeStruct((windows, 3 * width, AREA), jnp.bfloat16),
        jax.ShapeDtypeStruct((HEADS, AREA, AREA), jnp.float32),
    ]
    arrays = (triple, grad, log_total, bias, labels[:, None, :], labels[:, :, None])
    if grads is None:
        return pl.pallas_call(
            backward_kernel,
            grid=(windows,),
            in_specs=in_specs,
            out_specs=out_specs,
            out_shape=out_shape,
            name="backward_kernel",
        )(*arrays)
    sizes = [(grad.shape[0] // 16, grad.shape[1]) for grad in grads]
    heights, widths = zip(*sizes)
    out = pl.pallas_call(
        backward_riding,
        grid=(windows,),
        in_specs=in_specs + [pl.BlockSpec(memory_space=pl.ANY)] * 3,
        out_specs=out_specs + [pl.BlockSpec(memory_space=pltpu.VMEM)] * 3,
        out_shape=out_shape
        + [jax.ShapeDtypeStruct((rows, cols // 2), jnp.float32) for rows, cols in sizes],
        scratch_shapes=scatter_scratch(heights, widths) + comm_sems(3),
        compiler_params=pltpu.CompilerParams(
            collective_id=5, has_side_effects=True, vmem_limit_bytes=60 * 2**20
        ),
        name="backward_kernel",
    )(*arrays, *[grad.reshape(ZS, 2, 2, rows, cols) for grad, (rows, cols) in zip(grads, sizes)])
    return out[0], out[1], out[2:]


def product_left(left, right):
    return lax.dot_general(
        left, right, (((0,), (0,)), ((), ())), preferred_element_type=jnp.float32
    )


def product_right(left, right):
    return lax.dot_general(
        left, right, (((1,), (1,)), ((), ())), preferred_element_type=jnp.float32
    )


def whole_step(
    values_low, cot_low, normed_low, full, shards, gains, shifts, biases, bias, labels, rows, scale
):
    attend = full[0]
    width = attend.shape[0]
    hidden_width = biases.shape[0] - 5 * width
    windows = values_low.shape[0] // AREA
    values = values_low.astype(jnp.float32)
    norm_back = jax.vjp(layer_norm, values, gains[0], shifts[0])[1]
    windowed = normed_low.reshape(windows, AREA, width)
    triple = jnp.einsum("wtc,ce->wet", windowed, attend, preferred_element_type=jnp.float32)
    triple = (triple + biases[: 3 * width][None, :, None]).astype(jnp.bfloat16)
    if shards is None:
        mixed, log_total = attend_forward(triple, bias, labels, None)
        project, expand, contract = full[1:]
    else:
        mixed, log_total, (project, expand, contract) = attend_forward(triple, bias, labels, shards)
    branch = (
        jnp.einsum("wct,ce->wte", mixed, project, preferred_element_type=jnp.float32).reshape(
            -1, width
        )
        + biases[3 * width : 4 * width]
    )
    middle = values + branch
    normed_two, norm_two_back = jax.vjp(layer_norm, middle, gains[1], shifts[1])
    normed_two_low = normed_two.astype(jnp.bfloat16)
    hidden = (
        jnp.dot(normed_two_low, expand, preferred_element_type=jnp.float32)
        + biases[4 * width : 4 * width + hidden_width]
    )
    active, gelu_back = jax.vjp(gelu_exact, hidden)
    active_low = active.astype(jnp.bfloat16)
    result = middle + (
        jnp.dot(active_low, contract, preferred_element_type=jnp.float32)
        + biases[4 * width + hidden_width :]
    )
    cot_float = cot_low.astype(jnp.float32)
    grad_contract = product_left(active_low, cot_low)
    grad_bias_contract = jnp.sum(cot_float, axis=0)
    grad_active = product_right(cot_low, contract)
    grad_hidden_low = gelu_back(grad_active)[0].astype(jnp.bfloat16)
    grad_expand = product_left(normed_two_low, grad_hidden_low)
    grad_bias_expand = jnp.sum(grad_hidden_low, axis=0, dtype=jnp.float32)
    grad_normed_two = product_right(grad_hidden_low, expand)
    grad_middle_part, grad_gain_two, grad_shift_two = norm_two_back(grad_normed_two)
    grad_middle = cot_float + grad_middle_part
    grad_branch_low = grad_middle.astype(jnp.bfloat16)
    grad_branch_windows = grad_branch_low.reshape(windows, AREA, width)
    grad_project = jnp.einsum(
        "wct,wte->ce", mixed, grad_branch_windows, preferred_element_type=jnp.float32
    )
    grad_bias_project = jnp.sum(grad_branch_low, axis=0, dtype=jnp.float32)
    grad_mixed = jnp.einsum(
        "wte,ce->wct", grad_branch_windows, project, preferred_element_type=jnp.float32
    ).astype(jnp.bfloat16)
    others = tuple(
        (grad * scale).astype(jnp.bfloat16) for grad in (grad_project, grad_expand, grad_contract)
    )
    if shards is None:
        grad_triple, grad_scores = attend_backward(
            triple, grad_mixed, log_total, bias, labels, None
        )
    else:
        grad_triple, grad_scores, others = attend_backward(
            triple, grad_mixed, log_total, bias, labels, others
        )
    grad_position = scores_to_table(grad_scores, rows)
    grad_attend = jnp.einsum(
        "wtc,wet->ce", windowed, grad_triple, preferred_element_type=jnp.float32
    )
    grad_bias_attend = jnp.sum(grad_triple, axis=(0, 2), dtype=jnp.float32)
    grad_normed = jnp.einsum(
        "wet,ce->wtc", grad_triple, attend, preferred_element_type=jnp.float32
    ).reshape(-1, width)
    grad_input_part, grad_gain_one, grad_shift_one = norm_back(grad_normed)
    grad_input = grad_middle + grad_input_part
    grads = ((grad_attend * scale).astype(jnp.bfloat16),) + tuple(others)
    small = (
        jnp.stack([grad_gain_one, grad_gain_two]),
        jnp.stack([grad_shift_one, grad_shift_two]),
        jnp.concatenate(
            [grad_bias_attend, grad_bias_project, grad_bias_expand, grad_bias_contract]
        ),
        grad_position,
    )
    small = tuple(grad * scale for grad in small)
    return (result.astype(jnp.bfloat16), grad_input, grads, small)


ZS = 4
SPLIT = 2
ATTEND_PARTS = ((0, 0), (0, 1), (0, 2))
OTHER_PARTS = ((0, None), (1, None), (2, None))


def special_mesh(dp_count, shard_count):
    return dp_count == ZS * SPLIT * SPLIT and shard_count == SPLIT


def places():
    at = lax.axis_index("dp")
    return at // 4, lax.rem(at // 2, 2), lax.rem(at, 2), lax.axis_index("shard")


def far_z(z, step):
    return (z, z + 1 - 2 * lax.rem(z, 2), lax.rem(z + 2, 4), 3 - z)[step]


def device(z, y, c, x):
    return {"dp": (z * 2 + y) * 2 + c, "shard": x}


def partners(z, y, c, x):
    return [device(far_z(z, step), y, c, x) for step in (1, 2, 3)] + [
        device(z, y, c, 1 - x),
        device(z, 1 - y, c, x),
        device(z, y, 1 - c, x),
    ]


def greet(devices):
    barrier = pltpu.get_barrier_semaphore()
    for one in devices:
        pl.semaphore_signal(
            barrier, inc=1, device_id=one, device_id_type=pl.DeviceIdType.MESH
        )
    pl.semaphore_wait(barrier, len(devices))


def remote(source, target, sends, receives, slot, where):
    return pltpu.make_async_remote_copy(
        src_ref=source,
        dst_ref=target,
        send_sem=sends.at[slot],
        recv_sem=receives.at[slot],
        device_id=where,
        device_id_type=pl.DeviceIdType.MESH,
    )


def columns_of(ref, x):
    half = ref.shape[-1] // 2
    return pl.ds(pl.multiple_of(x * half, 128), half)


def x_first(parts, step, part):
    lone = 2 if parts is ATTEND_PARTS else 0
    if part == lone:
        return step % 2 == 0
    return part == (0 if parts is ATTEND_PARTS else 1)


class Gather:
    def __init__(self, parts, own, full, sems):
        self.parts, self.own, self.full = parts, own, full
        self.local_sem, self.sends, self.receives = sems
        self.count = len(parts)
        self.at = places()

    def own_part(self, part):
        matrix, piece = self.parts[part]
        return self.own[matrix] if piece is None else self.own[matrix].at[piece]

    def spot(self, part, zi, yi, cols):
        matrix, piece = self.parts[part]
        c = self.at[2]
        if piece is None:
            return self.full[matrix].at[zi, yi, c, :, cols]
        return self.full[matrix].at[zi, yi, c, piece, :, cols]

    def flight(self, phase, step, part):
        z, y, c, x = self.at
        zi = far_z(z, step)
        cols = columns_of(self.full[self.parts[part][0]], x)
        everything = slice(None)
        first = x_first(self.parts, step, part)
        if phase == 0:
            here = self.own_part(part)
            there = self.spot(part, z, y, cols)
            where = device(zi, y, c, x)
        elif phase == 1:
            here = there = self.spot(part, zi, y, cols)
            where = device(z, y, c, 1 - x) if first else device(z, 1 - y, c, x)
        elif phase == 2 and first:
            here = there = self.spot(part, zi, y, everything)
            where = device(z, 1 - y, c, x)
        elif phase == 2:
            here = there = self.spot(part, zi, everything, cols)
            where = device(z, y, c, 1 - x)
        else:
            here = there = self.spot(part, zi, everything, everything)
            where = device(z, y, 1 - c, x)
        slot = (phase * 4 + step) * self.count + part
        return remote(here, there, self.sends, self.receives, slot, where)

    def begin(self):
        z, y, c, x = self.at
        greet(partners(z, y, c, x))
        for step in (1, 2, 3):
            for part in range(self.count):
                self.flight(0, step, part).start()
        copies = []
        for part in range(self.count):
            cols = columns_of(self.full[self.parts[part][0]], x)
            copies.append(
                pltpu.make_async_copy(
                    self.own_part(part), self.spot(part, z, y, cols), self.local_sem.at[part]
                )
            )
        for copy in copies:
            copy.start()
        for copy in copies:
            copy.wait()

    def advance(self, phase, step):
        for part in range(self.count):
            if phase > 1 or step:
                self.flight(phase - 1, step, part).wait_recv()
            self.flight(phase, step, part).start()

    def stage(self, number):
        for phase in (1, 2, 3):
            if 0 <= number - phase + 1 < 4:
                self.advance(phase, number - phase + 1)

    def finish(self):
        for step in range(4):
            for part in range(self.count):
                self.flight(3, step, part).wait_recv()
        for phase in range(4):
            for step in range(0 if phase else 1, 4):
                for part in range(self.count):
                    self.flight(phase, step, part).wait_send()


def comm_sems(count):
    return [
        pltpu.SemaphoreType.DMA((4 * count,)),
        pltpu.SemaphoreType.DMA((16 * count,)),
        pltpu.SemaphoreType.DMA((16 * count,)),
    ]


def gather_kernel(own_ref, full_ref, *sems):
    gather = Gather(ATTEND_PARTS, (own_ref,), (full_ref,), sems)
    gather.begin()
    for number in range(6):
        gather.stage(number)
    gather.finish()


def gather_one(shard):
    rows, half = shard.shape
    anywhere = pl.BlockSpec(memory_space=pl.ANY)
    full = pl.pallas_call(
        gather_kernel,
        in_specs=[anywhere],
        out_specs=anywhere,
        out_shape=jax.ShapeDtypeStruct((ZS, 2, 2, 3, rows // 3, 2 * half), jnp.bfloat16),
        scratch_shapes=comm_sems(len(ATTEND_PARTS)),
        compiler_params=pltpu.CompilerParams(collective_id=0, has_side_effects=True),
        name="gather_kernel",
    )(shard.reshape(3, rows // 3, half))
    return full.reshape(ZS * 4 * rows, 2 * half)


def add_rows(first, second, target):
    rows = target.shape[0]

    def step(index, carry):
        at = pl.ds(pl.multiple_of(index * 16, 16), 16)
        total = first(at).astype(jnp.float32) + second(at).astype(jnp.float32)
        target[at, :] = total.astype(target.dtype)
        return carry

    lax.fori_loop(0, rows // 16, step, 0)


class Scatter:
    order = (3, 2, 1, 0)

    def __init__(self, parts, grads, outs, scratch, sems):
        self.parts, self.grads, self.outs = parts, grads, outs
        self.local_sem, self.sends, self.receives = sems
        self.count = count = len(parts)
        self.at = places()
        self.own = scratch[:count]
        self.core_in = scratch[count : 2 * count]
        self.two_x = scratch[2 * count : 3 * count]
        self.two_y = scratch[3 * count : 4 * count]
        self.three_in = scratch[4 * count : 5 * count]
        self.last = scratch[5 * count : 6 * count]
        self.last_in = scratch[6 * count : 7 * count]

    def block(self, part, zi, ci):
        matrix, piece = self.parts[part]
        ref = self.grads[matrix]
        return ref.at[zi, :, ci] if piece is None else ref.at[zi, :, ci, piece]

    def local(self, step, part):
        z, y, c, x = self.at
        return pltpu.make_async_copy(
            self.block(part, far_z(z, step), c),
            self.own[part].at[step],
            self.local_sem.at[step * self.count + part],
        )

    def flight(self, phase, step, part):
        z, y, c, x = self.at
        own = self.own[part]
        first = x_first(self.parts, step, part)
        across_x, across_y = device(z, y, c, 1 - x), device(z, 1 - y, c, x)
        other_cols = columns_of(own, 1 - x)
        if phase == 0:
            here = self.block(part, far_z(z, step), 1 - c)
            there, where = self.core_in[part].at[step], device(z, y, 1 - c, x)
        elif phase == 1 and first:
            here = own.at[step, :, :, other_cols]
            there, where = self.two_x[part].at[step], across_x
        elif phase == 1:
            here = own.at[step, 1 - y]
            there, where = self.two_y[part].at[step], across_y
        elif phase == 2 and first:
            here = self.two_x[part].at[step, 1 - y]
            there, where = self.three_in[part].at[step], across_y
        elif phase == 2:
            here = self.two_y[part].at[step, :, other_cols]
            there, where = self.three_in[part].at[step], across_x
        else:
            here, there = self.last[part].at[step], self.last_in[part].at[step - 1]
            where = device(far_z(z, step), y, c, x)
        slot = (phase * 4 + step) * self.count + part
        return remote(here, there, self.sends, self.receives, slot, where)

    def begin(self):
        greet(partners(*self.at))
        for step in self.order:
            for part in range(self.count):
                self.flight(0, step, part).start()
                self.local(step, part).start()

    def second(self, step):
        for part in range(self.count):
            self.local(step, part).wait()
            self.flight(0, step, part).wait_recv()
            for yi in range(2):
                mine, other = self.own[part].at[step, yi], self.core_in[part].at[step, yi]
                add_rows(lambda at: mine[at, :], lambda at: other[at, :], mine)
            self.flight(1, step, part).start()

    def third(self, step):
        z, y, c, x = self.at
        for part in range(self.count):
            self.flight(1, step, part).wait_recv()
            if x_first(self.parts, step, part):
                cols = columns_of(self.own[part], x)
                for yi in range(2):
                    mine, other = self.own[part].at[step, yi], self.two_x[part].at[step, yi]
                    add_rows(lambda at: mine[at, cols], lambda at: other[at, :], other)
            else:
                mine, other = self.own[part].at[step, y], self.two_y[part].at[step]
                add_rows(lambda at: mine[at, :], lambda at: other[at, :], other)
            self.flight(2, step, part).start()

    def fourth(self, step):
        z, y, c, x = self.at
        for part in range(self.count):
            self.flight(2, step, part).wait_recv()
            other = self.three_in[part].at[step]
            if x_first(self.parts, step, part):
                mine = self.two_x[part].at[step, y]
                first = lambda at: mine[at, :]
            else:
                mine = self.two_y[part].at[step]
                cols = columns_of(self.own[part], x)
                first = lambda at: mine[at, cols]
            add_rows(first, lambda at: other[at, :], self.last[part].at[step])
            if step:
                self.flight(3, step, part).start()

    def stage(self, number):
        if number < 4:
            self.second(self.order[number])
        if 0 <= number - 1 < 4:
            self.third(self.order[number - 1])
        if 0 <= number - 2 < 4:
            self.fourth(self.order[number - 2])

    def finish(self):
        for part in range(self.count):
            for step in (3, 2, 1):
                self.flight(3, step, part).wait_recv()
            matrix, piece = self.parts[part]
            target = self.outs[matrix] if piece is None else self.outs[matrix].at[piece]
            mine, others = self.last[part].at[0], self.last_in[part]

            def total(index, carry):
                at = pl.ds(pl.multiple_of(index * 16, 16), 16)
                value = mine[at, :].astype(jnp.float32)
                for step in range(3):
                    value = value + others[step, at, :].astype(jnp.float32)
                target[at, :] = value
                return carry

            lax.fori_loop(0, target.shape[0] // 16, total, 0)
        for phase in range(4):
            for step in range(1 if phase == 3 else 0, 4):
                for part in range(self.count):
                    self.flight(phase, step, part).wait_send()


def scatter_scratch(heights, widths):
    low = jnp.bfloat16
    sizes = list(zip(heights, widths))
    return (
        [pltpu.VMEM((4, 2, h, w), low) for h, w in sizes]
        + [pltpu.VMEM((4, 2, h, w), low) for h, w in sizes]
        + [pltpu.VMEM((4, 2, h, w // 2), low) for h, w in sizes]
        + [pltpu.VMEM((4, h, w), low) for h, w in sizes]
        + [pltpu.VMEM((4, h, w // 2), low) for h, w in sizes]
        + [pltpu.VMEM((4, h, w // 2), low) for h, w in sizes]
        + [pltpu.VMEM((3, h, w // 2), low) for h, w in sizes]
    )


def scatter_kernel(grad_ref, out_ref, *rest):
    scatter = Scatter(ATTEND_PARTS, (grad_ref,), (out_ref,), rest[:-3], rest[-3:])
    scatter.begin()
    for number in range(6):
        scatter.stage(number)
    scatter.finish()


def scatter_one(grad):
    rows, cols = grad.shape[0] // 16, grad.shape[1]
    count = len(ATTEND_PARTS)
    out = pl.pallas_call(
        scatter_kernel,
        in_specs=[pl.BlockSpec(memory_space=pl.ANY)],
        out_specs=pl.BlockSpec(memory_space=pltpu.VMEM),
        out_shape=jax.ShapeDtypeStruct((3, rows // 3, cols // 2), jnp.float32),
        scratch_shapes=scatter_scratch([rows // 3] * count, [cols] * count) + comm_sems(count),
        compiler_params=pltpu.CompilerParams(
            collective_id=1, has_side_effects=True, vmem_limit_bytes=40 * 2**20
        ),
        name="scatter_kernel",
    )(grad.reshape(ZS, 2, 2, 3, rows // 3, cols))
    return out.reshape(rows, cols // 2)


def at_steps(actions):
    for number, action in actions:
        pl.when(pl.program_id(0) == number)(action)


def forward_riding(triple_ref, bias_ref, label_ref, column_ref, *rest):
    gather = Gather(OTHER_PARTS, rest[:3], rest[5:8], rest[8:])

    def start():
        gather.begin()
        gather.stage(0)

    at_steps(
        [(0, start)] + [(number, lambda number=number: gather.stage(number)) for number in range(1, 6)]
    )
    forward_kernel(triple_ref, bias_ref, label_ref, column_ref, rest[3], rest[4])
    at_steps([(pl.num_programs(0) - 1, gather.finish)])


def backward_riding(
    triple_ref, grad_ref, log_ref, bias_ref, label_ref, column_ref, *rest
):
    scatter = Scatter(OTHER_PARTS, rest[:3], rest[5:8], rest[8:-3], rest[-3:])
    at_steps(
        [(0, scatter.begin)]
        + [(number + 1, lambda number=number: scatter.stage(number)) for number in range(6)]
    )
    backward_kernel(
        triple_ref, grad_ref, log_ref, bias_ref, label_ref, column_ref, rest[3], rest[4]
    )
    at_steps([(pl.num_programs(0) - 1, scatter.finish)])


def sum_kernel(value_ref, out_ref, incoming, sends, receives):
    z, y, c, x = places()
    hops = [
        device(z, y, 1 - c, x),
        device(z, y, c, 1 - x),
        device(z, 1 - y, c, x),
        device(far_z(z, 1), y, c, x),
        device(far_z(z, 2), y, c, x),
    ]
    greet(hops)
    source = value_ref
    for hop in range(5):
        copy = remote(source, incoming.at[hop], sends, receives, hop, hops[hop])
        copy.start()
        copy.wait()
        out_ref[...] = source[...] + incoming[hop]
        source = out_ref


def sum_all(value, name):
    return pl.pallas_call(
        sum_kernel,
        in_specs=[pl.BlockSpec(memory_space=pltpu.VMEM)],
        out_specs=pl.BlockSpec(memory_space=pltpu.VMEM),
        out_shape=jax.ShapeDtypeStruct(value.shape, jnp.float32),
        scratch_shapes=[
            pltpu.VMEM((5,) + value.shape, jnp.float32),
            pltpu.SemaphoreType.DMA((5,)),
            pltpu.SemaphoreType.DMA((5,)),
        ],
        compiler_params=pltpu.CompilerParams(collective_id=name, has_side_effects=True),
        name="sum_kernel",
    )(value)


def sum_small(arrays):
    sizes = [array.size for array in arrays]
    total = sum(sizes)
    rows = -(-total // 1024) * 8
    flat = jnp.concatenate([array.reshape(-1) for array in arrays])
    summed = sum_all(jnp.pad(flat, (0, rows * 128 - total)).reshape(rows, 128), 2).reshape(-1)
    outs = []
    at = 0
    for array, size in zip(arrays, sizes):
        outs.append(summed[at : at + size].reshape(array.shape))
        at += size
    return tuple(outs)


def sum_squares(value):
    wide = jnp.pad(value.reshape(-1), (0, 1024 - value.size)).reshape(8, 128)
    return sum_all(wide, 3).reshape(-1)[: value.size].reshape(value.shape)


def moments(weight, first, second, gradient, decay):
    momentum = beta_one * first + (1.0 - beta_one) * gradient
    variance = beta_two * second + (1.0 - beta_two) * gradient * gradient
    ratio = (
        momentum / (1.0 - beta_one**STEP) / (jnp.sqrt(variance / (1.0 - beta_two**STEP)) + adam_eps)
    )
    return (momentum, variance, ratio + decay * weight)


def body(
    inputs,
    cotangent,
    regions,
    attend,
    attend_first,
    attend_second,
    project,
    project_first,
    project_second,
    expand,
    expand_first,
    expand_second,
    contract,
    contract_first,
    contract_second,
    gains,
    gains_first,
    gains_second,
    shifts,
    shifts_first,
    shifts_second,
    biases,
    biases_first,
    biases_second,
    position,
    position_first,
    position_second,
):
    masters = (attend, project, expand, contract, gains, shifts, biases, position)
    firsts = (
        attend_first,
        project_first,
        expand_first,
        contract_first,
        gains_first,
        shifts_first,
        biases_first,
        position_first,
    )
    seconds = (
        attend_second,
        project_second,
        expand_second,
        contract_second,
        gains_second,
        shifts_second,
        biases_second,
        position_second,
    )
    dp_count = lax.axis_size("dp")
    shard_count = lax.axis_size("shard")
    tokens_all = inputs.shape[0] * inputs.shape[1] * dp_count * shard_count
    special = special_mesh(dp_count, shard_count)
    shards = tuple(master.astype(jnp.bfloat16) for master in masters[:4])
    if special:
        full = (gather_one(shards[0]),)
    else:
        halves = [lax.all_gather(shard, "dp", axis=0, tiled=True) for shard in shards]
        full = tuple(lax.all_gather(half, "shard", axis=1, tiled=True) for half in halves)
    labels = window_labels(regions)
    bias = table_to_bias(position)
    images = inputs.shape[0]
    values_low, cot_low, normed_low = enter(inputs, cotangent, gains[0], shifts[0])
    result_low, grad_input, grads, small_grads = whole_step(
        values_low,
        cot_low,
        normed_low,
        full,
        shards[1:] if special else None,
        gains,
        shifts,
        biases,
        bias,
        labels,
        position.shape[0],
        1.0 / tokens_all,
    )
    result_low, grad_input = leave(result_low, grad_input, images)
    if special:
        small_total = sum_small(small_grads)
        owned = (scatter_one(grads[0]),) + tuple(grads[1:])
    else:
        small_total = lax.psum(small_grads, ("dp", "shard"))
        columns = [
            lax.psum_scatter(grad, "shard", scatter_dimension=1, tiled=True).astype(jnp.float32)
            for grad in grads
        ]
        owned = tuple(
            lax.psum_scatter(column, "dp", scatter_dimension=0, tiled=True) for column in columns
        )
    pieces = [
        moments(masters[slot], firsts[slot], seconds[slot], owned[slot], decay_rate)
        for slot in range(4)
    ]
    partial_value = jnp.stack(
        [
            jnp.stack(
                [jnp.sum(masters[slot] * masters[slot]), jnp.sum(pieces[slot][2] * pieces[slot][2])]
            )
            for slot in range(4)
        ]
    )
    if special:
        squares = sum_squares(partial_value)
    else:
        squares = lax.psum(partial_value, ("dp", "shard"))
    matrix_norms = jnp.sqrt(squares)
    outputs = [result_low, grad_input]
    pairs = []
    for slot in range(4):
        momentum, variance, update = pieces[slot]
        fresh = (
            masters[slot]
            - learn_rate * matrix_norms[slot, 0] / (matrix_norms[slot, 1] + adam_eps) * update
        )
        outputs = outputs + [fresh, momentum, variance, fresh.astype(jnp.bfloat16)]
        pairs.append(matrix_norms[slot])
    for slot in range(4):
        weight = masters[4 + slot]
        momentum, variance, update = moments(
            weight, firsts[4 + slot], seconds[4 + slot], small_total[slot], 0.0
        )
        norms = jnp.stack([jnp.sqrt(jnp.sum(weight * weight)), jnp.sqrt(jnp.sum(update * update))])
        fresh = weight - learn_rate * norms[0] / (norms[1] + adam_eps) * update
        outputs = outputs + [fresh, momentum, variance]
        pairs.append(norms)
    outputs = outputs + [jnp.stack(pairs)]
    return tuple(outputs)


def solution(mesh):
    return jax.shard_map(
        body,
        mesh=mesh,
        in_specs=(
            P(("dp", "shard"), None, None),
            P(("dp", "shard"), None, None),
            P(),
            P("dp", "shard"),
            P("dp", "shard"),
            P("dp", "shard"),
            P("dp", "shard"),
            P("dp", "shard"),
            P("dp", "shard"),
            P("dp", "shard"),
            P("dp", "shard"),
            P("dp", "shard"),
            P("dp", "shard"),
            P("dp", "shard"),
            P("dp", "shard"),
            P(),
            P(),
            P(),
            P(),
            P(),
            P(),
            P(),
            P(),
            P(),
            P(),
            P(),
            P(),
        ),
        out_specs=(
            P(("dp", "shard"), None, None),
            P(("dp", "shard"), None, None),
            P("dp", "shard"),
            P("dp", "shard"),
            P("dp", "shard"),
            P("dp", "shard"),
            P("dp", "shard"),
            P("dp", "shard"),
            P("dp", "shard"),
            P("dp", "shard"),
            P("dp", "shard"),
            P("dp", "shard"),
            P("dp", "shard"),
            P("dp", "shard"),
            P("dp", "shard"),
            P("dp", "shard"),
            P("dp", "shard"),
            P("dp", "shard"),
            P(),
            P(),
            P(),
            P(),
            P(),
            P(),
            P(),
            P(),
            P(),
            P(),
            P(),
            P(),
            P(),
        ),
        check_vma=False,
    )
```

```python
import functools

import jax
import jax.numpy as jnp
from jax import lax
from jax.experimental import pallas as pl
from jax.experimental.pallas import tpu as pltpu
from jax.sharding import PartitionSpec as P

HD = 32
WIN = 12
STEP = 10
HEADS = 24
GRID = 24
SHIFT = 6


beta_one = 0.9
beta_two = 0.999
adam_eps = 1e-06
decay_rate = 0.01
learn_rate = 0.25
norm_eps = 1e-05
masked_score = -100.0


def layer_norm(values, gain_row, shift_row):
    centred = values - jnp.mean(values, axis=-1, keepdims=True)
    spread = jnp.mean(centred * centred, axis=-1, keepdims=True)
    return centred * lax.rsqrt(spread + norm_eps) * gain_row + shift_row


def window_labels(regions):
    return (
        regions.reshape(GRID // WIN, WIN, GRID // WIN, WIN)
        .transpose(0, 2, 1, 3)
        .reshape((GRID // WIN) ** 2, WIN * WIN)
    )


AREA = WIN * WIN
SPAN = 2 * WIN - 1
REACH = 384
TABLE_PAD = 640
HEAD_STEP = 4
CENTRE = (WIN - 1) * SPAN + WIN - 1


def dot00(left, right):
    return lax.dot_general(
        left, right, (((0,), (0,)), ((), ())), preferred_element_type=jnp.float32
    )


def dot11(left, right):
    return lax.dot_general(
        left, right, (((1,), (1,)), ((), ())), preferred_element_type=jnp.float32
    )


def dot10(left, right):
    return lax.dot_general(
        left, right, (((1,), (0,)), ((), ())), preferred_element_type=jnp.float32
    )


def spread_places(shape, table_dim, token_dim):
    token = lax.broadcasted_iota(jnp.int32, shape, token_dim)
    place = lax.broadcasted_iota(jnp.int32, shape, table_dim)
    token_row = token // WIN
    return place == token + (SPAN - WIN) * token_row


def bias_kernel(table_ref, bias_ref):
    spot = spread_places((REACH, AREA), 0, 1).astype(jnp.bfloat16)
    table = table_ref[...]
    for row in range(WIN):
        rolled = []
        for column in range(WIN):
            back = SPAN * (WIN - 1 - row) + WIN - 1 - column
            rolled.append(pltpu.roll(table, (TABLE_PAD - back) % TABLE_PAD, 1)[:, :REACH])
        block = jnp.concatenate(rolled, axis=0)
        high = block.astype(jnp.bfloat16)
        rest = block - high.astype(jnp.float32)
        middle = rest.astype(jnp.bfloat16)
        low = (rest - middle.astype(jnp.float32)).astype(jnp.bfloat16)
        picked = dot10(high, spot) + (dot10(middle, spot) + dot10(low, spot))
        for column in range(WIN):
            bias_ref[row * WIN + column] = picked[column * HEADS : (column + 1) * HEADS]


def table_kernel(scores_ref, table_ref):
    spot = spread_places((AREA, REACH), 1, 0).astype(jnp.bfloat16)
    total = jnp.zeros((HEADS, TABLE_PAD), jnp.float32)
    for row in range(WIN):
        block = scores_ref[row * WIN : (row + 1) * WIN].reshape(WIN * HEADS, AREA)
        high = block.astype(jnp.bfloat16)
        low = (block - high.astype(jnp.float32)).astype(jnp.bfloat16)
        spread = dot10(high, spot) + dot10(low, spot)
        inner = spread[:HEADS]
        for column in range(1, WIN):
            inner = pltpu.roll(inner, 1, 1) + spread[column * HEADS : (column + 1) * HEADS]
        inner = jnp.concatenate(
            [inner, jnp.zeros((HEADS, TABLE_PAD - REACH), jnp.float32)], axis=1
        )
        if row:
            total = pltpu.roll(total, SPAN, 1)
        total = total + inner
    table_ref[...] = total


def table_to_bias(position):
    rows = position.shape[0]
    table = jnp.pad(position.T, ((0, 0), (0, TABLE_PAD - rows)))
    spread = pl.pallas_call(
        bias_kernel,
        out_shape=jax.ShapeDtypeStruct((AREA, HEADS, AREA), jnp.float32),
        name="bias_kernel",
    )(table)
    return spread.transpose(1, 0, 2)


def scores_to_table(scores, rows):
    table = pl.pallas_call(
        table_kernel,
        out_shape=jax.ShapeDtypeStruct((HEADS, TABLE_PAD), jnp.float32),
        name="table_kernel",
    )(scores.transpose(1, 0, 2))
    return table[:, :rows].T


def scores_of(keyed, query, bias, allowed):
    return jnp.where(allowed, dot00(keyed, query) * HD ** (-0.5) + bias, masked_score)


def head_slices(ref, head):
    width = HEADS * HD
    return tuple(
        ref[0, pl.ds(pl.multiple_of(block * width + head * HD, HD), HD), :] for block in range(3)
    )


def forward_kernel(triple_ref, bias_ref, label_ref, column_ref, mixed_ref, log_ref):
    allowed = column_ref[0] == label_ref[0]

    def step(group, carry):
        for member in range(HEAD_STEP):
            head = group * HEAD_STEP + member
            query, keyed, valued = head_slices(triple_ref, head)
            scores = scores_of(keyed, query, bias_ref[head], allowed)
            top = jnp.max(scores, axis=0, keepdims=True)
            raised = jnp.exp(scores - top)
            total = jnp.sum(raised, axis=0, keepdims=True)
            probs = (raised * (1.0 / total)).astype(jnp.bfloat16)
            mixed_ref[0, pl.ds(pl.multiple_of(head * HD, HD), HD), :] = dot10(
                valued, probs
            ).astype(jnp.bfloat16)
            log_ref[0, head] = top + jnp.log(total)
        return carry

    lax.fori_loop(0, HEADS // HEAD_STEP, step, 0)


def backward_kernel(
    triple_ref, grad_ref, log_ref, bias_ref, label_ref, column_ref, out_ref, scores_ref
):
    allowed = column_ref[0] == label_ref[0]
    width = HEADS * HD

    @pl.when(pl.program_id(0) == 0)
    def _():
        scores_ref[...] = jnp.zeros_like(scores_ref)

    def step(group, carry):
        for member in range(HEAD_STEP):
            head = group * HEAD_STEP + member
            query, keyed, valued = head_slices(triple_ref, head)
            grad = grad_ref[0, pl.ds(pl.multiple_of(head * HD, HD), HD), :]
            scores = scores_of(keyed, query, bias_ref[head], allowed)
            probs = jnp.exp(scores - log_ref[0, head])
            grad_probs = dot00(valued, grad)
            weighted = probs * grad_probs
            mean = jnp.sum(weighted, axis=0, keepdims=True)
            grad_scores = jnp.where(allowed, weighted - probs * mean, 0.0)
            scores_ref[head] += grad_scores
            raw = (grad_scores * HD ** (-0.5)).astype(jnp.bfloat16)
            results = (
                dot10(keyed, raw),
                dot11(query, raw),
                dot11(grad, probs.astype(jnp.bfloat16)),
            )
            for block in range(3):
                rows = pl.ds(pl.multiple_of(block * width + head * HD, HD), HD)
                out_ref[0, rows, :] = results[block].astype(jnp.bfloat16)
        return carry

    lax.fori_loop(0, HEADS // HEAD_STEP, step, 0)


def entry_kernel(value_ref, cot_ref, gain_ref, shift_ref, value_out, cot_out, norm_out, turned):
    for source, target in ((cot_ref, cot_out), (value_ref, value_out)):
        for row in range(GRID):
            line = source[0, row * GRID : (row + 1) * GRID, :].astype(jnp.float32)
            line = pltpu.roll(line, GRID - SHIFT, 0)
            place = (row - SHIFT) % GRID
            down, within = place // WIN, place % WIN
            for across in range(GRID // WIN):
                at = (down * (GRID // WIN) + across) * AREA + within * WIN
                turned[at : at + WIN, :] = line[across * WIN : (across + 1) * WIN]
        if source is cot_ref:
            target[...] = turned[...].astype(jnp.bfloat16)

    def step(index, carry):
        at = pl.ds(pl.multiple_of(index * 48, 48), 48)
        values = turned[at, :]
        value_out[at, :] = values.astype(jnp.bfloat16)
        norm_out[at, :] = layer_norm(values, gain_ref[...], shift_ref[...]).astype(jnp.bfloat16)
        return carry

    lax.fori_loop(0, GRID * GRID // 48, step, 0)


def enter(values, cot, gain, shift):
    images, tokens, width = values.shape
    image = pl.BlockSpec((1, tokens, width), lambda index: (index, 0, 0))
    line = pl.BlockSpec((1, width), lambda index: (0, 0))
    rows = pl.BlockSpec((tokens, width), lambda index: (index, 0))
    return pl.pallas_call(
        entry_kernel,
        grid=(images,),
        in_specs=[image, image, line, line],
        out_specs=[rows] * 3,
        out_shape=[jax.ShapeDtypeStruct((images * tokens, width), jnp.bfloat16)] * 3,
        scratch_shapes=[pltpu.VMEM((tokens, width), jnp.float32)],
        name="entry_kernel",
    )(values, cot, gain[None], shift[None])


def exit_kernel(result_ref, grad_ref, result_out, grad_out, turned):
    for source, target in ((result_ref, result_out), (grad_ref, grad_out)):
        turned[...] = source[...].astype(jnp.float32)
        for row in range(GRID):
            place = (row - SHIFT) % GRID
            down, within = place // WIN, place % WIN
            starts = [(down * (GRID // WIN) + across) * AREA + within * WIN for across in range(2)]
            line = jnp.concatenate([turned[at : at + WIN, :] for at in starts], axis=0)
            line = pltpu.roll(line, SHIFT, 0)
            target[0, row * GRID : (row + 1) * GRID, :] = line.astype(target.dtype)


def leave(result, grad, images):
    width = result.shape[1]
    tokens = GRID * GRID
    image = pl.BlockSpec((1, tokens, width), lambda index: (index, 0, 0))
    rows = pl.BlockSpec((tokens, width), lambda index: (index, 0))
    return pl.pallas_call(
        exit_kernel,
        grid=(images,),
        in_specs=[rows] * 2,
        out_specs=[image] * 2,
        out_shape=[
            jax.ShapeDtypeStruct((images, tokens, width), jnp.bfloat16),
            jax.ShapeDtypeStruct((images, tokens, width), jnp.float32),
        ],
        scratch_shapes=[pltpu.VMEM((tokens, width), jnp.float32)],
        name="exit_kernel",
    )(result, grad)


def window_block(rows):
    return pl.BlockSpec((1, rows, AREA), lambda window: (window, 0, 0))


def label_blocks(count):
    return [
        pl.BlockSpec((1, 1, AREA), lambda window: (window % count, 0, 0)),
        pl.BlockSpec((1, AREA, 1), lambda window: (window % count, 0, 0)),
    ]


def attend_forward(triple, bias, labels, shards):
    windows = triple.shape[0]
    width = HEADS * HD
    whole = pl.BlockSpec((HEADS, AREA, AREA), lambda window: (0, 0, 0))
    log_block = pl.BlockSpec((1, HEADS, 1, AREA), lambda window: (window, 0, 0, 0))
    in_specs = [window_block(3 * width), whole] + label_blocks(labels.shape[0])
    out_specs = [window_block(width), log_block]
    out_shape = [
        jax.ShapeDtypeStruct((windows, width, AREA), jnp.bfloat16),
        jax.ShapeDtypeStruct((windows, HEADS, 1, AREA), jnp.float32),
    ]
    arrays = (triple, bias, labels[:, None, :], labels[:, :, None])
    if shards is None:
        return pl.pallas_call(
            forward_kernel,
            grid=(windows,),
            in_specs=in_specs,
            out_specs=out_specs,
            out_shape=out_shape,
            name="forward_kernel",
        )(*arrays)
    anywhere = pl.BlockSpec(memory_space=pl.ANY)
    full_shapes = [(ZS, 2, 2, shard.shape[0], 2 * shard.shape[1]) for shard in shards]
    mixed, log_total, *full = pl.pallas_call(
        forward_riding,
        grid=(windows,),
        in_specs=in_specs + [anywhere] * 3,
        out_specs=out_specs + [anywhere] * 3,
        out_shape=out_shape + [jax.ShapeDtypeStruct(shape, jnp.bfloat16) for shape in full_shapes],
        scratch_shapes=comm_sems(3),
        compiler_params=pltpu.CompilerParams(collective_id=4, has_side_effects=True),
        name="forward_kernel",
    )(*arrays, *shards)
    full = [each.reshape(ZS * 4 * shard.shape[0], -1) for each, shard in zip(full, shards)]
    return mixed, log_total, full


def attend_backward(triple, grad, log_total, bias, labels, grads):
    windows = triple.shape[0]
    width = HEADS * HD
    whole = pl.BlockSpec((HEADS, AREA, AREA), lambda window: (0, 0, 0))
    log_block = pl.BlockSpec((1, HEADS, 1, AREA), lambda window: (window, 0, 0, 0))
    in_specs = [window_block(3 * width), window_block(width), log_block, whole]
    in_specs = in_specs + label_blocks(labels.shape[0])
    out_specs = [window_block(3 * width), whole]
    out_shape = [
        jax.ShapeDtypeStruct((windows, 3 * width, AREA), jnp.bfloat16),
        jax.ShapeDtypeStruct((HEADS, AREA, AREA), jnp.float32),
    ]
    arrays = (triple, grad, log_total, bias, labels[:, None, :], labels[:, :, None])
    if grads is None:
        return pl.pallas_call(
            backward_kernel,
            grid=(windows,),
            in_specs=in_specs,
            out_specs=out_specs,
            out_shape=out_shape,
            name="backward_kernel",
        )(*arrays)
    sizes = [(grad.shape[0] // 16, grad.shape[1]) for grad in grads]
    heights, widths = zip(*sizes)
    out = pl.pallas_call(
        backward_riding,
        grid=(windows,),
        in_specs=in_specs + [pl.BlockSpec(memory_space=pl.ANY)] * 3,
        out_specs=out_specs + [pl.BlockSpec(memory_space=pltpu.VMEM)] * 3,
        out_shape=out_shape
        + [jax.ShapeDtypeStruct((rows, cols // 2), jnp.float32) for rows, cols in sizes],
        scratch_shapes=scatter_scratch(heights, widths) + comm_sems(3),
        compiler_params=pltpu.CompilerParams(
            collective_id=5, has_side_effects=True, vmem_limit_bytes=60 * 2**20
        ),
        name="backward_kernel",
    )(*arrays, *[grad.reshape(ZS, 2, 2, rows, cols) for grad, (rows, cols) in zip(grads, sizes)])
    return out[0], out[1], out[2:]


FEED_TILE = 512
FEED_ROWS = 192


def feed_kernel(
    scale,
    norm_ref,
    turned_ref,
    cot_ref,
    middle_ref,
    expand_ref,
    contract_ref,
    bias_in_ref,
    bias_out_ref,
    result_ref,
    back_ref,
    grad_contract_ref,
    grad_expand_ref,
    grad_bias_ref,
    total,
    active_all,
    grad_all,
):
    tile = pl.program_id(0)
    rows = norm_ref.shape[0]

    @pl.when(tile == 0)
    def _():
        back_ref[...] = jnp.zeros_like(back_ref)
        total[...] = middle_ref[...] + bias_out_ref[...]

    def step(index, carry):
        for member in range(2):
            at = pl.ds(pl.multiple_of((index * 2 + member) * FEED_ROWS, FEED_ROWS), FEED_ROWS)
            hidden = dot10(norm_ref[at, :], expand_ref[...]) + bias_in_ref[...]
            grad_active = dot11(cot_ref[at, :], contract_ref[...])
            share = 0.5 + 0.5 * lax.erf(hidden * 0.5**0.5)
            bell = jnp.exp(-0.5 * hidden * hidden) * 0.3989422804014327
            active = (hidden * share).astype(jnp.bfloat16)
            grad_hidden = grad_active * (share + hidden * bell)
            grad_low = grad_hidden.astype(jnp.bfloat16)
            active_all[at, :] = active
            grad_all[at, :] = grad_low
            total[at, :] += dot10(active, contract_ref[...])
            back_ref[at, :] += dot11(grad_low, expand_ref[...])
            carry = carry + jnp.sum(
                grad_low.astype(jnp.float32).reshape(FEED_ROWS // 8, 8, FEED_TILE), axis=0
            )
        return carry

    sums = lax.fori_loop(
        0, rows // (2 * FEED_ROWS), step, jnp.zeros((8, FEED_TILE), jnp.float32)
    )
    grad_bias_ref[...] = jnp.sum(sums, axis=0, keepdims=True)
    grad_contract_ref[...] = (dot00(active_all[...], cot_ref[...]) * scale).astype(jnp.bfloat16)
    grad_expand_ref[...] = (dot10(turned_ref[...], grad_all[...]) * scale).astype(jnp.bfloat16)

    @pl.when(tile == pl.num_programs(0) - 1)
    def _():
        result_ref[...] = total[...].astype(jnp.bfloat16)


def feed(norm, cot, middle, expand, contract, bias_in, bias_out, scale):
    rows, width = norm.shape
    hidden = expand.shape[1]
    whole = pl.BlockSpec((rows, width), lambda tile: (0, 0))
    turned = pl.BlockSpec((width, rows), lambda tile: (0, 0))
    wide = pl.BlockSpec((width, FEED_TILE), lambda tile: (0, tile))
    tall = pl.BlockSpec((FEED_TILE, width), lambda tile: (tile, 0))
    line = pl.BlockSpec((1, FEED_TILE), lambda tile: (0, tile))
    out_line = pl.BlockSpec((1, width), lambda tile: (0, 0))
    return pl.pallas_call(
        functools.partial(feed_kernel, scale),
        grid=(hidden // FEED_TILE,),
        in_specs=[whole, turned, whole, whole, wide, tall, line, out_line],
        out_specs=[whole, whole, tall, wide, line],
        out_shape=[
            jax.ShapeDtypeStruct((rows, width), jnp.bfloat16),
            jax.ShapeDtypeStruct((rows, width), jnp.float32),
            jax.ShapeDtypeStruct((hidden, width), jnp.bfloat16),
            jax.ShapeDtypeStruct((width, hidden), jnp.bfloat16),
            jax.ShapeDtypeStruct((1, hidden), jnp.float32),
        ],
        scratch_shapes=[
            pltpu.VMEM((rows, width), jnp.float32),
            pltpu.VMEM((rows, FEED_TILE), jnp.bfloat16),
            pltpu.VMEM((rows, FEED_TILE), jnp.bfloat16),
        ],
        compiler_params=pltpu.CompilerParams(vmem_limit_bytes=56 * 2**20),
        name="feed_kernel",
    )(norm, norm.T, cot, middle, expand, contract, bias_in[None], bias_out[None])


def whole_step(
    values_low, cot_low, normed_low, full, shards, gains, shifts, biases, bias, labels, rows, scale
):
    attend = full[0]
    width = attend.shape[0]
    hidden_width = biases.shape[0] - 5 * width
    windows = values_low.shape[0] // AREA
    values = values_low.astype(jnp.float32)
    norm_back = jax.vjp(layer_norm, values, gains[0], shifts[0])[1]
    windowed = normed_low.reshape(windows, AREA, width)
    triple = jnp.einsum("wtc,ce->wet", windowed, attend, preferred_element_type=jnp.float32)
    triple = (triple + biases[: 3 * width][None, :, None]).astype(jnp.bfloat16)
    if shards is None:
        mixed, log_total = attend_forward(triple, bias, labels, None)
        project, expand, contract = full[1:]
    else:
        mixed, log_total, (project, expand, contract) = attend_forward(triple, bias, labels, shards)
    branch = (
        jnp.einsum("wct,ce->wte", mixed, project, preferred_element_type=jnp.float32).reshape(
            -1, width
        )
        + biases[3 * width : 4 * width]
    )
    middle = values + branch
    normed_two, norm_two_back = jax.vjp(layer_norm, middle, gains[1], shifts[1])
    normed_two_low = normed_two.astype(jnp.bfloat16)
    cot_float = cot_low.astype(jnp.float32)
    grad_bias_contract = jnp.sum(cot_float, axis=0)
    result, grad_normed_two, grad_contract, grad_expand, grad_bias_expand = feed(
        normed_two_low,
        cot_low,
        middle,
        expand,
        contract,
        biases[4 * width : 4 * width + hidden_width],
        biases[4 * width + hidden_width :],
        scale,
    )
    grad_middle_part, grad_gain_two, grad_shift_two = norm_two_back(grad_normed_two)
    grad_middle = cot_float + grad_middle_part
    grad_branch_low = grad_middle.astype(jnp.bfloat16)
    grad_branch_windows = grad_branch_low.reshape(windows, AREA, width)
    grad_project = jnp.einsum(
        "wct,wte->ce", mixed, grad_branch_windows, preferred_element_type=jnp.float32
    )
    grad_bias_project = jnp.sum(grad_branch_low, axis=0, dtype=jnp.float32)
    grad_mixed = jnp.einsum(
        "wte,ce->wct", grad_branch_windows, project, preferred_element_type=jnp.float32
    ).astype(jnp.bfloat16)
    others = ((grad_project * scale).astype(jnp.bfloat16), grad_expand, grad_contract)
    if shards is None:
        grad_triple, grad_scores = attend_backward(
            triple, grad_mixed, log_total, bias, labels, None
        )
    else:
        grad_triple, grad_scores, others = attend_backward(
            triple, grad_mixed, log_total, bias, labels, others
        )
    grad_position = scores_to_table(grad_scores, rows)
    grad_attend = jnp.einsum(
        "wtc,wet->ce", windowed, grad_triple, preferred_element_type=jnp.float32
    )
    grad_bias_attend = jnp.sum(grad_triple, axis=(0, 2), dtype=jnp.float32)
    grad_normed = jnp.einsum(
        "wet,ce->wtc", grad_triple, attend, preferred_element_type=jnp.float32
    ).reshape(-1, width)
    grad_input_part, grad_gain_one, grad_shift_one = norm_back(grad_normed)
    grad_input = grad_middle + grad_input_part
    grads = ((grad_attend * scale).astype(jnp.bfloat16),) + tuple(others)
    small = (
        (grad_gain_one, grad_gain_two, grad_shift_one, grad_shift_two),
        (grad_bias_attend, grad_bias_project, grad_bias_expand[0], grad_bias_contract),
        grad_position,
    )
    return (result, grad_input, grads, small)


ZS = 4
SPLIT = 2
ATTEND_PARTS = ((0, 0), (0, 1), (0, 2))
OTHER_PARTS = ((0, None), (1, None), (2, None))


def special_mesh(dp_count, shard_count):
    return dp_count == ZS * SPLIT * SPLIT and shard_count == SPLIT


def places():
    at = lax.axis_index("dp")
    return at // 4, lax.rem(at // 2, 2), lax.rem(at, 2), lax.axis_index("shard")


def far_z(z, step):
    return (z, z + 1 - 2 * lax.rem(z, 2), lax.rem(z + 2, 4), 3 - z)[step]


def device(z, y, c, x):
    return {"dp": (z * 2 + y) * 2 + c, "shard": x}


def partners(z, y, c, x):
    return [device(far_z(z, step), y, c, x) for step in (1, 2, 3)] + [
        device(z, y, c, 1 - x),
        device(z, 1 - y, c, x),
        device(z, y, 1 - c, x),
    ]


def greet(devices):
    barrier = pltpu.get_barrier_semaphore()
    for one in devices:
        pl.semaphore_signal(
            barrier, inc=1, device_id=one, device_id_type=pl.DeviceIdType.MESH
        )
    pl.semaphore_wait(barrier, len(devices))


def remote(source, target, sends, receives, slot, where):
    return pltpu.make_async_remote_copy(
        src_ref=source,
        dst_ref=target,
        send_sem=sends.at[slot],
        recv_sem=receives.at[slot],
        device_id=where,
        device_id_type=pl.DeviceIdType.MESH,
    )


def columns_of(ref, x):
    half = ref.shape[-1] // 2
    return pl.ds(pl.multiple_of(x * half, 128), half)


def x_first(parts, step, part):
    lone = 2 if parts is ATTEND_PARTS else 0
    if part == lone:
        return step % 2 == 0
    return part == (0 if parts is ATTEND_PARTS else 1)


class Gather:
    def __init__(self, parts, own, full, sems):
        self.parts, self.own, self.full = parts, own, full
        self.local_sem, self.sends, self.receives = sems
        self.count = len(parts)
        self.at = places()

    def own_part(self, part):
        matrix, piece = self.parts[part]
        return self.own[matrix] if piece is None else self.own[matrix].at[piece]

    def spot(self, part, zi, yi, cols):
        matrix, piece = self.parts[part]
        c = self.at[2]
        if piece is None:
            return self.full[matrix].at[zi, yi, c, :, cols]
        return self.full[matrix].at[zi, yi, c, piece, :, cols]

    def flight(self, phase, step, part):
        z, y, c, x = self.at
        zi = far_z(z, step)
        cols = columns_of(self.full[self.parts[part][0]], x)
        everything = slice(None)
        first = x_first(self.parts, step, part)
        if phase == 0:
            here = self.own_part(part)
            there = self.spot(part, z, y, cols)
            where = device(zi, y, c, x)
        elif phase == 1:
            here = there = self.spot(part, zi, y, cols)
            where = device(z, y, c, 1 - x) if first else device(z, 1 - y, c, x)
        elif phase == 2 and first:
            here = there = self.spot(part, zi, y, everything)
            where = device(z, 1 - y, c, x)
        elif phase == 2:
            here = there = self.spot(part, zi, everything, cols)
            where = device(z, y, c, 1 - x)
        else:
            here = there = self.spot(part, zi, everything, everything)
            where = device(z, y, 1 - c, x)
        slot = (phase * 4 + step) * self.count + part
        return remote(here, there, self.sends, self.receives, slot, where)

    def begin(self):
        z, y, c, x = self.at
        greet(partners(z, y, c, x))
        for step in (1, 2, 3):
            for part in range(self.count):
                self.flight(0, step, part).start()
        copies = []
        for part in range(self.count):
            cols = columns_of(self.full[self.parts[part][0]], x)
            copies.append(
                pltpu.make_async_copy(
                    self.own_part(part), self.spot(part, z, y, cols), self.local_sem.at[part]
                )
            )
        for copy in copies:
            copy.start()
        for copy in copies:
            copy.wait()

    def advance(self, phase, step):
        for part in range(self.count):
            if phase > 1 or step:
                self.flight(phase - 1, step, part).wait_recv()
            self.flight(phase, step, part).start()

    def stage(self, number):
        for phase in (1, 2, 3):
            if 0 <= number - phase + 1 < 4:
                self.advance(phase, number - phase + 1)

    def finish(self):
        for step in range(4):
            for part in range(self.count):
                self.flight(3, step, part).wait_recv()
        for phase in range(4):
            for step in range(0 if phase else 1, 4):
                for part in range(self.count):
                    self.flight(phase, step, part).wait_send()


def comm_sems(count):
    return [
        pltpu.SemaphoreType.DMA((4 * count,)),
        pltpu.SemaphoreType.DMA((16 * count,)),
        pltpu.SemaphoreType.DMA((16 * count,)),
    ]


def gather_kernel(own_ref, full_ref, *sems):
    gather = Gather(ATTEND_PARTS, (own_ref,), (full_ref,), sems)
    gather.begin()
    for number in range(6):
        gather.stage(number)
    gather.finish()


def gather_one(shard):
    rows, half = shard.shape
    anywhere = pl.BlockSpec(memory_space=pl.ANY)
    full = pl.pallas_call(
        gather_kernel,
        in_specs=[anywhere],
        out_specs=anywhere,
        out_shape=jax.ShapeDtypeStruct((ZS, 2, 2, 3, rows // 3, 2 * half), jnp.bfloat16),
        scratch_shapes=comm_sems(len(ATTEND_PARTS)),
        compiler_params=pltpu.CompilerParams(collective_id=0, has_side_effects=True),
        name="gather_kernel",
    )(shard.reshape(3, rows // 3, half))
    return full.reshape(ZS * 4 * rows, 2 * half)


def add_rows(first, second, target):
    rows = target.shape[0]

    def step(index, carry):
        at = pl.ds(pl.multiple_of(index * 16, 16), 16)
        total = first(at).astype(jnp.float32) + second(at).astype(jnp.float32)
        target[at, :] = total.astype(target.dtype)
        return carry

    lax.fori_loop(0, rows // 16, step, 0)


class Scatter:
    order = (3, 2, 1, 0)

    def __init__(self, parts, grads, outs, scratch, sems):
        self.parts, self.grads, self.outs = parts, grads, outs
        self.local_sem, self.sends, self.receives = sems
        self.count = count = len(parts)
        self.at = places()
        self.own = scratch[:count]
        self.core_in = scratch[count : 2 * count]
        self.two_x = scratch[2 * count : 3 * count]
        self.two_y = scratch[3 * count : 4 * count]
        self.three_in = scratch[4 * count : 5 * count]
        self.last = scratch[5 * count : 6 * count]
        self.last_in = scratch[6 * count : 7 * count]

    def block(self, part, zi, ci):
        matrix, piece = self.parts[part]
        ref = self.grads[matrix]
        return ref.at[zi, :, ci] if piece is None else ref.at[zi, :, ci, piece]

    def local(self, step, part):
        z, y, c, x = self.at
        return pltpu.make_async_copy(
            self.block(part, far_z(z, step), c),
            self.own[part].at[step],
            self.local_sem.at[step * self.count + part],
        )

    def flight(self, phase, step, part):
        z, y, c, x = self.at
        own = self.own[part]
        first = x_first(self.parts, step, part)
        across_x, across_y = device(z, y, c, 1 - x), device(z, 1 - y, c, x)
        other_cols = columns_of(own, 1 - x)
        if phase == 0:
            here = self.block(part, far_z(z, step), 1 - c)
            there, where = self.core_in[part].at[step], device(z, y, 1 - c, x)
        elif phase == 1 and first:
            here = own.at[step, :, :, other_cols]
            there, where = self.two_x[part].at[step], across_x
        elif phase == 1:
            here = own.at[step, 1 - y]
            there, where = self.two_y[part].at[step], across_y
        elif phase == 2 and first:
            here = self.two_x[part].at[step, 1 - y]
            there, where = self.three_in[part].at[step], across_y
        elif phase == 2:
            here = self.two_y[part].at[step, :, other_cols]
            there, where = self.three_in[part].at[step], across_x
        else:
            here, there = self.last[part].at[step], self.last_in[part].at[step - 1]
            where = device(far_z(z, step), y, c, x)
        slot = (phase * 4 + step) * self.count + part
        return remote(here, there, self.sends, self.receives, slot, where)

    def begin(self):
        greet(partners(*self.at))
        for step in self.order:
            for part in range(self.count):
                self.flight(0, step, part).start()
                self.local(step, part).start()

    def second(self, step):
        for part in range(self.count):
            self.local(step, part).wait()
            self.flight(0, step, part).wait_recv()
            for yi in range(2):
                mine, other = self.own[part].at[step, yi], self.core_in[part].at[step, yi]
                add_rows(lambda at: mine[at, :], lambda at: other[at, :], mine)
            self.flight(1, step, part).start()

    def third(self, step):
        z, y, c, x = self.at
        for part in range(self.count):
            self.flight(1, step, part).wait_recv()
            if x_first(self.parts, step, part):
                cols = columns_of(self.own[part], x)
                for yi in range(2):
                    mine, other = self.own[part].at[step, yi], self.two_x[part].at[step, yi]
                    add_rows(lambda at: mine[at, cols], lambda at: other[at, :], other)
            else:
                mine, other = self.own[part].at[step, y], self.two_y[part].at[step]
                add_rows(lambda at: mine[at, :], lambda at: other[at, :], other)
            self.flight(2, step, part).start()

    def fourth(self, step):
        z, y, c, x = self.at
        for part in range(self.count):
            self.flight(2, step, part).wait_recv()
            other = self.three_in[part].at[step]
            if x_first(self.parts, step, part):
                mine = self.two_x[part].at[step, y]
                first = lambda at: mine[at, :]
            else:
                mine = self.two_y[part].at[step]
                cols = columns_of(self.own[part], x)
                first = lambda at: mine[at, cols]
            add_rows(first, lambda at: other[at, :], self.last[part].at[step])
            if step:
                self.flight(3, step, part).start()

    def stage(self, number):
        if number < 4:
            self.second(self.order[number])
        if 0 <= number - 1 < 4:
            self.third(self.order[number - 1])
        if 0 <= number - 2 < 4:
            self.fourth(self.order[number - 2])

    def finish(self):
        for part in range(self.count):
            for step in (3, 2, 1):
                self.flight(3, step, part).wait_recv()
            matrix, piece = self.parts[part]
            target = self.outs[matrix] if piece is None else self.outs[matrix].at[piece]
            mine, others = self.last[part].at[0], self.last_in[part]

            def total(index, carry):
                at = pl.ds(pl.multiple_of(index * 16, 16), 16)
                value = mine[at, :].astype(jnp.float32)
                for step in range(3):
                    value = value + others[step, at, :].astype(jnp.float32)
                target[at, :] = value
                return carry

            lax.fori_loop(0, target.shape[0] // 16, total, 0)
        for phase in range(4):
            for step in range(1 if phase == 3 else 0, 4):
                for part in range(self.count):
                    self.flight(phase, step, part).wait_send()


def scatter_scratch(heights, widths):
    low = jnp.bfloat16
    sizes = list(zip(heights, widths))
    return (
        [pltpu.VMEM((4, 2, h, w), low) for h, w in sizes]
        + [pltpu.VMEM((4, 2, h, w), low) for h, w in sizes]
        + [pltpu.VMEM((4, 2, h, w // 2), low) for h, w in sizes]
        + [pltpu.VMEM((4, h, w), low) for h, w in sizes]
        + [pltpu.VMEM((4, h, w // 2), low) for h, w in sizes]
        + [pltpu.VMEM((4, h, w // 2), low) for h, w in sizes]
        + [pltpu.VMEM((3, h, w // 2), low) for h, w in sizes]
    )


def scatter_kernel(grad_ref, out_ref, *rest):
    scatter = Scatter(ATTEND_PARTS, (grad_ref,), (out_ref,), rest[:-3], rest[-3:])
    scatter.begin()
    for number in range(6):
        scatter.stage(number)
    scatter.finish()


def scatter_one(grad):
    rows, cols = grad.shape[0] // 16, grad.shape[1]
    count = len(ATTEND_PARTS)
    out = pl.pallas_call(
        scatter_kernel,
        in_specs=[pl.BlockSpec(memory_space=pl.ANY)],
        out_specs=pl.BlockSpec(memory_space=pltpu.VMEM),
        out_shape=jax.ShapeDtypeStruct((3, rows // 3, cols // 2), jnp.float32),
        scratch_shapes=scatter_scratch([rows // 3] * count, [cols] * count) + comm_sems(count),
        compiler_params=pltpu.CompilerParams(
            collective_id=1, has_side_effects=True, vmem_limit_bytes=40 * 2**20
        ),
        name="scatter_kernel",
    )(grad.reshape(ZS, 2, 2, 3, rows // 3, cols))
    return out.reshape(rows, cols // 2)


def at_steps(actions):
    for number, action in actions:
        pl.when(pl.program_id(0) == number)(action)


def forward_riding(triple_ref, bias_ref, label_ref, column_ref, *rest):
    gather = Gather(OTHER_PARTS, rest[:3], rest[5:8], rest[8:])

    def start():
        gather.begin()
        gather.stage(0)

    at_steps(
        [(0, start)] + [(number, lambda number=number: gather.stage(number)) for number in range(1, 6)]
    )
    forward_kernel(triple_ref, bias_ref, label_ref, column_ref, rest[3], rest[4])
    at_steps([(pl.num_programs(0) - 1, gather.finish)])


def backward_riding(
    triple_ref, grad_ref, log_ref, bias_ref, label_ref, column_ref, *rest
):
    scatter = Scatter(OTHER_PARTS, rest[:3], rest[5:8], rest[8:-3], rest[-3:])
    at_steps(
        [(0, scatter.begin)]
        + [(number + 1, lambda number=number: scatter.stage(number)) for number in range(6)]
    )
    backward_kernel(
        triple_ref, grad_ref, log_ref, bias_ref, label_ref, column_ref, rest[3], rest[4]
    )
    at_steps([(pl.num_programs(0) - 1, scatter.finish)])


def total_of(values):
    return jnp.sum(jnp.sum(values, axis=0, keepdims=True), axis=1, keepdims=True)


def finish_kernel(scale, *refs):
    refs = list(refs)

    def take(count):
        taken = refs[:count]
        del refs[:count]
        return taken

    owned, masters, firsts, seconds = take(4), take(4), take(4), take(4)
    lines, bias_lines, (table_grad,) = take(4), take(4), take(1)
    small_masters, small_firsts, small_seconds = take(4), take(4), take(4)
    outs = [take(4) for _ in range(4)]
    small_outs = [take(3) for _ in range(4)]
    (pair_ref,) = take(1)
    updates = take(4)
    packs = take(3)
    incoming = take(3)
    square_ref, square_in, sends, receives = refs
    z, y, c, x = places()
    hops = [
        device(z, y, 1 - c, x),
        device(z, y, c, 1 - x),
        device(z, 1 - y, c, x),
        device(far_z(z, 1), y, c, x),
        device(far_z(z, 2), y, c, x),
    ]
    greet(hops)
    for row in range(4):
        packs[0][row : row + 1, :] = lines[row][...]
    start = 0
    for part in bias_lines:
        packs[1][:, start : start + part.shape[1]] = part[...]
        start += part.shape[1]
    packs[2][...] = table_grad[...]

    def matrix(slot):
        rows, width = masters[slot].shape

        def step(index, carry):
            at = pl.ds(pl.multiple_of(index * 16, 16), 16)
            weight = masters[slot][at, :]
            momentum, variance, update = moments(
                weight, firsts[slot][at, :], seconds[slot][at, :], owned[slot][at, :], decay_rate
            )
            outs[slot][1][at, :] = momentum
            outs[slot][2][at, :] = variance
            updates[slot][at, :] = update
            return (carry[0] + weight * weight, carry[1] + update * update)

        zero = jnp.zeros((16, width), jnp.float32)
        left, right = lax.fori_loop(0, rows // 16, step, (zero, zero))
        return total_of(left), total_of(right)

    squares = []
    for hop in range(5):
        copies = [
            remote(packs[k], incoming[k].at[hop], sends, receives, hop * 3 + k, hops[hop])
            for k in range(3)
        ]
        for copy in copies:
            copy.start()
        if hop < 4:
            squares.append(matrix(hop))
        for k in range(3):
            copies[k].wait()
            packs[k][...] = packs[k][...] + incoming[k][hop]
    place = lax.broadcasted_iota(jnp.int32, (8, 128), 0)
    lane = lax.broadcasted_iota(jnp.int32, (8, 128), 1)
    vector = jnp.zeros((8, 128), jnp.float32)
    for slot in range(4):
        for side in range(2):
            here = (place == slot) & (lane == side)
            vector = jnp.where(here, squares[slot][side], vector)
    square_ref[...] = vector
    small_grads = (packs[0].at[0:2], packs[0].at[2:4], packs[1], packs[2])
    small_updates = []
    for hop in range(5):
        copy = remote(square_ref, square_in.at[hop], sends, receives, 15 + hop, hops[hop])
        copy.start()
        if hop < 4:
            weight = small_masters[hop][...]
            momentum, variance, update = moments(
                weight,
                small_firsts[hop][...],
                small_seconds[hop][...],
                small_grads[hop][...] * scale,
                0.0,
            )
            small_outs[hop][1][...] = momentum
            small_outs[hop][2][...] = variance
            left = jnp.sqrt(total_of(weight * weight))
            right = jnp.sqrt(total_of(update * update))
            small_outs[hop][0][...] = weight - learn_rate * left / (right + adam_eps) * update
            small_updates.append((left, right))
        copy.wait()
        square_ref[...] = square_ref[...] + square_in[hop]
    norms = jnp.sqrt(square_ref[...])
    pairs = norms
    for slot in range(4):
        for side in range(2):
            here = (place == 4 + slot) & (lane == side)
            pairs = jnp.where(here, small_updates[slot][side], pairs)
    pair_ref[...] = pairs
    for slot in range(4):
        left, right = norms[slot : slot + 1, 0:1], norms[slot : slot + 1, 1:2]
        rate = learn_rate * left / (right + adam_eps)

        def apply(index, carry):
            at = pl.ds(pl.multiple_of(index * 16, 16), 16)
            fresh = masters[slot][at, :] - rate * updates[slot][at, :]
            outs[slot][0][at, :] = fresh
            outs[slot][3][at, :] = fresh.astype(jnp.bfloat16)
            return carry

        lax.fori_loop(0, masters[slot].shape[0] // 16, apply, 0)


def finish_all(owned, masters, firsts, seconds, small, scale):
    shapes = [master.shape for master in masters[:4]]
    flat = lambda entry: entry[None] if entry.ndim == 1 else entry
    small_masters = [flat(entry) for entry in masters[4:]]
    small_firsts = [flat(entry) for entry in firsts[4:]]
    small_seconds = [flat(entry) for entry in seconds[4:]]
    small_shapes = [entry.shape for entry in small_masters]
    wide = jnp.float32
    out_shape = []
    for shape in shapes:
        out_shape = out_shape + [jax.ShapeDtypeStruct(shape, wide)] * 3
        out_shape = out_shape + [jax.ShapeDtypeStruct(shape, jnp.bfloat16)]
    for shape in small_shapes:
        out_shape = out_shape + [jax.ShapeDtypeStruct(shape, wide)] * 3
    out_shape = out_shape + [jax.ShapeDtypeStruct((8, 128), wide)]
    pack_shapes = [(4, small_shapes[0][1]), small_shapes[2], small_shapes[3]]
    args = (
        tuple(owned)
        + tuple(masters[:4])
        + tuple(firsts[:4])
        + tuple(seconds[:4])
        + tuple(line[None] for line in small[0])
        + tuple(line[None] for line in small[1])
        + (small[2],)
        + tuple(small_masters)
        + tuple(small_firsts)
        + tuple(small_seconds)
    )
    inside = pl.BlockSpec(memory_space=pltpu.VMEM)
    outs = pl.pallas_call(
        functools.partial(finish_kernel, scale),
        in_specs=[inside] * len(args),
        out_specs=[inside] * len(out_shape),
        out_shape=out_shape,
        scratch_shapes=[pltpu.VMEM(shape, wide) for shape in shapes]
        + [pltpu.VMEM(shape, wide) for shape in pack_shapes]
        + [pltpu.VMEM((5,) + shape, wide) for shape in pack_shapes]
        + [
            pltpu.VMEM((8, 128), wide),
            pltpu.VMEM((5, 8, 128), wide),
            pltpu.SemaphoreType.DMA((20,)),
            pltpu.SemaphoreType.DMA((20,)),
        ],
        compiler_params=pltpu.CompilerParams(
            collective_id=2, has_side_effects=True, vmem_limit_bytes=40 * 2**20
        ),
        name="finish_kernel",
    )(*args)
    outs = list(outs)
    for slot in range(4):
        for side in range(3):
            at = 16 + 3 * slot + side
            outs[at] = outs[at].reshape(masters[4 + slot].shape)
    return outs[:-1] + [outs[-1][:, :2]]


def moments(weight, first, second, gradient, decay):
    momentum = beta_one * first + (1.0 - beta_one) * gradient
    variance = beta_two * second + (1.0 - beta_two) * gradient * gradient
    ratio = (
        momentum / (1.0 - beta_one**STEP) / (jnp.sqrt(variance / (1.0 - beta_two**STEP)) + adam_eps)
    )
    return (momentum, variance, ratio + decay * weight)


def body(
    inputs,
    cotangent,
    regions,
    attend,
    attend_first,
    attend_second,
    project,
    project_first,
    project_second,
    expand,
    expand_first,
    expand_second,
    contract,
    contract_first,
    contract_second,
    gains,
    gains_first,
    gains_second,
    shifts,
    shifts_first,
    shifts_second,
    biases,
    biases_first,
    biases_second,
    position,
    position_first,
    position_second,
):
    masters = (attend, project, expand, contract, gains, shifts, biases, position)
    firsts = (
        attend_first,
        project_first,
        expand_first,
        contract_first,
        gains_first,
        shifts_first,
        biases_first,
        position_first,
    )
    seconds = (
        attend_second,
        project_second,
        expand_second,
        contract_second,
        gains_second,
        shifts_second,
        biases_second,
        position_second,
    )
    dp_count = lax.axis_size("dp")
    shard_count = lax.axis_size("shard")
    tokens_all = inputs.shape[0] * inputs.shape[1] * dp_count * shard_count
    special = special_mesh(dp_count, shard_count)
    shards = tuple(master.astype(jnp.bfloat16) for master in masters[:4])
    if special:
        full = (gather_one(shards[0]),)
    else:
        halves = [lax.all_gather(shard, "dp", axis=0, tiled=True) for shard in shards]
        full = tuple(lax.all_gather(half, "shard", axis=1, tiled=True) for half in halves)
    labels = window_labels(regions)
    bias = table_to_bias(position)
    images = inputs.shape[0]
    values_low, cot_low, normed_low = enter(inputs, cotangent, gains[0], shifts[0])
    result_low, grad_input, grads, small_grads = whole_step(
        values_low,
        cot_low,
        normed_low,
        full,
        shards[1:] if special else None,
        gains,
        shifts,
        biases,
        bias,
        labels,
        position.shape[0],
        1.0 / tokens_all,
    )
    result_low, grad_input = leave(result_low, grad_input, images)
    if special:
        owned = (scatter_one(grads[0]),) + tuple(grads[1:])
        rest = finish_all(owned, masters, firsts, seconds, small_grads, 1.0 / tokens_all)
        return tuple([result_low, grad_input] + rest)
    lines, bias_lines, table_grad = small_grads
    small_total = lax.psum(
        (
            jnp.stack(lines[:2]) / tokens_all,
            jnp.stack(lines[2:]) / tokens_all,
            jnp.concatenate(bias_lines) / tokens_all,
            table_grad / tokens_all,
        ),
        ("dp", "shard"),
    )
    columns = [
        lax.psum_scatter(grad, "shard", scatter_dimension=1, tiled=True).astype(jnp.float32)
        for grad in grads
    ]
    owned = tuple(
        lax.psum_scatter(column, "dp", scatter_dimension=0, tiled=True) for column in columns
    )
    pieces = [
        moments(masters[slot], firsts[slot], seconds[slot], owned[slot], decay_rate)
        for slot in range(4)
    ]
    partial_value = jnp.stack(
        [
            jnp.stack(
                [jnp.sum(masters[slot] * masters[slot]), jnp.sum(pieces[slot][2] * pieces[slot][2])]
            )
            for slot in range(4)
        ]
    )
    squares = lax.psum(partial_value, ("dp", "shard"))
    matrix_norms = jnp.sqrt(squares)
    outputs = [result_low, grad_input]
    pairs = []
    for slot in range(4):
        momentum, variance, update = pieces[slot]
        fresh = (
            masters[slot]
            - learn_rate * matrix_norms[slot, 0] / (matrix_norms[slot, 1] + adam_eps) * update
        )
        outputs = outputs + [fresh, momentum, variance, fresh.astype(jnp.bfloat16)]
        pairs.append(matrix_norms[slot])
    for slot in range(4):
        weight = masters[4 + slot]
        momentum, variance, update = moments(
            weight, firsts[4 + slot], seconds[4 + slot], small_total[slot], 0.0
        )
        norms = jnp.stack([jnp.sqrt(jnp.sum(weight * weight)), jnp.sqrt(jnp.sum(update * update))])
        fresh = weight - learn_rate * norms[0] / (norms[1] + adam_eps) * update
        outputs = outputs + [fresh, momentum, variance]
        pairs.append(norms)
    outputs = outputs + [jnp.stack(pairs)]
    return tuple(outputs)


def solution(mesh):
    return jax.shard_map(
        body,
        mesh=mesh,
        in_specs=(
            P(("dp", "shard"), None, None),
            P(("dp", "shard"), None, None),
            P(),
            P("dp", "shard"),
            P("dp", "shard"),
            P("dp", "shard"),
            P("dp", "shard"),
            P("dp", "shard"),
            P("dp", "shard"),
            P("dp", "shard"),
            P("dp", "shard"),
            P("dp", "shard"),
            P("dp", "shard"),
            P("dp", "shard"),
            P("dp", "shard"),
            P(),
            P(),
            P(),
            P(),
            P(),
            P(),
            P(),
            P(),
            P(),
            P(),
            P(),
            P(),
        ),
        out_specs=(
            P(("dp", "shard"), None, None),
            P(("dp", "shard"), None, None),
            P("dp", "shard"),
            P("dp", "shard"),
            P("dp", "shard"),
            P("dp", "shard"),
            P("dp", "shard"),
            P("dp", "shard"),
            P("dp", "shard"),
            P("dp", "shard"),
            P("dp", "shard"),
            P("dp", "shard"),
            P("dp", "shard"),
            P("dp", "shard"),
            P("dp", "shard"),
            P("dp", "shard"),
            P("dp", "shard"),
            P("dp", "shard"),
            P(),
            P(),
            P(),
            P(),
            P(),
            P(),
            P(),
            P(),
            P(),
            P(),
            P(),
            P(),
            P(),
        ),
        check_vma=False,
    )
```

```python
import functools

import jax
import jax.numpy as jnp
from jax import lax
from jax.experimental import pallas as pl
from jax.experimental.pallas import tpu as pltpu
from jax.sharding import PartitionSpec as P

HD = 32
WIN = 12
STEP = 10
HEADS = 24
GRID = 24
SHIFT = 6


beta_one = 0.9
beta_two = 0.999
adam_eps = 1e-06
decay_rate = 0.01
learn_rate = 0.25
norm_eps = 1e-05
masked_score = -100.0


def layer_norm(values, gain_row, shift_row):
    centred = values - jnp.mean(values, axis=-1, keepdims=True)
    spread = jnp.mean(centred * centred, axis=-1, keepdims=True)
    return centred * lax.rsqrt(spread + norm_eps) * gain_row + shift_row


def window_labels(regions):
    return (
        regions.reshape(GRID // WIN, WIN, GRID // WIN, WIN)
        .transpose(0, 2, 1, 3)
        .reshape((GRID // WIN) ** 2, WIN * WIN)
    )


AREA = WIN * WIN
SPAN = 2 * WIN - 1
REACH = 384
TABLE_PAD = 640
HEAD_STEP = 4
CENTRE = (WIN - 1) * SPAN + WIN - 1


def dot00(left, right):
    return lax.dot_general(
        left, right, (((0,), (0,)), ((), ())), preferred_element_type=jnp.float32
    )


def dot11(left, right):
    return lax.dot_general(
        left, right, (((1,), (1,)), ((), ())), preferred_element_type=jnp.float32
    )


def dot10(left, right):
    return lax.dot_general(
        left, right, (((1,), (0,)), ((), ())), preferred_element_type=jnp.float32
    )


def spread_places(shape, table_dim, token_dim):
    token = lax.broadcasted_iota(jnp.int32, shape, token_dim)
    place = lax.broadcasted_iota(jnp.int32, shape, table_dim)
    token_row = token // WIN
    return place == token + (SPAN - WIN) * token_row


def bias_kernel(table_ref, bias_ref):
    spot = spread_places((REACH, AREA), 0, 1).astype(jnp.bfloat16)
    table = table_ref[...]
    for row in range(WIN):
        rolled = []
        for column in range(WIN):
            back = SPAN * (WIN - 1 - row) + WIN - 1 - column
            rolled.append(pltpu.roll(table, (TABLE_PAD - back) % TABLE_PAD, 1)[:, :REACH])
        block = jnp.concatenate(rolled, axis=0)
        high = block.astype(jnp.bfloat16)
        rest = block - high.astype(jnp.float32)
        middle = rest.astype(jnp.bfloat16)
        low = (rest - middle.astype(jnp.float32)).astype(jnp.bfloat16)
        picked = dot10(high, spot) + (dot10(middle, spot) + dot10(low, spot))
        for column in range(WIN):
            bias_ref[row * WIN + column] = picked[column * HEADS : (column + 1) * HEADS]


def table_kernel(scores_ref, table_ref):
    spot = spread_places((AREA, REACH), 1, 0).astype(jnp.bfloat16)
    total = jnp.zeros((HEADS, TABLE_PAD), jnp.float32)
    for row in range(WIN):
        block = scores_ref[row * WIN : (row + 1) * WIN].reshape(WIN * HEADS, AREA)
        high = block.astype(jnp.bfloat16)
        low = (block - high.astype(jnp.float32)).astype(jnp.bfloat16)
        spread = dot10(high, spot) + dot10(low, spot)
        inner = spread[:HEADS]
        for column in range(1, WIN):
            inner = pltpu.roll(inner, 1, 1) + spread[column * HEADS : (column + 1) * HEADS]
        inner = jnp.concatenate(
            [inner, jnp.zeros((HEADS, TABLE_PAD - REACH), jnp.float32)], axis=1
        )
        if row:
            total = pltpu.roll(total, SPAN, 1)
        total = total + inner
    table_ref[...] = total


def table_to_bias(position):
    rows = position.shape[0]
    table = jnp.pad(position.T, ((0, 0), (0, TABLE_PAD - rows)))
    spread = pl.pallas_call(
        bias_kernel,
        out_shape=jax.ShapeDtypeStruct((AREA, HEADS, AREA), jnp.float32),
        name="bias_kernel",
    )(table)
    return spread.transpose(1, 0, 2)


def scores_to_table(scores):
    return pl.pallas_call(
        table_kernel,
        out_shape=jax.ShapeDtypeStruct((HEADS, TABLE_PAD), jnp.float32),
        name="table_kernel",
    )(scores.transpose(1, 0, 2))


def scores_of(keyed, query, bias, allowed):
    return jnp.where(allowed, dot00(keyed, query) * HD ** (-0.5) + bias, masked_score)


def head_slices(ref, head):
    width = HEADS * HD
    return tuple(
        ref[0, pl.ds(pl.multiple_of(block * width + head * HD, HD), HD), :] for block in range(3)
    )


def forward_kernel(triple_ref, bias_ref, label_ref, column_ref, mixed_ref, log_ref):
    allowed = column_ref[0] == label_ref[0]

    def step(group, carry):
        for member in range(HEAD_STEP):
            head = group * HEAD_STEP + member
            query, keyed, valued = head_slices(triple_ref, head)
            scores = scores_of(keyed, query, bias_ref[head], allowed)
            top = jnp.max(scores, axis=0, keepdims=True)
            raised = jnp.exp(scores - top)
            total = jnp.sum(raised, axis=0, keepdims=True)
            probs = (raised * (1.0 / total)).astype(jnp.bfloat16)
            mixed_ref[0, pl.ds(pl.multiple_of(head * HD, HD), HD), :] = dot10(
                valued, probs
            ).astype(jnp.bfloat16)
            log_ref[0, head] = top + jnp.log(total)
        return carry

    lax.fori_loop(0, HEADS // HEAD_STEP, step, 0)


def backward_kernel(
    triple_ref, grad_ref, log_ref, bias_ref, label_ref, column_ref, out_ref, scores_ref
):
    allowed = column_ref[0] == label_ref[0]
    width = HEADS * HD

    @pl.when(pl.program_id(0) == 0)
    def _():
        scores_ref[...] = jnp.zeros_like(scores_ref)

    def step(group, carry):
        for member in range(HEAD_STEP):
            head = group * HEAD_STEP + member
            query, keyed, valued = head_slices(triple_ref, head)
            grad = grad_ref[0, pl.ds(pl.multiple_of(head * HD, HD), HD), :]
            scores = scores_of(keyed, query, bias_ref[head], allowed)
            probs = jnp.exp(scores - log_ref[0, head])
            grad_probs = dot00(valued, grad)
            weighted = probs * grad_probs
            mean = jnp.sum(weighted, axis=0, keepdims=True)
            grad_scores = jnp.where(allowed, weighted - probs * mean, 0.0)
            scores_ref[head] += grad_scores
            raw = (grad_scores * HD ** (-0.5)).astype(jnp.bfloat16)
            results = (
                dot10(keyed, raw),
                dot11(query, raw),
                dot11(grad, probs.astype(jnp.bfloat16)),
            )
            for block in range(3):
                rows = pl.ds(pl.multiple_of(block * width + head * HD, HD), HD)
                out_ref[0, rows, :] = results[block].astype(jnp.bfloat16)
        return carry

    lax.fori_loop(0, HEADS // HEAD_STEP, step, 0)


def entry_kernel(value_ref, cot_ref, gain_ref, shift_ref, value_out, cot_out, norm_out, turned):
    for source, target in ((cot_ref, cot_out), (value_ref, value_out)):
        for row in range(GRID):
            line = source[0, row * GRID : (row + 1) * GRID, :].astype(jnp.float32)
            line = pltpu.roll(line, GRID - SHIFT, 0)
            place = (row - SHIFT) % GRID
            down, within = place // WIN, place % WIN
            for across in range(GRID // WIN):
                at = (down * (GRID // WIN) + across) * AREA + within * WIN
                turned[at : at + WIN, :] = line[across * WIN : (across + 1) * WIN]
        if source is cot_ref:
            target[...] = turned[...].astype(jnp.bfloat16)

    def step(index, carry):
        at = pl.ds(pl.multiple_of(index * 48, 48), 48)
        values = turned[at, :]
        value_out[at, :] = values.astype(jnp.bfloat16)
        norm_out[at, :] = layer_norm(values, gain_ref[...], shift_ref[...]).astype(jnp.bfloat16)
        return carry

    lax.fori_loop(0, GRID * GRID // 48, step, 0)


def enter(values, cot, gain, shift):
    images, tokens, width = values.shape
    image = pl.BlockSpec((1, tokens, width), lambda index: (index, 0, 0))
    line = pl.BlockSpec((1, width), lambda index: (0, 0))
    rows = pl.BlockSpec((tokens, width), lambda index: (index, 0))
    return pl.pallas_call(
        entry_kernel,
        grid=(images,),
        in_specs=[image, image, line, line],
        out_specs=[rows] * 3,
        out_shape=[jax.ShapeDtypeStruct((images * tokens, width), jnp.bfloat16)] * 3,
        scratch_shapes=[pltpu.VMEM((tokens, width), jnp.float32)],
        name="entry_kernel",
    )(values, cot, gain[None], shift[None])


def exit_kernel(result_ref, grad_ref, result_out, grad_out, turned):
    for source, target in ((result_ref, result_out), (grad_ref, grad_out)):
        turned[...] = source[...].astype(jnp.float32)
        for row in range(GRID):
            place = (row - SHIFT) % GRID
            down, within = place // WIN, place % WIN
            starts = [(down * (GRID // WIN) + across) * AREA + within * WIN for across in range(2)]
            line = jnp.concatenate([turned[at : at + WIN, :] for at in starts], axis=0)
            line = pltpu.roll(line, SHIFT, 0)
            target[0, row * GRID : (row + 1) * GRID, :] = line.astype(target.dtype)


def leave(result, grad, images):
    width = result.shape[1]
    tokens = GRID * GRID
    image = pl.BlockSpec((1, tokens, width), lambda index: (index, 0, 0))
    rows = pl.BlockSpec((tokens, width), lambda index: (index, 0))
    return pl.pallas_call(
        exit_kernel,
        grid=(images,),
        in_specs=[rows] * 2,
        out_specs=[image] * 2,
        out_shape=[
            jax.ShapeDtypeStruct((images, tokens, width), jnp.bfloat16),
            jax.ShapeDtypeStruct((images, tokens, width), jnp.float32),
        ],
        scratch_shapes=[pltpu.VMEM((tokens, width), jnp.float32)],
        name="exit_kernel",
    )(result, grad)


def window_block(rows):
    return pl.BlockSpec((1, rows, AREA), lambda window: (window, 0, 0))


def label_blocks(count):
    return [
        pl.BlockSpec((1, 1, AREA), lambda window: (window % count, 0, 0)),
        pl.BlockSpec((1, AREA, 1), lambda window: (window % count, 0, 0)),
    ]


def attend_forward(triple, bias, labels, shards):
    windows = triple.shape[0]
    width = HEADS * HD
    whole = pl.BlockSpec((HEADS, AREA, AREA), lambda window: (0, 0, 0))
    log_block = pl.BlockSpec((1, HEADS, 1, AREA), lambda window: (window, 0, 0, 0))
    in_specs = [window_block(3 * width), whole] + label_blocks(labels.shape[0])
    out_specs = [window_block(width), log_block]
    out_shape = [
        jax.ShapeDtypeStruct((windows, width, AREA), jnp.bfloat16),
        jax.ShapeDtypeStruct((windows, HEADS, 1, AREA), jnp.float32),
    ]
    arrays = (triple, bias, labels[:, None, :], labels[:, :, None])
    if shards is None:
        return pl.pallas_call(
            forward_kernel,
            grid=(windows,),
            in_specs=in_specs,
            out_specs=out_specs,
            out_shape=out_shape,
            name="forward_kernel",
        )(*arrays)
    anywhere = pl.BlockSpec(memory_space=pl.ANY)
    full_shapes = [(ZS, 2, 2, shard.shape[0], 2 * shard.shape[1]) for shard in shards]
    mixed, log_total, *full = pl.pallas_call(
        forward_riding,
        grid=(windows,),
        in_specs=in_specs + [anywhere] * 3,
        out_specs=out_specs + [anywhere] * 3,
        out_shape=out_shape + [jax.ShapeDtypeStruct(shape, jnp.bfloat16) for shape in full_shapes],
        scratch_shapes=comm_sems(3),
        compiler_params=pltpu.CompilerParams(collective_id=4, has_side_effects=True),
        name="forward_kernel",
    )(*arrays, *shards)
    full = [each.reshape(ZS * 4 * shard.shape[0], -1) for each, shard in zip(full, shards)]
    return mixed, log_total, full


def attend_backward(triple, grad, log_total, bias, labels, grads):
    windows = triple.shape[0]
    width = HEADS * HD
    whole = pl.BlockSpec((HEADS, AREA, AREA), lambda window: (0, 0, 0))
    log_block = pl.BlockSpec((1, HEADS, 1, AREA), lambda window: (window, 0, 0, 0))
    in_specs = [window_block(3 * width), window_block(width), log_block, whole]
    in_specs = in_specs + label_blocks(labels.shape[0])
    out_specs = [window_block(3 * width), whole]
    out_shape = [
        jax.ShapeDtypeStruct((windows, 3 * width, AREA), jnp.bfloat16),
        jax.ShapeDtypeStruct((HEADS, AREA, AREA), jnp.float32),
    ]
    arrays = (triple, grad, log_total, bias, labels[:, None, :], labels[:, :, None])
    if grads is None:
        return pl.pallas_call(
            backward_kernel,
            grid=(windows,),
            in_specs=in_specs,
            out_specs=out_specs,
            out_shape=out_shape,
            name="backward_kernel",
        )(*arrays)
    sizes = [(grad.shape[0] // 16, grad.shape[1]) for grad in grads]
    heights, widths = zip(*sizes)
    out = pl.pallas_call(
        backward_riding,
        grid=(windows,),
        in_specs=in_specs + [pl.BlockSpec(memory_space=pl.ANY)] * 3,
        out_specs=out_specs + [pl.BlockSpec(memory_space=pltpu.VMEM)] * 3,
        out_shape=out_shape
        + [jax.ShapeDtypeStruct((rows, cols // 2), jnp.float32) for rows, cols in sizes],
        scratch_shapes=scatter_scratch(heights, widths) + comm_sems(3),
        compiler_params=pltpu.CompilerParams(
            collective_id=5, has_side_effects=True, vmem_limit_bytes=60 * 2**20
        ),
        name="backward_kernel",
    )(*arrays, *[grad.reshape(ZS, 2, 2, rows, cols) for grad, (rows, cols) in zip(grads, sizes)])
    return out[0], out[1], out[2:]


FEED_TILE = 512
FEED_ROWS = 192


def feed_kernel(
    scale,
    norm_ref,
    turned_ref,
    cot_ref,
    middle_ref,
    expand_ref,
    contract_ref,
    bias_in_ref,
    bias_out_ref,
    result_ref,
    back_ref,
    grad_contract_ref,
    grad_expand_ref,
    grad_bias_ref,
    total,
    active_all,
    grad_all,
):
    tile = pl.program_id(0)
    rows = norm_ref.shape[0]

    @pl.when(tile == 0)
    def _():
        back_ref[...] = jnp.zeros_like(back_ref)
        total[...] = middle_ref[...] + bias_out_ref[...]

    def step(index, carry):
        for member in range(2):
            at = pl.ds(pl.multiple_of((index * 2 + member) * FEED_ROWS, FEED_ROWS), FEED_ROWS)
            hidden = dot10(norm_ref[at, :], expand_ref[...]) + bias_in_ref[...]
            grad_active = dot11(cot_ref[at, :], contract_ref[...])
            share = 0.5 + 0.5 * lax.erf(hidden * 0.5**0.5)
            bell = jnp.exp(-0.5 * hidden * hidden) * 0.3989422804014327
            active = (hidden * share).astype(jnp.bfloat16)
            grad_hidden = grad_active * (share + hidden * bell)
            grad_low = grad_hidden.astype(jnp.bfloat16)
            active_all[at, :] = active
            grad_all[at, :] = grad_low
            total[at, :] += dot10(active, contract_ref[...])
            back_ref[at, :] += dot11(grad_low, expand_ref[...])
            carry = carry + jnp.sum(
                grad_low.astype(jnp.float32).reshape(FEED_ROWS // 8, 8, FEED_TILE), axis=0
            )
        return carry

    sums = lax.fori_loop(
        0, rows // (2 * FEED_ROWS), step, jnp.zeros((8, FEED_TILE), jnp.float32)
    )
    grad_bias_ref[...] = jnp.sum(sums, axis=0, keepdims=True)
    grad_contract_ref[...] = (dot00(active_all[...], cot_ref[...]) * scale).astype(jnp.bfloat16)
    grad_expand_ref[...] = (dot10(turned_ref[...], grad_all[...]) * scale).astype(jnp.bfloat16)

    @pl.when(tile == pl.num_programs(0) - 1)
    def _():
        result_ref[...] = total[...].astype(jnp.bfloat16)


def feed(norm, cot, middle, expand, contract, bias_in, bias_out, scale):
    rows, width = norm.shape
    hidden = expand.shape[1]
    whole = pl.BlockSpec((rows, width), lambda tile: (0, 0))
    turned = pl.BlockSpec((width, rows), lambda tile: (0, 0))
    wide = pl.BlockSpec((width, FEED_TILE), lambda tile: (0, tile))
    tall = pl.BlockSpec((FEED_TILE, width), lambda tile: (tile, 0))
    line = pl.BlockSpec((1, FEED_TILE), lambda tile: (0, tile))
    out_line = pl.BlockSpec((1, width), lambda tile: (0, 0))
    return pl.pallas_call(
        functools.partial(feed_kernel, scale),
        grid=(hidden // FEED_TILE,),
        in_specs=[whole, turned, whole, whole, wide, tall, line, out_line],
        out_specs=[whole, whole, tall, wide, line],
        out_shape=[
            jax.ShapeDtypeStruct((rows, width), jnp.bfloat16),
            jax.ShapeDtypeStruct((rows, width), jnp.float32),
            jax.ShapeDtypeStruct((hidden, width), jnp.bfloat16),
            jax.ShapeDtypeStruct((width, hidden), jnp.bfloat16),
            jax.ShapeDtypeStruct((1, hidden), jnp.float32),
        ],
        scratch_shapes=[
            pltpu.VMEM((rows, width), jnp.float32),
            pltpu.VMEM((rows, FEED_TILE), jnp.bfloat16),
            pltpu.VMEM((rows, FEED_TILE), jnp.bfloat16),
        ],
        compiler_params=pltpu.CompilerParams(vmem_limit_bytes=56 * 2**20),
        name="feed_kernel",
    )(norm, norm.T, cot, middle, expand, contract, bias_in[None], bias_out[None])


def whole_step(
    values_low, cot_low, normed_low, full, shards, gains, shifts, biases, bias, labels, scale
):
    attend = full[0]
    width = attend.shape[0]
    hidden_width = biases.shape[0] - 5 * width
    windows = values_low.shape[0] // AREA
    values = values_low.astype(jnp.float32)
    norm_back = jax.vjp(layer_norm, values, gains[0], shifts[0])[1]
    windowed = normed_low.reshape(windows, AREA, width)
    triple = jnp.einsum("wtc,ce->wet", windowed, attend, preferred_element_type=jnp.float32)
    triple = (triple + biases[: 3 * width][None, :, None]).astype(jnp.bfloat16)
    if shards is None:
        mixed, log_total = attend_forward(triple, bias, labels, None)
        project, expand, contract = full[1:]
    else:
        mixed, log_total, (project, expand, contract) = attend_forward(triple, bias, labels, shards)
    branch = (
        jnp.einsum("wct,ce->wte", mixed, project, preferred_element_type=jnp.float32).reshape(
            -1, width
        )
        + biases[3 * width : 4 * width]
    )
    middle = values + branch
    normed_two, norm_two_back = jax.vjp(layer_norm, middle, gains[1], shifts[1])
    normed_two_low = normed_two.astype(jnp.bfloat16)
    cot_float = cot_low.astype(jnp.float32)
    grad_bias_contract = jnp.sum(cot_float, axis=0)
    result, grad_normed_two, grad_contract, grad_expand, grad_bias_expand = feed(
        normed_two_low,
        cot_low,
        middle,
        expand,
        contract,
        biases[4 * width : 4 * width + hidden_width],
        biases[4 * width + hidden_width :],
        scale,
    )
    grad_middle_part, grad_gain_two, grad_shift_two = norm_two_back(grad_normed_two)
    grad_middle = cot_float + grad_middle_part
    grad_branch_low = grad_middle.astype(jnp.bfloat16)
    grad_branch_windows = grad_branch_low.reshape(windows, AREA, width)
    grad_project = jnp.einsum(
        "wct,wte->ce", mixed, grad_branch_windows, preferred_element_type=jnp.float32
    )
    grad_bias_project = jnp.sum(grad_branch_low, axis=0, dtype=jnp.float32)
    grad_mixed = jnp.einsum(
        "wte,ce->wct", grad_branch_windows, project, preferred_element_type=jnp.float32
    ).astype(jnp.bfloat16)
    others = ((grad_project * scale).astype(jnp.bfloat16), grad_expand, grad_contract)
    if shards is None:
        grad_triple, grad_scores = attend_backward(
            triple, grad_mixed, log_total, bias, labels, None
        )
    else:
        grad_triple, grad_scores, others = attend_backward(
            triple, grad_mixed, log_total, bias, labels, others
        )
    grad_position = scores_to_table(grad_scores)
    grad_attend = jnp.einsum(
        "wtc,wet->ce", windowed, grad_triple, preferred_element_type=jnp.float32
    )
    grad_bias_attend = jnp.sum(grad_triple, axis=(0, 2), dtype=jnp.float32)
    grad_normed = jnp.einsum(
        "wet,ce->wtc", grad_triple, attend, preferred_element_type=jnp.float32
    ).reshape(-1, width)
    grad_input_part, grad_gain_one, grad_shift_one = norm_back(grad_normed)
    grad_input = grad_middle + grad_input_part
    grads = ((grad_attend * scale).astype(jnp.bfloat16),) + tuple(others)
    small = (
        (grad_gain_one, grad_gain_two, grad_shift_one, grad_shift_two),
        (grad_bias_attend, grad_bias_project, grad_bias_expand[0], grad_bias_contract),
        grad_position,
    )
    return (result, grad_input, grads, small)


ZS = 4
SPLIT = 2
ATTEND_PARTS = ((0, 0), (0, 1), (0, 2))
OTHER_PARTS = ((0, None), (1, None), (2, None))


def special_mesh(dp_count, shard_count):
    return dp_count == ZS * SPLIT * SPLIT and shard_count == SPLIT


def places():
    at = lax.axis_index("dp")
    return at // 4, lax.rem(at // 2, 2), lax.rem(at, 2), lax.axis_index("shard")


def far_z(z, step):
    return (z, z + 1 - 2 * lax.rem(z, 2), lax.rem(z + 2, 4), 3 - z)[step]


def device(z, y, c, x):
    return {"dp": (z * 2 + y) * 2 + c, "shard": x}


def partners(z, y, c, x):
    return [device(far_z(z, step), y, c, x) for step in (1, 2, 3)] + [
        device(z, y, c, 1 - x),
        device(z, 1 - y, c, x),
        device(z, y, 1 - c, x),
    ]


def greet(devices):
    barrier = pltpu.get_barrier_semaphore()
    for one in devices:
        pl.semaphore_signal(
            barrier, inc=1, device_id=one, device_id_type=pl.DeviceIdType.MESH
        )
    pl.semaphore_wait(barrier, len(devices))


def remote(source, target, sends, receives, slot, where):
    return pltpu.make_async_remote_copy(
        src_ref=source,
        dst_ref=target,
        send_sem=sends.at[slot],
        recv_sem=receives.at[slot],
        device_id=where,
        device_id_type=pl.DeviceIdType.MESH,
    )


def columns_of(ref, x):
    half = ref.shape[-1] // 2
    return pl.ds(pl.multiple_of(x * half, 128), half)


def x_first(parts, step, part):
    lone = 2 if parts is ATTEND_PARTS else 0
    if part == lone:
        return step % 2 == 0
    return part == (0 if parts is ATTEND_PARTS else 1)


class Gather:
    def __init__(self, parts, own, full, sems):
        self.parts, self.own, self.full = parts, own, full
        self.local_sem, self.sends, self.receives = sems
        self.count = len(parts)
        self.at = places()

    def own_part(self, part):
        matrix, piece = self.parts[part]
        return self.own[matrix] if piece is None else self.own[matrix].at[piece]

    def spot(self, part, zi, yi, cols):
        matrix, piece = self.parts[part]
        c = self.at[2]
        if piece is None:
            return self.full[matrix].at[zi, yi, c, :, cols]
        return self.full[matrix].at[zi, yi, c, piece, :, cols]

    def flight(self, phase, step, part):
        z, y, c, x = self.at
        zi = far_z(z, step)
        cols = columns_of(self.full[self.parts[part][0]], x)
        everything = slice(None)
        first = x_first(self.parts, step, part)
        if phase == 0:
            here = self.own_part(part)
            there = self.spot(part, z, y, cols)
            where = device(zi, y, c, x)
        elif phase == 1:
            here = there = self.spot(part, zi, y, cols)
            where = device(z, y, c, 1 - x) if first else device(z, 1 - y, c, x)
        elif phase == 2 and first:
            here = there = self.spot(part, zi, y, everything)
            where = device(z, 1 - y, c, x)
        elif phase == 2:
            here = there = self.spot(part, zi, everything, cols)
            where = device(z, y, c, 1 - x)
        else:
            here = there = self.spot(part, zi, everything, everything)
            where = device(z, y, 1 - c, x)
        slot = (phase * 4 + step) * self.count + part
        return remote(here, there, self.sends, self.receives, slot, where)

    def begin(self):
        z, y, c, x = self.at
        greet(partners(z, y, c, x))
        for step in (1, 2, 3):
            for part in range(self.count):
                self.flight(0, step, part).start()
        copies = []
        for part in range(self.count):
            cols = columns_of(self.full[self.parts[part][0]], x)
            copies.append(
                pltpu.make_async_copy(
                    self.own_part(part), self.spot(part, z, y, cols), self.local_sem.at[part]
                )
            )
        for copy in copies:
            copy.start()
        for copy in copies:
            copy.wait()

    def advance(self, phase, step):
        for part in range(self.count):
            if phase > 1 or step:
                self.flight(phase - 1, step, part).wait_recv()
            self.flight(phase, step, part).start()

    def stage(self, number):
        for phase in (3, 2, 1):
            if 0 <= number - phase + 1 < 4:
                self.advance(phase, number - phase + 1)

    def finish(self):
        for step in range(4):
            for part in range(self.count):
                self.flight(3, step, part).wait_recv()
        for phase in range(4):
            for step in range(0 if phase else 1, 4):
                for part in range(self.count):
                    self.flight(phase, step, part).wait_send()


def comm_sems(count):
    return [
        pltpu.SemaphoreType.DMA((4 * count,)),
        pltpu.SemaphoreType.DMA((16 * count,)),
        pltpu.SemaphoreType.DMA((16 * count,)),
    ]


def gather_kernel(own_ref, full_ref, *sems):
    gather = Gather(ATTEND_PARTS, (own_ref,), (full_ref,), sems)
    gather.begin()
    for number in range(6):
        gather.stage(number)
    gather.finish()


def gather_one(shard):
    rows, half = shard.shape
    anywhere = pl.BlockSpec(memory_space=pl.ANY)
    full = pl.pallas_call(
        gather_kernel,
        in_specs=[anywhere],
        out_specs=anywhere,
        out_shape=jax.ShapeDtypeStruct((ZS, 2, 2, 3, rows // 3, 2 * half), jnp.bfloat16),
        scratch_shapes=comm_sems(len(ATTEND_PARTS)),
        compiler_params=pltpu.CompilerParams(collective_id=0, has_side_effects=True),
        name="gather_kernel",
    )(shard.reshape(3, rows // 3, half))
    return full.reshape(ZS * 4 * rows, 2 * half)


def add_rows(first, second, target):
    rows = target.shape[0]

    def step(index, carry):
        at = pl.ds(pl.multiple_of(index * 16, 16), 16)
        total = first(at).astype(jnp.float32) + second(at).astype(jnp.float32)
        target[at, :] = total.astype(target.dtype)
        return carry

    lax.fori_loop(0, rows // 16, step, 0)


class Scatter:
    order = (3, 2, 1, 0)

    def __init__(self, parts, grads, outs, scratch, sems):
        self.parts, self.grads, self.outs = parts, grads, outs
        self.local_sem, self.sends, self.receives = sems
        self.count = count = len(parts)
        self.at = places()
        self.own = scratch[:count]
        self.core_in = scratch[count : 2 * count]
        self.two_x = scratch[2 * count : 3 * count]
        self.two_y = scratch[3 * count : 4 * count]
        self.three_in = scratch[4 * count : 5 * count]
        self.last = scratch[5 * count : 6 * count]
        self.last_in = scratch[6 * count : 7 * count]

    def block(self, part, zi, ci):
        matrix, piece = self.parts[part]
        ref = self.grads[matrix]
        return ref.at[zi, :, ci] if piece is None else ref.at[zi, :, ci, piece]

    def local(self, step, part):
        z, y, c, x = self.at
        return pltpu.make_async_copy(
            self.block(part, far_z(z, step), c),
            self.own[part].at[step],
            self.local_sem.at[step * self.count + part],
        )

    def flight(self, phase, step, part):
        z, y, c, x = self.at
        own = self.own[part]
        first = x_first(self.parts, step, part)
        across_x, across_y = device(z, y, c, 1 - x), device(z, 1 - y, c, x)
        other_cols = columns_of(own, 1 - x)
        if phase == 0:
            here = self.block(part, far_z(z, step), 1 - c)
            there, where = self.core_in[part].at[step], device(z, y, 1 - c, x)
        elif phase == 1 and first:
            here = own.at[step, :, :, other_cols]
            there, where = self.two_x[part].at[step], across_x
        elif phase == 1:
            here = own.at[step, 1 - y]
            there, where = self.two_y[part].at[step], across_y
        elif phase == 2 and first:
            here = self.two_x[part].at[step, 1 - y]
            there, where = self.three_in[part].at[step], across_y
        elif phase == 2:
            here = self.two_y[part].at[step, :, other_cols]
            there, where = self.three_in[part].at[step], across_x
        else:
            here, there = self.last[part].at[step], self.last_in[part].at[step - 1]
            where = device(far_z(z, step), y, c, x)
        slot = (phase * 4 + step) * self.count + part
        return remote(here, there, self.sends, self.receives, slot, where)

    def begin(self):
        greet(partners(*self.at))
        for step in self.order:
            for part in range(self.count):
                self.flight(0, step, part).start()
                self.local(step, part).start()

    def second(self, step):
        for part in range(self.count):
            self.local(step, part).wait()
            self.flight(0, step, part).wait_recv()
            for yi in range(2):
                mine, other = self.own[part].at[step, yi], self.core_in[part].at[step, yi]
                add_rows(lambda at: mine[at, :], lambda at: other[at, :], mine)
            self.flight(1, step, part).start()

    def third(self, step):
        z, y, c, x = self.at
        for part in range(self.count):
            self.flight(1, step, part).wait_recv()
            if x_first(self.parts, step, part):
                cols = columns_of(self.own[part], x)
                for yi in range(2):
                    mine, other = self.own[part].at[step, yi], self.two_x[part].at[step, yi]
                    add_rows(lambda at: mine[at, cols], lambda at: other[at, :], other)
            else:
                mine, other = self.own[part].at[step, y], self.two_y[part].at[step]
                add_rows(lambda at: mine[at, :], lambda at: other[at, :], other)
            self.flight(2, step, part).start()

    def fourth(self, step):
        z, y, c, x = self.at
        for part in range(self.count):
            self.flight(2, step, part).wait_recv()
            other = self.three_in[part].at[step]
            if x_first(self.parts, step, part):
                mine = self.two_x[part].at[step, y]
                first = lambda at: mine[at, :]
            else:
                mine = self.two_y[part].at[step]
                cols = columns_of(self.own[part], x)
                first = lambda at: mine[at, cols]
            add_rows(first, lambda at: other[at, :], self.last[part].at[step])
            if step:
                self.flight(3, step, part).start()

    def stage(self, number):
        if 0 <= number - 2 < 4:
            self.fourth(self.order[number - 2])
        if 0 <= number - 1 < 4:
            self.third(self.order[number - 1])
        if number < 4:
            self.second(self.order[number])

    def finish(self):
        for part in range(self.count):
            for step in (3, 2, 1):
                self.flight(3, step, part).wait_recv()
            matrix, piece = self.parts[part]
            target = self.outs[matrix] if piece is None else self.outs[matrix].at[piece]
            mine, others = self.last[part].at[0], self.last_in[part]

            def total(index, carry):
                at = pl.ds(pl.multiple_of(index * 16, 16), 16)
                value = mine[at, :].astype(jnp.float32)
                for step in range(3):
                    value = value + others[step, at, :].astype(jnp.float32)
                target[at, :] = value
                return carry

            lax.fori_loop(0, target.shape[0] // 16, total, 0)
        for phase in range(4):
            for step in range(1 if phase == 3 else 0, 4):
                for part in range(self.count):
                    self.flight(phase, step, part).wait_send()


def scatter_scratch(heights, widths):
    low = jnp.bfloat16
    sizes = list(zip(heights, widths))
    return (
        [pltpu.VMEM((4, 2, h, w), low) for h, w in sizes]
        + [pltpu.VMEM((4, 2, h, w), low) for h, w in sizes]
        + [pltpu.VMEM((4, 2, h, w // 2), low) for h, w in sizes]
        + [pltpu.VMEM((4, h, w), low) for h, w in sizes]
        + [pltpu.VMEM((4, h, w // 2), low) for h, w in sizes]
        + [pltpu.VMEM((4, h, w // 2), low) for h, w in sizes]
        + [pltpu.VMEM((3, h, w // 2), low) for h, w in sizes]
    )


def scatter_kernel(grad_ref, out_ref, *rest):
    scatter = Scatter(ATTEND_PARTS, (grad_ref,), (out_ref,), rest[:-3], rest[-3:])
    scatter.begin()
    for number in range(6):
        scatter.stage(number)
    scatter.finish()


def scatter_one(grad):
    rows, cols = grad.shape[0] // 16, grad.shape[1]
    count = len(ATTEND_PARTS)
    out = pl.pallas_call(
        scatter_kernel,
        in_specs=[pl.BlockSpec(memory_space=pl.ANY)],
        out_specs=pl.BlockSpec(memory_space=pltpu.VMEM),
        out_shape=jax.ShapeDtypeStruct((3, rows // 3, cols // 2), jnp.float32),
        scratch_shapes=scatter_scratch([rows // 3] * count, [cols] * count) + comm_sems(count),
        compiler_params=pltpu.CompilerParams(
            collective_id=1, has_side_effects=True, vmem_limit_bytes=40 * 2**20
        ),
        name="scatter_kernel",
    )(grad.reshape(ZS, 2, 2, 3, rows // 3, cols))
    return out.reshape(rows, cols // 2)


def at_steps(actions):
    for number, action in actions:
        pl.when(pl.program_id(0) == number)(action)


def forward_riding(triple_ref, bias_ref, label_ref, column_ref, *rest):
    gather = Gather(OTHER_PARTS, rest[:3], rest[5:8], rest[8:])

    def start():
        gather.begin()
        gather.stage(0)

    at_steps(
        [(0, start)] + [(number, lambda number=number: gather.stage(number)) for number in range(1, 6)]
    )
    forward_kernel(triple_ref, bias_ref, label_ref, column_ref, rest[3], rest[4])
    at_steps([(pl.num_programs(0) - 1, gather.finish)])


def backward_riding(
    triple_ref, grad_ref, log_ref, bias_ref, label_ref, column_ref, *rest
):
    scatter = Scatter(OTHER_PARTS, rest[:3], rest[5:8], rest[8:-3], rest[-3:])
    at_steps(
        [(0, scatter.begin)]
        + [(number + 1, lambda number=number: scatter.stage(number)) for number in range(6)]
    )
    backward_kernel(
        triple_ref, grad_ref, log_ref, bias_ref, label_ref, column_ref, rest[3], rest[4]
    )
    at_steps([(pl.num_programs(0) - 1, scatter.finish)])


def total_of(values):
    return jnp.sum(jnp.sum(values, axis=0, keepdims=True), axis=1, keepdims=True)


FINISH_STEPS = 3


def moment_kernel(*refs):
    owned, masters, firsts, seconds = refs[:4], refs[4:8], refs[8:12], refs[12:16]
    outs, square_ref = [refs[16 + 3 * slot : 19 + 3 * slot] for slot in range(4)], refs[28]
    place = lax.broadcasted_iota(jnp.int32, (8, 128), 0)
    lane = lax.broadcasted_iota(jnp.int32, (8, 128), 1)
    vector = jnp.zeros((8, 128), jnp.float32)
    for slot in range(4):
        rows, width = masters[slot].shape
        sums = [jnp.zeros((16, width), jnp.float32)] * 2
        for start in range(0, rows, 16):
            at = slice(start, start + 16)
            weight = masters[slot][at, :]
            results = moments(
                weight, firsts[slot][at, :], seconds[slot][at, :], owned[slot][at, :], decay_rate
            )
            for side in range(3):
                outs[slot][side][at, :] = results[side]
            sums = [sums[0] + weight * weight, sums[1] + results[2] * results[2]]
        for side in range(2):
            vector = jnp.where((place == slot) & (lane == side), total_of(sums[side]), vector)

    @pl.when(pl.program_id(0) == 0)
    def _():
        square_ref[...] = jnp.zeros_like(square_ref)

    square_ref[...] += vector


def sum_kernel(*refs):
    lines, bias_lines, table_ref, square_ref = refs[:4], refs[4:8], refs[8], refs[9]
    packs, incoming = refs[10:14], refs[14:18]
    sends, receives = refs[18:]
    z, y, c, x = places()
    hops = [
        device(z, y, 1 - c, x),
        device(z, y, c, 1 - x),
        device(z, 1 - y, c, x),
        device(far_z(z, 1), y, c, x),
        device(far_z(z, 2), y, c, x),
    ]
    greet(hops)
    for row in range(4):
        packs[0][row : row + 1, :] = lines[row][...]
    start = 0
    for part in bias_lines:
        packs[1][:, start : start + part.shape[1]] = part[...]
        start += part.shape[1]
    packs[2][...] = table_ref[...]
    packs[3][...] = square_ref[...]
    for hop in range(5):
        copies = [
            remote(packs[k], incoming[k].at[hop], sends, receives, hop * 4 + k, hops[hop])
            for k in range(4)
        ]
        for copy in copies:
            copy.start()
        for k in range(4):
            copies[k].wait()
            packs[k][...] = packs[k][...] + incoming[k][hop]


def apply_kernel(scale, *refs):
    masters, updates, packs = refs[:4], refs[4:8], refs[8:12]
    small = [refs[12 + 3 * slot : 15 + 3 * slot] for slot in range(4)]
    outs = [refs[24 + 2 * slot : 26 + 2 * slot] for slot in range(4)]
    small_outs = [refs[32 + 3 * slot : 35 + 3 * slot] for slot in range(4)]
    pair_ref = refs[44]
    norms = jnp.sqrt(packs[3][...])
    for slot in range(4):
        left, right = norms[slot : slot + 1, 0:1], norms[slot : slot + 1, 1:2]
        rate = learn_rate * left / (right + adam_eps)
        for start in range(0, masters[slot].shape[0], 16):
            at = slice(start, start + 16)
            fresh = masters[slot][at, :] - rate * updates[slot][at, :]
            outs[slot][0][at, :] = fresh
            outs[slot][1][at, :] = fresh.astype(jnp.bfloat16)

    @pl.when(pl.program_id(0) == 0)
    def _():
        place = lax.broadcasted_iota(jnp.int32, (8, 128), 0)
        lane = lax.broadcasted_iota(jnp.int32, (8, 128), 1)
        pairs = norms
        gradients = (
            packs[0][0:2, :],
            packs[0][2:4, :],
            packs[1][...],
            packs[2][:, : small[3][0].shape[1]],
        )
        for slot in range(4):
            weight = small[slot][0][...]
            momentum, variance, update = moments(
                weight, small[slot][1][...], small[slot][2][...], gradients[slot] * scale, 0.0
            )
            left = jnp.sqrt(total_of(weight * weight))
            right = jnp.sqrt(total_of(update * update))
            small_outs[slot][0][...] = weight - learn_rate * left / (right + adam_eps) * update
            small_outs[slot][1][...] = momentum
            small_outs[slot][2][...] = variance
            for side, value in enumerate((left, right)):
                pairs = jnp.where((place == 4 + slot) & (lane == side), value, pairs)
        pair_ref[...] = pairs


def finish_all(owned, masters, firsts, seconds, small, scale):
    wide = jnp.float32
    shapes = [master.shape for master in masters[:4]]

    def flat(slot, entry):
        return entry[None] if entry.ndim == 1 else entry.T if slot == 3 else entry

    def blocks(count):
        return [
            pl.BlockSpec((rows // FINISH_STEPS, cols), lambda step: (step, 0))
            for rows, cols in shapes
            for _ in range(count)
        ]

    def whole(shape):
        return pl.BlockSpec(shape, lambda step: (0, 0))

    def like(shape, kind=wide):
        return jax.ShapeDtypeStruct(shape, kind)

    first_out = pl.pallas_call(
        moment_kernel,
        grid=(FINISH_STEPS,),
        in_specs=blocks(1) * 4,
        out_specs=blocks(3) + [whole((8, 128))],
        out_shape=[like(shape) for shape in shapes for _ in range(3)] + [like((8, 128))],
        name="moment_kernel",
    )(*owned, *masters[:4], *firsts[:4], *seconds[:4])
    width = small[0][0].shape[0]
    pack_shapes = [(4, width), (1, masters[6].shape[0]), small[2].shape, (8, 128)]
    inside = pl.BlockSpec(memory_space=pltpu.VMEM)
    packs = pl.pallas_call(
        sum_kernel,
        in_specs=[inside] * 10,
        out_specs=[inside] * 4,
        out_shape=[like(shape) for shape in pack_shapes],
        scratch_shapes=[pltpu.VMEM((5,) + shape, wide) for shape in pack_shapes]
        + [pltpu.SemaphoreType.DMA((20,))] * 2,
        compiler_params=pltpu.CompilerParams(collective_id=2, has_side_effects=True),
        name="sum_kernel",
    )(
        *[line[None] for line in small[0]],
        *[line[None] for line in small[1]],
        small[2],
        first_out[-1],
    )
    small_in = [
        flat(slot, kind[4 + slot]) for slot in range(4) for kind in (masters, firsts, seconds)
    ]
    small_shapes = [entry.shape for entry in small_in]
    outs = pl.pallas_call(
        functools.partial(apply_kernel, scale),
        grid=(FINISH_STEPS,),
        in_specs=blocks(1) * 2
        + [whole(shape) for shape in pack_shapes]
        + [whole(shape) for shape in small_shapes],
        out_specs=blocks(2) + [whole(shape) for shape in small_shapes] + [whole((8, 128))],
        out_shape=[like(shape, kind) for shape in shapes for kind in (wide, jnp.bfloat16)]
        + [like(shape) for shape in small_shapes]
        + [like((8, 128))],
        name="apply_kernel",
    )(*masters[:4], *[first_out[3 * slot + 2] for slot in range(4)], *packs, *small_in)
    results = []
    for slot in range(4):
        fresh, copy = outs[2 * slot : 2 * slot + 2]
        results = results + [fresh, first_out[3 * slot], first_out[3 * slot + 1], copy]
    for slot in range(4):
        for side in range(3):
            entry = outs[8 + 3 * slot + side]
            entry = entry[0] if slot == 2 else entry.T if slot == 3 else entry
            results.append(entry)
    return results + [outs[-1][:, :2]]


def moments(weight, first, second, gradient, decay):
    momentum = beta_one * first + (1.0 - beta_one) * gradient
    variance = beta_two * second + (1.0 - beta_two) * gradient * gradient
    ratio = (
        momentum / (1.0 - beta_one**STEP) / (jnp.sqrt(variance / (1.0 - beta_two**STEP)) + adam_eps)
    )
    return (momentum, variance, ratio + decay * weight)


def body(
    inputs,
    cotangent,
    regions,
    attend,
    attend_first,
    attend_second,
    project,
    project_first,
    project_second,
    expand,
    expand_first,
    expand_second,
    contract,
    contract_first,
    contract_second,
    gains,
    gains_first,
    gains_second,
    shifts,
    shifts_first,
    shifts_second,
    biases,
    biases_first,
    biases_second,
    position,
    position_first,
    position_second,
):
    masters = (attend, project, expand, contract, gains, shifts, biases, position)
    firsts = (
        attend_first,
        project_first,
        expand_first,
        contract_first,
        gains_first,
        shifts_first,
        biases_first,
        position_first,
    )
    seconds = (
        attend_second,
        project_second,
        expand_second,
        contract_second,
        gains_second,
        shifts_second,
        biases_second,
        position_second,
    )
    dp_count = lax.axis_size("dp")
    shard_count = lax.axis_size("shard")
    tokens_all = inputs.shape[0] * inputs.shape[1] * dp_count * shard_count
    special = special_mesh(dp_count, shard_count)
    shards = tuple(master.astype(jnp.bfloat16) for master in masters[:4])
    if special:
        full = (gather_one(shards[0]),)
    else:
        halves = [lax.all_gather(shard, "dp", axis=0, tiled=True) for shard in shards]
        full = tuple(lax.all_gather(half, "shard", axis=1, tiled=True) for half in halves)
    labels = window_labels(regions)
    bias = table_to_bias(position)
    images = inputs.shape[0]
    values_low, cot_low, normed_low = enter(inputs, cotangent, gains[0], shifts[0])
    result_low, grad_input, grads, small_grads = whole_step(
        values_low,
        cot_low,
        normed_low,
        full,
        shards[1:] if special else None,
        gains,
        shifts,
        biases,
        bias,
        labels,
        1.0 / tokens_all,
    )
    result_low, grad_input = leave(result_low, grad_input, images)
    if special:
        owned = (scatter_one(grads[0]),) + tuple(grads[1:])
        rest = finish_all(owned, masters, firsts, seconds, small_grads, 1.0 / tokens_all)
        return tuple([result_low, grad_input] + rest)
    lines, bias_lines, table_grad = small_grads
    small_total = lax.psum(
        (
            jnp.stack(lines[:2]) / tokens_all,
            jnp.stack(lines[2:]) / tokens_all,
            jnp.concatenate(bias_lines) / tokens_all,
            table_grad[:, : position.shape[0]].T / tokens_all,
        ),
        ("dp", "shard"),
    )
    columns = [
        lax.psum_scatter(grad, "shard", scatter_dimension=1, tiled=True).astype(jnp.float32)
        for grad in grads
    ]
    owned = tuple(
        lax.psum_scatter(column, "dp", scatter_dimension=0, tiled=True) for column in columns
    )
    pieces = [
        moments(masters[slot], firsts[slot], seconds[slot], owned[slot], decay_rate)
        for slot in range(4)
    ]
    partial_value = jnp.stack(
        [
            jnp.stack(
                [jnp.sum(masters[slot] * masters[slot]), jnp.sum(pieces[slot][2] * pieces[slot][2])]
            )
            for slot in range(4)
        ]
    )
    squares = lax.psum(partial_value, ("dp", "shard"))
    matrix_norms = jnp.sqrt(squares)
    outputs = [result_low, grad_input]
    pairs = []
    for slot in range(4):
        momentum, variance, update = pieces[slot]
        fresh = (
            masters[slot]
            - learn_rate * matrix_norms[slot, 0] / (matrix_norms[slot, 1] + adam_eps) * update
        )
        outputs = outputs + [fresh, momentum, variance, fresh.astype(jnp.bfloat16)]
        pairs.append(matrix_norms[slot])
    for slot in range(4):
        weight = masters[4 + slot]
        momentum, variance, update = moments(
            weight, firsts[4 + slot], seconds[4 + slot], small_total[slot], 0.0
        )
        norms = jnp.stack([jnp.sqrt(jnp.sum(weight * weight)), jnp.sqrt(jnp.sum(update * update))])
        fresh = weight - learn_rate * norms[0] / (norms[1] + adam_eps) * update
        outputs = outputs + [fresh, momentum, variance]
        pairs.append(norms)
    outputs = outputs + [jnp.stack(pairs)]
    return tuple(outputs)


def solution(mesh):
    return jax.shard_map(
        body,
        mesh=mesh,
        in_specs=(
            P(("dp", "shard"), None, None),
            P(("dp", "shard"), None, None),
            P(),
            P("dp", "shard"),
            P("dp", "shard"),
            P("dp", "shard"),
            P("dp", "shard"),
            P("dp", "shard"),
            P("dp", "shard"),
            P("dp", "shard"),
            P("dp", "shard"),
            P("dp", "shard"),
            P("dp", "shard"),
            P("dp", "shard"),
            P("dp", "shard"),
            P(),
            P(),
            P(),
            P(),
            P(),
            P(),
            P(),
            P(),
            P(),
            P(),
            P(),
            P(),
        ),
        out_specs=(
            P(("dp", "shard"), None, None),
            P(("dp", "shard"), None, None),
            P("dp", "shard"),
            P("dp", "shard"),
            P("dp", "shard"),
            P("dp", "shard"),
            P("dp", "shard"),
            P("dp", "shard"),
            P("dp", "shard"),
            P("dp", "shard"),
            P("dp", "shard"),
            P("dp", "shard"),
            P("dp", "shard"),
            P("dp", "shard"),
            P("dp", "shard"),
            P("dp", "shard"),
            P("dp", "shard"),
            P("dp", "shard"),
            P(),
            P(),
            P(),
            P(),
            P(),
            P(),
            P(),
            P(),
            P(),
            P(),
            P(),
            P(),
            P(),
        ),
        check_vma=False,
    )
```
